16 devices in a mesh: dp: 2 (over y, z), ep: 8 (over x, core).
Axes of the slice: x: 4, y: 2, z: 1, core: 2. Of those that a mesh axis runs over, the one named last changes fastest.
The devices are a block of a 4x4x8 slice.
Arguments:
- x_in: bfloat16 [1024, 768], P(('dp', 'ep')), parts along dimension 0
- idx_a: int32 [1024, 8], P(('dp', 'ep')), parts along dimension 0
- idx_b: int32 [1024, 8], P(('dp', 'ep')), parts along dimension 0
- gate_a: float32 [1024, 8], P(('dp', 'ep')), parts along dimension 0
- gate_b: float32 [1024, 8], P(('dp', 'ep')), parts along dimension 0
- dy_out: bfloat16 [1024, 768], P(('dp', 'ep')), parts along dimension 0
- w1_a: bfloat16 [128, 768, 256], P('ep')
- w3_a: bfloat16 [128, 768, 256], P('ep')
- w2_a: bfloat16 [128, 256, 768], P('ep')
- w1_b: bfloat16 [128, 768, 256], P('ep')
- w3_b: bfloat16 [128, 768, 256], P('ep')
- w2_b: bfloat16 [128, 256, 768], P('ep')
Outputs:
- output 1: bfloat16 [1024, 768], P(('dp', 'ep')), parts along dimension 0
- output 2: bfloat16 [1024, 768], P(('dp', 'ep')), parts along dimension 0
- output 3: float32 [256, 768, 256], P(('dp', 'ep')), parts along dimension 0
- output 4: float32 [256, 768, 256], P(('dp', 'ep')), parts along dimension 0
- output 5: float32 [256, 256, 768], P(('dp', 'ep')), parts along dimension 0
- output 6: float32 [256, 768, 256], P(('dp', 'ep')), parts along dimension 0
- output 7: float32 [256, 768, 256], P(('dp', 'ep')), parts along dimension 0
- output 8: float32 [256, 256, 768], P(('dp', 'ep')), parts along dimension 0
- output 9: float32 [1024, 8], P(('dp', 'ep')), parts along dimension 0
- output 10: float32 [1024, 8], P(('dp', 'ep')), parts along dimension 0
There are 2 independent parts. The reference program is written for one: setup_inputs(seed, part) draws one part's arguments, and reference() takes and returns one part's arrays. A program takes and returns all parts, laid end to end along the dimension named above; an argument that names none is the same for every part.
All inputs are finite; a program needn't handle non-finite values.
Results may differ from the reference program's by a relative error of at most 0.00668.
Values are sent between devices in bfloat16 or wider.
A program may use at most 768 MiB of HBM per device.

```python
import jax
import jax.numpy as jnp
from jax import lax

TOKENS = 64
D = 768
FF = 256
EXPERTS = 128
TOP = 8
GROUP = 8
CAP = 16
HOT = 8


def draw_routing(root_key):
    key_hot, key_dev = jax.random.split(root_key)
    ranking = jax.random.permutation(key_hot, EXPERTS)
    cold_total = EXPERTS - HOT
    spare_pairs = TOKENS * TOP - HOT * CAP
    base_count = spare_pairs // cold_total
    extra_count = spare_pairs - base_count * cold_total

    def one_device(dev_key):
        key_count, key_rows, key_shift = jax.random.split(dev_key, 3)
        cold_rank = jax.random.permutation(key_count, cold_total)
        cold_count = base_count + (cold_rank < extra_count).astype(jnp.int32)
        by_rank = jnp.concatenate([jnp.full((HOT,), CAP, jnp.int32), cold_count])
        expert_count = jnp.zeros((EXPERTS,), jnp.int32).at[ranking].set(by_rank)
        run_ends = jnp.cumsum(expert_count)
        positions = jnp.arange(TOKENS * TOP, dtype=jnp.int32)
        sorted_ids = jnp.searchsorted(run_ends, positions, side="right").astype(jnp.int32)
        id_table = sorted_ids.reshape(TOP, TOKENS).T
        id_table = id_table[jax.random.permutation(key_rows, TOKENS)]
        row_shift = jax.random.randint(key_shift, (TOKENS, 1), 0, TOP)
        col_order = (jnp.arange(TOP)[None, :] + row_shift) % TOP
        return jnp.take_along_axis(id_table, col_order, axis=1)

    return jax.vmap(one_device)(jax.random.split(key_dev, GROUP)).reshape(GROUP * TOKENS, TOP)


def setup_inputs(seed: int = 0, part: int = 0) -> dict:
    root_key = jax.random.key(seed)
    shared_keys = jax.random.split(root_key, 6)
    part_keys = jax.random.split(jax.random.fold_in(root_key, part), 6)
    row_total = GROUP * TOKENS
    gate_scale = 1.5 / TOP ** 0.5
    in_scale = D ** -0.5
    mid_scale = FF ** -0.5
    x_in = jax.random.normal(part_keys[0], (row_total, D), jnp.float32).astype(jnp.bfloat16)
    idx_a = draw_routing(part_keys[1])
    idx_b = draw_routing(part_keys[2])
    gate_a = (0.5 + jax.random.uniform(part_keys[3], (row_total, TOP), jnp.float32)) * gate_scale
    gate_b = (0.5 + jax.random.uniform(part_keys[4], (row_total, TOP), jnp.float32)) * gate_scale
    dy_out = jax.random.normal(part_keys[5], (row_total, D), jnp.float32).astype(jnp.bfloat16)
    w1_a = (jax.random.normal(shared_keys[0], (EXPERTS, D, FF), jnp.float32) * in_scale).astype(jnp.bfloat16)
    w3_a = (jax.random.normal(shared_keys[1], (EXPERTS, D, FF), jnp.float32) * in_scale).astype(jnp.bfloat16)
    w2_a = (jax.random.normal(shared_keys[2], (EXPERTS, FF, D), jnp.float32) * mid_scale).astype(jnp.bfloat16)
    w1_b = (jax.random.normal(shared_keys[3], (EXPERTS, D, FF), jnp.float32) * in_scale).astype(jnp.bfloat16)
    w3_b = (jax.random.normal(shared_keys[4], (EXPERTS, D, FF), jnp.float32) * in_scale).astype(jnp.bfloat16)
    w2_b = (jax.random.normal(shared_keys[5], (EXPERTS, FF, D), jnp.float32) * mid_scale).astype(jnp.bfloat16)
    return {"x_in": x_in, "idx_a": idx_a, "idx_b": idx_b, "gate_a": gate_a, "gate_b": gate_b, "dy_out": dy_out, "w1_a": w1_a, "w3_a": w3_a, "w2_a": w2_a, "w1_b": w1_b, "w3_b": w3_b, "w2_b": w2_b}


def expert_forward(u_rows, w_gate, w_up, w_down):
    pre_gate = jnp.dot(u_rows, w_gate, preferred_element_type=jnp.float32)
    pre_up = jnp.dot(u_rows, w_up, preferred_element_type=jnp.float32)
    hidden = (jax.nn.silu(pre_gate) * pre_up).astype(jnp.bfloat16)
    out_rows = jnp.dot(hidden, w_down, preferred_element_type=jnp.float32).astype(jnp.bfloat16)
    return pre_gate, pre_up, hidden, out_rows


def device_slots(flat_ids):
    onehot = (flat_ids[:, None] == jnp.arange(EXPERTS, dtype=jnp.int32)[None, :]).astype(jnp.int32)
    return jnp.sum(jnp.cumsum(onehot, axis=0) * onehot, axis=1) - 1


def expert_table(ids):
    per_device = ids.reshape(GROUP, TOKENS * TOP)
    pair_slot = lax.map(device_slots, per_device)
    expert_row = jnp.arange(GROUP, dtype=jnp.int32)[:, None] * CAP + pair_slot
    pair_ids = jnp.arange(GROUP * TOKENS * TOP, dtype=jnp.int32).reshape(GROUP, TOKENS * TOP)
    empty_pair = GROUP * TOKENS * TOP
    return jnp.full((EXPERTS, GROUP * CAP), empty_pair, jnp.int32).at[per_device, expert_row].set(pair_ids)


def layer_forward(x_rows, gates, table, w_gate, w_up, w_down):
    x_pad = jnp.concatenate([x_rows, jnp.zeros((1, D), x_rows.dtype)])
    gate_pad = jnp.concatenate([gates.reshape(-1), jnp.zeros((1,), gates.dtype)])

    def expert_step(out_acc, step_in):
        pair_ids, gate_w, up_w, down_w = step_in
        tok_index = pair_ids // TOP
        out_rows = expert_forward(x_pad[tok_index], gate_w, up_w, down_w)[3]
        weighted = gate_pad[pair_ids][:, None] * out_rows.astype(jnp.float32)
        return out_acc.at[tok_index].add(weighted), None

    out_acc = jnp.zeros((GROUP * TOKENS + 1, D), jnp.float32)
    out_acc = lax.scan(expert_step, out_acc, (table, w_gate, w_up, w_down))[0]
    return (x_rows.astype(jnp.float32) + out_acc[:-1]).astype(jnp.bfloat16)


def layer_backward(dy_rows, x_rows, gates, table, w_gate, w_up, w_down):
    x_pad = jnp.concatenate([x_rows, jnp.zeros((1, D), x_rows.dtype)])
    dy_pad = jnp.concatenate([dy_rows, jnp.zeros((1, D), dy_rows.dtype)])
    gate_pad = jnp.concatenate([gates.reshape(-1), jnp.zeros((1,), gates.dtype)])

    def expert_step(carry_in, step_in):
        dx_acc, dgate_acc = carry_in
        pair_ids, gate_w, up_w, down_w = step_in
        tok_index = pair_ids // TOP
        u_rows = x_pad[tok_index]
        dy_exp = dy_pad[tok_index].astype(jnp.float32)
        pre_gate, pre_up, hidden, out_rows = expert_forward(u_rows, gate_w, up_w, down_w)
        dgate_rows = jnp.sum(dy_exp * out_rows.astype(jnp.float32), axis=1)
        d_out = (gate_pad[pair_ids][:, None] * dy_exp).astype(jnp.bfloat16)
        dw_down = jnp.dot(hidden.T, d_out, preferred_element_type=jnp.float32)
        d_hidden = jnp.dot(d_out, down_w.T, preferred_element_type=jnp.float32)
        gate_sig = jax.nn.sigmoid(pre_gate)
        d_pre_gate = (d_hidden * pre_up * gate_sig * (1.0 + pre_gate * (1.0 - gate_sig))).astype(jnp.bfloat16)
        d_pre_up = (d_hidden * jax.nn.silu(pre_gate)).astype(jnp.bfloat16)
        dw_gate = jnp.dot(u_rows.T, d_pre_gate, preferred_element_type=jnp.float32)
        dw_up = jnp.dot(u_rows.T, d_pre_up, preferred_element_type=jnp.float32)
        du_rows = (jnp.dot(d_pre_gate, gate_w.T, preferred_element_type=jnp.float32) + jnp.dot(d_pre_up, up_w.T, preferred_element_type=jnp.float32)).astype(jnp.bfloat16)
        dx_acc = dx_acc.at[tok_index].add(du_rows.astype(jnp.float32))
        dgate_acc = dgate_acc.at[pair_ids].set(dgate_rows)
        return (dx_acc, dgate_acc), (dw_gate, dw_up, dw_down)

    dx_acc = jnp.zeros((GROUP * TOKENS + 1, D), jnp.float32)
    dgate_acc = jnp.zeros((GROUP * TOKENS * TOP + 1,), jnp.float32)
    (dx_acc, dgate_acc), grads = lax.scan(expert_step, (dx_acc, dgate_acc), (table, w_gate, w_up, w_down))
    dx_rows = (dy_rows.astype(jnp.float32) + dx_acc[:-1]).astype(jnp.bfloat16)
    return dx_rows, dgate_acc[:-1].reshape(GROUP * TOKENS, TOP), grads


def reference(x_in, idx_a, idx_b, gate_a, gate_b, dy_out, w1_a, w3_a, w2_a, w1_b, w3_b, w2_b):
    table_a = expert_table(idx_a)
    table_b = expert_table(idx_b)
    x_mid = layer_forward(x_in, gate_a, table_a, w1_a, w3_a, w2_a)
    x_out = layer_forward(x_mid, gate_b, table_b, w1_b, w3_b, w2_b)
    dx_mid, dgate_b, grads_b = layer_backward(dy_out, x_mid, gate_b, table_b, w1_b, w3_b, w2_b)
    dx_in, dgate_a, grads_a = layer_backward(dx_mid, x_in, gate_a, table_a, w1_a, w3_a, w2_a)
    return (x_out, dx_in, grads_a[0], grads_a[1], grads_a[2], grads_b[0], grads_b[1], grads_b[2], dgate_a, dgate_b)
```

```python
import functools

import jax
import jax.numpy as jnp
from jax import lax
from jax.experimental import pallas as pl
from jax.experimental.pallas import tpu as pltpu
from jax.sharding import PartitionSpec as P

BF16 = jnp.bfloat16
F32 = jnp.float32
MESH = pl.DeviceIdType.MESH
LANES = 128
CAP_FACTOR = 4
BF16_MAX = 3.3895313892515355e38
VMEM_LIMIT = 60 * 1024 * 1024
VMEM = pl.BlockSpec(memory_space=pltpu.VMEM)
ANY = pl.BlockSpec(memory_space=pl.ANY)


def mm(lhs, rhs):
    return jnp.dot(lhs, rhs, preferred_element_type=F32)


def mm_tn(lhs, rhs):
    return lax.dot_general(lhs, rhs, (((0,), (0,)), ((), ())), preferred_element_type=F32)


def mm_nt(lhs, rhs):
    return lax.dot_general(lhs, rhs, (((1,), (1,)), ((), ())), preferred_element_type=F32)


def iota(shape, dim):
    return lax.broadcasted_iota(jnp.int32, shape, dim)


def routing_maps(me, meta, layer, s_ref, g_ref, rel_ref, top_k, local):
    n_dev = meta.shape[0]
    base = (me * local).astype(F32)
    row = 2 * layer * top_k
    rel_ref[...] = meta[:, row : row + top_k, :] - base
    hit = [jnp.zeros((n_dev, LANES), F32) for _ in range(local)]
    gate = [jnp.zeros((n_dev, LANES), F32) for _ in range(local)]
    for j in range(top_k):
        rel_j = meta[:, row + j, :] - base
        gate_j = meta[:, row + top_k + j, :]
        for e in range(local):
            match = rel_j == float(e)
            hit[e] = jnp.where(match, 1.0, hit[e])
            gate[e] = jnp.where(match, gate_j, gate[e])
    hit = jnp.concatenate(hit, axis=0)
    earlier = (iota((LANES, LANES), 0) < iota((LANES, LANES), 1)).astype(F32).astype(BF16)
    slot = jnp.where(hit > 0.0, mm(hit.astype(BF16), earlier), -1.0)
    s_ref[...] = slot.reshape(local, n_dev, LANES)
    for e in range(local):
        g_ref[e] = gate[e]


def expert_rows(s_map, d, rows, cap):
    pairs, lanes = s_map.shape
    local, n_dev, tok = pairs // 8, 8, rows.shape[0]
    pick = (iota((local * cap, pairs), 1) == iota((local * cap, pairs), 0) // cap * n_dev + d)
    slot = mm(pick.astype(F32).astype(BF16), s_map.astype(BF16))
    onehot = jnp.where(slot == (iota((local * cap, lanes), 0) % cap).astype(F32), 1.0, 0.0).astype(BF16)
    return mm(onehot[:, :tok], rows).astype(BF16)


def limbs(gate):
    hi = jnp.minimum(gate, BF16_MAX).astype(BF16)
    rest = gate - hi.astype(F32)
    mid = rest.astype(BF16)
    return hi, mid, (rest - mid.astype(F32)).astype(BF16)


def scatter_lhs(s_map, g_map, tok):
    stack = [s_map.T[:tok].astype(BF16)]
    if g_map is not None:
        stack += [limb.T[:tok].astype(BF16) for limb in (x.astype(F32) for x in limbs(g_map))]
    return jnp.concatenate(stack, axis=0)


def token_sums(stack, d, out_rows, tok, cap):
    pairs = stack.shape[1]
    n_rows = out_rows.shape[0]
    spread = iota((pairs, n_rows), 0) == iota((pairs, n_rows), 1) // cap * 8 + d
    maps = mm(stack, spread.astype(F32).astype(BF16))
    match = maps[:tok] == (iota((tok, n_rows), 1) % cap).astype(F32)
    if stack.shape[0] == tok:
        return mm(jnp.where(match, 1.0, 0.0).astype(BF16), out_rows)
    terms = (stack.shape[0] - tok) // tok
    lhs = [jnp.where(match, maps[(i + 1) * tok : (i + 2) * tok], 0.0).astype(BF16) for i in range(terms)]
    sums = mm(jnp.concatenate(lhs, axis=0), out_rows)
    total = sums[:tok]
    for i in range(1, terms):
        total = total + sums[i * tok : (i + 1) * tok]
    return total


def forward_rows(u, w_gate, w_up, w_down):
    pre_gate = mm(u, w_gate)
    pre_up = mm(u, w_up)
    sig = jax.nn.sigmoid(pre_gate)
    act = pre_gate * sig
    hidden = (act * pre_up).astype(BF16)
    return pre_gate, pre_up, sig, act, hidden, mm(hidden, w_down).astype(BF16)


class Links:
    def __init__(self, n_dev, send_sems, recv_sems):
        me = lax.axis_index("ep")
        self.n = n_dev
        self.me = me
        self.core = lax.rem(me, 2)
        self.partner = me + 1 - 2 * self.core
        self.right = lax.rem(me + 2, n_dev)
        self.left = lax.rem(me + n_dev - 2, n_dev)
        self.opp = lax.rem(me + 4, n_dev)
        self.send_sems, self.recv_sems = send_sems, recv_sems
        self.used = 0
        self.started = []

    def greet(self):
        barrier = pltpu.get_barrier_semaphore()
        for peer in (self.partner, self.left, self.right):
            pl.semaphore_signal(barrier, inc=1, device_id={"ep": peer}, device_id_type=MESH)
        pl.semaphore_wait(barrier, 3)

    def copy(self, src, dst, peer):
        slot = self.used
        self.used += 1
        rdma = pltpu.make_async_remote_copy(
            src_ref=src, dst_ref=dst, send_sem=self.send_sems.at[slot], recv_sem=self.recv_sems.at[slot],
            device_id={"ep": peer}, device_id_type=MESH)
        rdma.start()
        self.started.append(rdma)
        return rdma

    def drain(self):
        for rdma in self.started:
            rdma.wait_send()


class Gather:
    COPIES = 9

    def __init__(self, links, own, full):
        k, self.k, self.full = links, links, full
        self.half = own.shape[0] // 2
        self.to_right = k.copy(own, full.at[k.me], k.right)
        self.to_left = k.copy(own, full.at[k.me], k.left)
        self.to_partner = k.copy(own, full.at[k.me], k.partner)

    def pass_on(self):
        k, full, half = self.k, self.full, self.half
        self.to_right.wait_recv()
        self.far_a = k.copy(full.at[k.left, pl.ds(0, half)], full.at[k.left, pl.ds(0, half)], k.right)
        self.side_a = k.copy(full.at[k.left], full.at[k.left], k.partner)
        self.to_left.wait_recv()
        self.far_b = k.copy(full.at[k.right, pl.ds(half, half)], full.at[k.right, pl.ds(half, half)], k.left)
        self.side_b = k.copy(full.at[k.right], full.at[k.right], k.partner)

    def pass_far(self):
        k, full, half = self.k, self.full, self.half
        self.far_a.wait_recv()
        self.last_a = k.copy(full.at[k.opp, pl.ds(0, half)], full.at[k.opp, pl.ds(0, half)], k.partner)
        self.far_b.wait_recv()
        self.last_b = k.copy(full.at[k.opp, pl.ds(half, half)], full.at[k.opp, pl.ds(half, half)], k.partner)

    def wait_partner(self):
        self.to_partner.wait_recv()

    def wait_sides(self):
        self.side_a.wait_recv()
        self.side_b.wait_recv()

    def wait_last(self):
        self.last_a.wait_recv()
        self.last_b.wait_recv()

    def finish(self):
        self.wait_partner()
        self.wait_sides()
        self.wait_last()


class Reduce:
    COPIES = 10

    @staticmethod
    def scratch(rows, width):
        return [pltpu.VMEM((4, rows, width), F32), pltpu.VMEM((4, rows, width), F32), pltpu.VMEM((3, rows, width), F32)]

    def __init__(self, links, part, bufs, split=True):
        self.k, self.part = links, part
        self.near, self.mine, self.got = bufs
        rows = part.shape[1]
        self.rows = rows
        self.half = rows // 2 if split else rows
        self.side = {}

    def block(self, hop, core):
        k = self.k
        return lax.rem(k.me - k.core + 2 * hop, k.n) + core

    def start_side(self, hop):
        k = self.k
        self.side[hop] = k.copy(self.part.at[self.block(hop, 1 - k.core)], self.near.at[hop], k.partner)

    def start(self):
        for hop in (2, 1, 3, 0):
            self.start_side(hop)

    def add(self, hop, lo, hi, extra=None):
        own = self.part[self.block(hop, self.k.core), lo:hi, :]
        total = own + self.near[hop, lo:hi, :]
        if extra is not None:
            total = total + extra
        self.mine[hop, lo:hi, :] = total

    def far(self):
        k, half, rows = self.k, self.half, self.rows
        self.side[2].wait_recv()
        self.add(2, 0, rows)
        a = pl.ds(0, half)
        self.far_a = k.copy(self.mine.at[2, a], self.got.at[2, a], k.right)
        if half < rows:
            b = pl.ds(half, rows - half)
            self.far_b = k.copy(self.mine.at[2, b], self.got.at[2, b], k.left)

    def near_sends(self):
        k, half, rows = self.k, self.half, self.rows
        self.side[1].wait_recv()
        if half < rows:
            b = pl.ds(half, rows - half)
            self.add(1, half, rows)
            self.right_b = k.copy(self.mine.at[1, b], self.got.at[0, b], k.right)
        self.side[3].wait_recv()
        self.add(3, 0, half)
        a = pl.ds(0, half)
        self.left_a = k.copy(self.mine.at[3, a], self.got.at[1, a], k.left)

    def relay(self):
        k, half, rows = self.k, self.half, self.rows
        a = pl.ds(0, half)
        self.far_a.wait_recv()
        self.add(1, 0, half, self.got[2, :half, :])
        self.right_a = k.copy(self.mine.at[1, a], self.got.at[0, a], k.right)
        if half < rows:
            b = pl.ds(half, rows - half)
            self.far_b.wait_recv()
            self.add(3, half, rows, self.got[2, half:, :])
            self.left_b = k.copy(self.mine.at[3, b], self.got.at[1, b], k.left)

    def result(self):
        half, rows = self.half, self.rows
        self.side[0].wait_recv()
        if half < rows:
            self.right_b.wait_recv()
        self.left_a.wait_recv()
        self.right_a.wait_recv()
        if half < rows:
            self.left_b.wait_recv()
        return self.part[self.k.me] + self.near[0] + self.got[0] + self.got[1]


def load_weights(pairs, sems, local):
    def start(e, carry):
        for i, (src, dst) in enumerate(pairs):
            pltpu.make_async_copy(src.at[e], dst.at[e], sems.at[i, e]).start()
        return carry
    lax.fori_loop(0, local, start, 0)


def wait_weights(pairs, sems, e):
    for i, (src, dst) in enumerate(pairs):
        pltpu.make_async_copy(src.at[e], dst.at[e], sems.at[i, e]).wait()


def forward_experts(pairs, sems, u_ref, o_ref, cap):
    n_dev, local, _, width = u_ref.shape

    def step(e, carry):
        wait_weights(pairs, sems, e)
        u = u_ref[:, e].reshape(n_dev * cap, width)
        out = forward_rows(u, *(dst[e] for _, dst in pairs))[-1]
        o_ref[:, e] = out.reshape(n_dev, cap, width)
        return carry
    lax.fori_loop(0, local, step, 0)


def first_kernel(dims, x_ref, dy_ref, meta_ref, w1, w3, w2,
                 mid_all, dy_all, mid_own, sa, ga, rela, sb, gb, relb,
                 x_all, y_all, m_all, meta_all, u_ref, o_ref, part, near, mine, got, mid_buf, w1_v, w3_v, w2_v,
                 w_sems, send_sems, recv_sems):
    n_dev, tok, width, local, cap, top_k = dims
    pairs = ((w1, w1_v), (w3, w3_v), (w2, w2_v))
    load_weights(pairs, w_sems, local)
    links = Links(n_dev, send_sems, recv_sems)
    me = links.me
    links.greet()
    meta_g = Gather(links, meta_ref, meta_all)
    x_g = Gather(links, x_ref, x_all)
    y_g = Gather(links, dy_ref, y_all)
    meta_all[me] = meta_ref[...]
    x_all[me] = x_ref[...]
    y_all[me] = dy_ref[...]
    meta_g.pass_on()
    x_g.pass_on()
    meta_g.pass_far()
    x_g.pass_far()
    meta_g.finish()
    meta = meta_all[...]
    routing_maps(me, meta, 0, sa, ga, rela, top_k, local)
    routing_maps(me, meta, 1, sb, gb, relb, top_k, local)
    s_map = sa[...].reshape(local * n_dev, LANES)

    def rows_of(d):
        u_ref[d] = expert_rows(s_map, d, x_all[d], cap).reshape(local, cap, width)

    rows_of(me)
    rows_of(links.left)
    rows_of(links.right)
    rows_of(links.opp)
    y_g.pass_on()
    x_g.wait_partner()
    rows_of(links.partner)
    x_g.wait_sides()
    side = 1 - 2 * links.core
    rows_of(links.left + side)
    rows_of(links.right + side)
    x_g.wait_last()
    rows_of(links.opp + side)
    forward_experts(pairs, w_sems, u_ref, o_ref, cap)
    y_g.pass_far()
    stack = scatter_lhs(s_map, ga[...].reshape(local * n_dev, LANES), tok)
    red = Reduce(links, part, (near, mine, got))

    def sums_of(d):
        part[d] = token_sums(stack, d, o_ref[d].reshape(local * cap, width), tok, cap)

    for hop in (2, 1, 3, 0):
        sums_of(red.block(hop, 1 - links.core))
        red.start_side(hop)
    for hop in (2, 1, 3, 0):
        sums_of(red.block(hop, links.core))
    red.far()
    red.near_sends()
    red.relay()
    x_mid = (x_ref[...].astype(F32) + red.result()).astype(BF16)
    mid_buf[...] = x_mid
    mid_own[...] = x_mid
    m_all[me] = x_mid
    m_g = Gather(links, mid_buf, m_all)
    m_g.pass_on()
    m_g.pass_far()
    y_g.finish()
    dy_all[...] = y_all[...]
    m_g.finish()
    mid_all[...] = m_all[...]
    links.drain()


def backward_kernel(dims, x_all, dy_all, s_ref, g_ref, rel_ref, w1, w3, w2,
                    dw1, dw3, dw2, part, dgate, u_ref, y_ref, du_ref, dg_ref):
    n_dev, tok, width, local, cap, top_k = dims
    e = pl.program_id(0)
    n_rows = n_dev * cap

    @pl.when(e == 0)
    def _():
        s_map = s_ref[...].reshape(local * n_dev, LANES)

        def rows_of(d, carry):
            u_ref[d] = expert_rows(s_map, d, x_all[d], cap).reshape(local, cap, width)
            y_ref[d] = expert_rows(s_map, d, dy_all[d], cap).reshape(local, cap, width)
            return carry
        lax.fori_loop(0, n_dev, rows_of, 0)

    u = u_ref[:, e].reshape(n_rows, width)
    dy = y_ref[:, e].reshape(n_rows, width).astype(F32)
    w_gate, w_up, w_down = w1[0], w3[0], w2[0]
    pre_gate, pre_up, sig, act, hidden, out = forward_rows(u, w_gate, w_up, w_down)
    slot = s_ref[e][:, None, :] == iota((n_dev, cap, LANES), 1).astype(F32)
    gate_row = jnp.sum(jnp.where(slot, g_ref[e][:, None, :], 0.0), axis=2, keepdims=True).reshape(n_rows, 1)
    dg_row = jnp.sum(dy * out.astype(F32), axis=1, keepdims=True).reshape(n_dev, cap, 1)
    dg_ref[e] = jnp.sum(jnp.where(slot, dg_row, 0.0), axis=1)
    q = (gate_row * dy).astype(BF16)
    dw2[0] = mm_tn(hidden, q)
    d_hidden = mm_nt(q, w_down)
    d_gate = (d_hidden * pre_up * sig * (1.0 + pre_gate * (1.0 - sig))).astype(BF16)
    d_up = (d_hidden * act).astype(BF16)
    dw1[0] = mm_tn(u, d_gate)
    dw3[0] = mm_tn(u, d_up)
    du = (mm_nt(d_gate, w_gate) + mm_nt(d_up, w_up)).astype(BF16)
    du_ref[:, e] = du.reshape(n_dev, cap, width)

    @pl.when(e == local - 1)
    def _():
        s_map = s_ref[...].reshape(local * n_dev, LANES)
        stack = scatter_lhs(s_map, None, tok)

        def sums_of(d, carry):
            part[d] = token_sums(stack, d, du_ref[d].reshape(local * cap, width), tok, cap)
            return carry
        lax.fori_loop(0, n_dev, sums_of, 0)
        for d in range(n_dev):
            total = jnp.zeros((top_k, LANES), F32)
            for i in range(local):
                total = jnp.where(rel_ref[d] == float(i), dg_ref[i, d : d + 1, :], total)
            dgate[d] = total


def middle_kernel(dims, part_b, dg_part, dy_ref, x_ref, mid_all, sb, gb, w1, w3, w2,
                  dmid_all, x_again, dmid_own, dgate, part_x,
                  d_all, x_all, u_ref, o_ref, near, mine, got, dg_near, dg_mine, dg_got, d_buf, w1_v, w3_v, w2_v,
                  w_sems, send_sems, recv_sems):
    n_dev, tok, width, local, cap, top_k = dims
    pairs = ((w1, w1_v), (w3, w3_v), (w2, w2_v))
    load_weights(pairs, w_sems, local)
    links = Links(n_dev, send_sems, recv_sems)
    me = links.me
    links.greet()
    red = Reduce(links, part_b, (near, mine, got))
    dg = Reduce(links, dg_part, (dg_near, dg_mine, dg_got), split=False)
    red.start()
    dg.start()
    x_g = Gather(links, x_ref, x_all)
    x_all[me] = x_ref[...]
    red.far()
    red.near_sends()
    red.relay()
    dg.far()
    dg.near_sends()
    x_g.pass_on()
    dx = (dy_ref[...].astype(F32) + red.result()).astype(BF16)
    d_buf[...] = dx
    dmid_own[...] = dx
    d_all[me] = dx
    d_g = Gather(links, d_buf, d_all)
    dg.relay()
    x_g.pass_far()
    d_g.pass_on()
    d_g.pass_far()

    s_map = sb[...].reshape(local * n_dev, LANES)

    def rows_of(d, carry):
        u_ref[d] = expert_rows(s_map, d, mid_all[d], cap).reshape(local, cap, width)
        return carry
    lax.fori_loop(0, n_dev, rows_of, 0)
    forward_experts(pairs, w_sems, u_ref, o_ref, cap)
    stack = scatter_lhs(s_map, gb[...].reshape(local * n_dev, LANES), tok)

    def sums_of(d, carry):
        part_x[d] = token_sums(stack, d, o_ref[d].reshape(local * cap, width), tok, cap)
        return carry
    lax.fori_loop(0, n_dev, sums_of, 0)
    dgate[...] = dg.result()
    x_g.finish()
    x_again[...] = x_all[...]
    d_g.finish()
    dmid_all[...] = d_all[...]
    links.drain()


def last_kernel(dims, part_a, dg_part, part_x, dmid_ref, mid_ref, dx_out, dgate, x_out,
                near, mine, got, dg_near, dg_mine, dg_got, x_near, x_mine, x_got, send_sems, recv_sems):
    links = Links(dims[0], send_sems, recv_sems)
    links.greet()
    reds = (Reduce(links, part_a, (near, mine, got)), Reduce(links, part_x, (x_near, x_mine, x_got)),
            Reduce(links, dg_part, (dg_near, dg_mine, dg_got), split=False))
    for red in reds:
        red.start()
    for red in reds:
        red.far()
        red.near_sends()
    for red in reds:
        red.relay()
    dx_out[...] = (dmid_ref[...].astype(F32) + reds[0].result()).astype(BF16)
    x_out[...] = (mid_ref[...].astype(F32) + reds[1].result()).astype(BF16)
    dgate[...] = reds[2].result()
    links.drain()


def remote_params(ident):
    return pltpu.CompilerParams(collective_id=ident, has_side_effects=True, vmem_limit_bytes=VMEM_LIMIT)


def dma_sems(count):
    return [pltpu.SemaphoreType.DMA((count,)), pltpu.SemaphoreType.DMA((count,))]


def solution(mesh):
    n_dev = mesh.shape["ep"]
    tok_spec = P(("dp", "ep"))
    w_spec = P("ep")

    def device_program(x_in, idx_a, idx_b, gate_a, gate_b, dy_out, w1_a, w3_a, w2_a, w1_b, w3_b, w2_b):
        tok, top_k = idx_a.shape
        width = x_in.shape[1]
        local, _, inner = w1_a.shape
        cap = CAP_FACTOR * tok * top_k // (local * n_dev)
        dims = (n_dev, tok, width, local, cap, top_k)
        sds = jax.ShapeDtypeStruct
        rows_all = sds((n_dev, tok, width), BF16)
        part_all = sds((n_dev, tok, width), F32)
        dg_all = sds((n_dev, top_k, LANES), F32)
        map_s = sds((local, n_dev, LANES), F32)
        own = sds((tok, width), BF16)

        def lanes(rows, fill):
            return jnp.pad(rows.T.astype(F32), ((0, 0), (0, LANES - tok)), constant_values=fill)

        meta = jnp.concatenate([lanes(idx_a, -1.0), lanes(gate_a, 0.0), lanes(idx_b, -1.0), lanes(gate_b, 0.0)])
        weights_v = [pltpu.VMEM((local, width, inner), BF16)] * 2 + [pltpu.VMEM((local, inner, width), BF16)]
        w_sems = pltpu.SemaphoreType.DMA((3, local))
        rows_v = pltpu.VMEM((n_dev, tok, width), BF16)
        expert_v = pltpu.VMEM((n_dev, local, cap, width), BF16)

        count = 4 * Gather.COPIES + Reduce.COPIES
        mid_all, dy_all, mid_own, sa, ga, rela, sb, gb, relb = pl.pallas_call(
            functools.partial(first_kernel, dims),
            out_shape=(rows_all, rows_all, own, map_s, map_s, dg_all, map_s, map_s, dg_all),
            in_specs=[VMEM] * 3 + [ANY] * 3,
            out_specs=[VMEM] * 9,
            scratch_shapes=[rows_v, rows_v, rows_v, pltpu.VMEM((n_dev, 4 * top_k, LANES), F32), expert_v, expert_v,
                            pltpu.VMEM((n_dev, tok, width), F32), *Reduce.scratch(tok, width),
                            pltpu.VMEM((tok, width), BF16), *weights_v, w_sems, *dma_sems(count)],
            compiler_params=remote_params(0), name="first",
        )(x_in, dy_out, meta, w1_a, w3_a, w2_a)

        def backward(x_all, d_all, s, g, rel, w1, w3, w2):
            whole = pl.BlockSpec(memory_space=pltpu.VMEM)
            w_in = pl.BlockSpec((1, width, inner), lambda e: (e, 0, 0))
            w_out = pl.BlockSpec((1, inner, width), lambda e: (e, 0, 0))
            return pl.pallas_call(
                functools.partial(backward_kernel, dims),
                grid=(local,),
                out_shape=(sds((local, width, inner), F32), sds((local, width, inner), F32),
                           sds((local, inner, width), F32), part_all, dg_all),
                in_specs=[whole] * 5 + [w_in, w_in, w_out],
                out_specs=[w_in, w_in, w_out, whole, whole],
                scratch_shapes=[expert_v, expert_v, expert_v, pltpu.VMEM((local, n_dev, LANES), F32)],
                compiler_params=pltpu.CompilerParams(dimension_semantics=("arbitrary",), vmem_limit_bytes=VMEM_LIMIT),
                name="backward",
            )(x_all, d_all, s, g, rel, w1, w3, w2)

        *grads_b, part_b, dg_b = backward(mid_all, dy_all, sb, gb, relb, w1_b, w3_b, w2_b)

        count = 2 * Gather.COPIES + 2 * Reduce.COPIES
        dmid_all, x_again, dmid_own, dgate_b, part_x = pl.pallas_call(
            functools.partial(middle_kernel, dims),
            out_shape=(rows_all, rows_all, own, sds((top_k, LANES), F32), part_all),
            in_specs=[VMEM] * 7 + [ANY] * 3,
            out_specs=[VMEM] * 5,
            scratch_shapes=[rows_v, rows_v, expert_v, expert_v, *Reduce.scratch(tok, width),
                            *Reduce.scratch(top_k, LANES), pltpu.VMEM((tok, width), BF16), *weights_v, w_sems,
                            *dma_sems(count)],
            compiler_params=remote_params(1), name="middle",
        )(part_b, dg_b, dy_out, x_in, mid_all, sb, gb, w1_b, w3_b, w2_b)

        *grads_a, part_a, dg_a = backward(x_again, dmid_all, sa, ga, rela, w1_a, w3_a, w2_a)

        count = 3 * Reduce.COPIES
        dx_in, dgate_a, x_out = pl.pallas_call(
            functools.partial(last_kernel, dims),
            out_shape=(own, sds((top_k, LANES), F32), own),
            in_specs=[VMEM] * 5,
            out_specs=[VMEM] * 3,
            scratch_shapes=[*Reduce.scratch(tok, width), *Reduce.scratch(top_k, LANES), *Reduce.scratch(tok, width),
                            *dma_sems(count)],
            compiler_params=remote_params(2), name="last",
        )(part_a, dg_a, part_x, dmid_own, mid_own)
        return (x_out, dx_in, *grads_a, *grads_b, dgate_a[:, :tok].T, dgate_b[:, :tok].T)

    return jax.shard_map(device_program, mesh=mesh, in_specs=(tok_spec,) * 6 + (w_spec,) * 6, out_specs=(tok_spec,) * 10, check_vma=False)
```

```python
import functools

import jax
import jax.numpy as jnp
from jax import lax
from jax.experimental import pallas as pl
from jax.experimental.pallas import tpu as pltpu
from jax.sharding import PartitionSpec as P

BF16 = jnp.bfloat16
F32 = jnp.float32
MESH = pl.DeviceIdType.MESH
LANES = 128
CAP_FACTOR = 4
BF16_MAX = 3.3895313892515355e38
GROUPED = 2
VMEM_LIMIT = 60 * 1024 * 1024
VMEM = pl.BlockSpec(memory_space=pltpu.VMEM)
ANY = pl.BlockSpec(memory_space=pl.ANY)


def mm(lhs, rhs):
    return jnp.dot(lhs, rhs, preferred_element_type=F32)


def mm_tn(lhs, rhs):
    return lax.dot_general(lhs, rhs, (((0,), (0,)), ((), ())), preferred_element_type=F32)


def mm_nt(lhs, rhs):
    return lax.dot_general(lhs, rhs, (((1,), (1,)), ((), ())), preferred_element_type=F32)


def iota(shape, dim):
    return lax.broadcasted_iota(jnp.int32, shape, dim)


def routing_maps(me, meta, layer, s_ref, g_ref, rel_ref, top_k, local):
    n_dev = meta.shape[0]
    base = (me * local).astype(F32)
    row = 2 * layer * top_k
    rel_ref[...] = meta[:, row : row + top_k, :] - base
    hit = [jnp.zeros((n_dev, LANES), F32) for _ in range(local)]
    gate = [jnp.zeros((n_dev, LANES), F32) for _ in range(local)]
    for j in range(top_k):
        rel_j = meta[:, row + j, :] - base
        gate_j = meta[:, row + top_k + j, :]
        for e in range(local):
            match = rel_j == float(e)
            hit[e] = jnp.where(match, 1.0, hit[e])
            gate[e] = jnp.where(match, gate_j, gate[e])
    hit = jnp.concatenate(hit, axis=0)
    earlier = (iota((LANES, LANES), 0) < iota((LANES, LANES), 1)).astype(F32).astype(BF16)
    slot = jnp.where(hit > 0.0, mm(hit.astype(BF16), earlier), -1.0)
    s_ref[...] = slot.reshape(local, n_dev, LANES)
    for e in range(local):
        g_ref[e] = gate[e]


def row_picks(s_map, d, tok, n_dev, cap):
    pairs, lanes = s_map.shape
    n_rows = pairs // n_dev * cap
    spread = iota((n_rows, pairs), 1) == iota((n_rows, pairs), 0) // cap * n_dev + d
    slot = mm(spread.astype(F32).astype(BF16), s_map.astype(BF16))
    return jnp.where(slot == (iota((n_rows, lanes), 0) % cap).astype(F32), 1.0, 0.0).astype(BF16)[:, :tok]


def fill_rows(s_map, d, sources, cap):
    picks = row_picks(s_map, d, sources[0][0].shape[1], sources[0][0].shape[0], cap)
    for rows, out in sources:
        out[d] = mm(picks, rows[d]).astype(BF16).reshape(out.shape[1:])


def limbs(gate):
    hi = jnp.minimum(gate, BF16_MAX).astype(BF16)
    rest = gate - hi.astype(F32)
    mid = rest.astype(BF16)
    return hi, mid, (rest - mid.astype(F32)).astype(BF16)


def scatter_lhs(s_map, g_map, tok):
    stack = [s_map.T[:tok].astype(BF16)]
    if g_map is not None:
        stack += [limb.T[:tok].astype(BF16) for limb in (x.astype(F32) for x in limbs(g_map))]
    return jnp.concatenate(stack, axis=0)


def token_sums(stack, d, out_rows, tok, cap):
    pairs = stack.shape[1]
    n_rows = out_rows.shape[0]
    spread = iota((pairs, n_rows), 0) == iota((pairs, n_rows), 1) // cap * 8 + d
    maps = mm(stack, spread.astype(F32).astype(BF16))
    match = maps[:tok] == (iota((tok, n_rows), 1) % cap).astype(F32)
    if stack.shape[0] == tok:
        return mm(jnp.where(match, 1.0, 0.0).astype(BF16), out_rows)
    terms = (stack.shape[0] - tok) // tok
    lhs = [jnp.where(match, maps[(i + 1) * tok : (i + 2) * tok], 0.0).astype(BF16) for i in range(terms)]
    sums = mm(jnp.concatenate(lhs, axis=0), out_rows)
    total = sums[:tok]
    for i in range(1, terms):
        total = total + sums[i * tok : (i + 1) * tok]
    return total


class Links:
    def __init__(self, n_dev, send_sems, recv_sems):
        me = lax.axis_index("ep")
        self.n = n_dev
        self.me = me
        self.core = lax.rem(me, 2)
        self.partner = me + 1 - 2 * self.core
        self.right = lax.rem(me + 2, n_dev)
        self.left = lax.rem(me + n_dev - 2, n_dev)
        self.opp = lax.rem(me + 4, n_dev)
        self.send_sems, self.recv_sems = send_sems, recv_sems
        self.used = 0
        self.started = []

    def greet(self):
        barrier = pltpu.get_barrier_semaphore()
        for peer in (self.partner, self.left, self.right):
            pl.semaphore_signal(barrier, inc=1, device_id={"ep": peer}, device_id_type=MESH)
        pl.semaphore_wait(barrier, 3)

    def copy(self, src, dst, peer):
        slot = self.used
        self.used += 1
        rdma = pltpu.make_async_remote_copy(
            src_ref=src, dst_ref=dst, send_sem=self.send_sems.at[slot], recv_sem=self.recv_sems.at[slot],
            device_id={"ep": peer}, device_id_type=MESH)
        rdma.start()
        self.started.append(rdma)
        return rdma

    def drain(self):
        for rdma in self.started:
            rdma.wait_send()


class Gather:
    COPIES = 9

    def __init__(self, links, own, full):
        k, self.k, self.full = links, links, full
        self.half = own.shape[0] // 2
        self.to_right = k.copy(own, full.at[k.me], k.right)
        self.to_left = k.copy(own, full.at[k.me], k.left)
        self.to_partner = k.copy(own, full.at[k.me], k.partner)

    def pass_on(self):
        k, full, half = self.k, self.full, self.half
        self.to_right.wait_recv()
        self.far_a = k.copy(full.at[k.left, pl.ds(0, half)], full.at[k.left, pl.ds(0, half)], k.right)
        self.side_a = k.copy(full.at[k.left], full.at[k.left], k.partner)
        self.to_left.wait_recv()
        self.far_b = k.copy(full.at[k.right, pl.ds(half, half)], full.at[k.right, pl.ds(half, half)], k.left)
        self.side_b = k.copy(full.at[k.right], full.at[k.right], k.partner)

    def pass_far(self):
        k, full, half = self.k, self.full, self.half
        self.far_a.wait_recv()
        self.last_a = k.copy(full.at[k.opp, pl.ds(0, half)], full.at[k.opp, pl.ds(0, half)], k.partner)
        self.far_b.wait_recv()
        self.last_b = k.copy(full.at[k.opp, pl.ds(half, half)], full.at[k.opp, pl.ds(half, half)], k.partner)

    def wait_partner(self):
        self.to_partner.wait_recv()

    def wait_sides(self):
        self.side_a.wait_recv()
        self.side_b.wait_recv()

    def wait_last(self):
        self.last_a.wait_recv()
        self.last_b.wait_recv()

    def finish(self):
        self.wait_partner()
        self.wait_sides()
        self.wait_last()


class Reduce:
    COPIES = 10

    @staticmethod
    def scratch(rows, width):
        return [pltpu.VMEM((4, rows, width), F32), pltpu.VMEM((4, rows, width), F32), pltpu.VMEM((3, rows, width), F32)]

    def __init__(self, links, part, bufs, split=True):
        self.k, self.part = links, part
        self.near, self.mine, self.got = bufs
        rows = part.shape[1]
        self.rows = rows
        self.half = rows // 2 if split else rows
        self.side = {}

    def block(self, hop, core):
        k = self.k
        return lax.rem(k.me - k.core + 2 * hop, k.n) + core

    def start_side(self, hop):
        k = self.k
        self.side[hop] = k.copy(self.part.at[self.block(hop, 1 - k.core)], self.near.at[hop], k.partner)

    def start(self):
        for hop in (2, 1, 3, 0):
            self.start_side(hop)

    def add(self, hop, lo, hi, extra=None):
        own = self.part[self.block(hop, self.k.core), lo:hi, :]
        total = own + self.near[hop, lo:hi, :]
        if extra is not None:
            total = total + extra
        self.mine[hop, lo:hi, :] = total

    def far(self):
        k, half, rows = self.k, self.half, self.rows
        self.side[2].wait_recv()
        self.add(2, 0, rows)
        a = pl.ds(0, half)
        self.far_a = k.copy(self.mine.at[2, a], self.got.at[2, a], k.right)
        if half < rows:
            b = pl.ds(half, rows - half)
            self.far_b = k.copy(self.mine.at[2, b], self.got.at[2, b], k.left)

    def near_sends(self):
        k, half, rows = self.k, self.half, self.rows
        self.side[1].wait_recv()
        if half < rows:
            b = pl.ds(half, rows - half)
            self.add(1, half, rows)
            self.right_b = k.copy(self.mine.at[1, b], self.got.at[0, b], k.right)
        self.side[3].wait_recv()
        self.add(3, 0, half)
        a = pl.ds(0, half)
        self.left_a = k.copy(self.mine.at[3, a], self.got.at[1, a], k.left)

    def relay(self):
        k, half, rows = self.k, self.half, self.rows
        a = pl.ds(0, half)
        self.far_a.wait_recv()
        self.add(1, 0, half, self.got[2, :half, :])
        self.right_a = k.copy(self.mine.at[1, a], self.got.at[0, a], k.right)
        if half < rows:
            b = pl.ds(half, rows - half)
            self.far_b.wait_recv()
            self.add(3, half, rows, self.got[2, half:, :])
            self.left_b = k.copy(self.mine.at[3, b], self.got.at[1, b], k.left)

    def result(self):
        half, rows = self.half, self.rows
        self.side[0].wait_recv()
        if half < rows:
            self.right_b.wait_recv()
        self.left_a.wait_recv()
        self.right_a.wait_recv()
        if half < rows:
            self.left_b.wait_recv()
        return self.part[self.k.me] + self.near[0] + self.got[0] + self.got[1]


def load_weights(pairs, sems, local):
    def start(e, carry):
        for i, (src, dst) in enumerate(pairs):
            pltpu.make_async_copy(src.at[e], dst.at[e], sems.at[i, e]).start()
        return carry
    lax.fori_loop(0, local, start, 0)


def wait_weights(pairs, sems, e):
    for i, (src, dst) in enumerate(pairs):
        pltpu.make_async_copy(src.at[e], dst.at[e], sems.at[i, e]).wait()


def forward_experts(pairs, sems, u_ref, o_ref, cap, first, last):
    n_dev, _, _, width = u_ref.shape

    def step(g, carry):
        experts = [g * GROUPED + i for i in range(GROUPED)]
        for e in experts:
            wait_weights(pairs, sems, e)
        w_gate, w_up, w_down = (dst for _, dst in pairs)
        rows = [u_ref[:, e].reshape(n_dev * cap, width) for e in experts]
        pre = [(mm(u, w_gate[e]), mm(u, w_up[e])) for u, e in zip(rows, experts)]
        hidden = [(gate * jax.nn.sigmoid(gate) * up).astype(BF16) for gate, up in pre]
        for h, e in zip(hidden, experts):
            o_ref[:, e] = mm(h, w_down[e]).astype(BF16).reshape(n_dev, cap, width)
        return carry
    lax.fori_loop(first // GROUPED, last // GROUPED, step, 0)


def first_kernel(dims, x_ref, dy_ref, idx_a, gate_a, idx_b, gate_b, w1, w3, w2,
                 mid_all, dy_all, mid_own, sa, ga, rela, sb, gb, relb,
                 x_all, y_all, m_all, meta_ref, meta_all, u_ref, o_ref, part, near, mine, got, mid_buf, w1_v, w3_v, w2_v,
                 w_sems, send_sems, recv_sems):
    n_dev, tok, width, local, cap, top_k = dims
    pairs = ((w1, w1_v), (w3, w3_v), (w2, w2_v))
    load_weights(pairs, w_sems, local)
    meta_ref[...] = jnp.full(meta_ref.shape, -1.0, F32)
    for i, ref in enumerate((idx_a, gate_a, idx_b, gate_b)):
        meta_ref[i * top_k : (i + 1) * top_k, :tok] = ref[...].astype(F32)
    links = Links(n_dev, send_sems, recv_sems)
    me = links.me
    links.greet()
    meta_g = Gather(links, meta_ref, meta_all)
    x_g = Gather(links, x_ref, x_all)
    y_g = Gather(links, dy_ref, y_all)
    meta_all[me] = meta_ref[...]
    x_all[me] = x_ref[...]
    y_all[me] = dy_ref[...]
    meta_g.pass_on()
    x_g.pass_on()
    meta_g.pass_far()
    x_g.pass_far()
    meta_g.finish()
    meta = meta_all[...]
    routing_maps(me, meta, 0, sa, ga, rela, top_k, local)
    routing_maps(me, meta, 1, sb, gb, relb, top_k, local)
    s_map = sa[...].reshape(local * n_dev, LANES)

    def rows_of(d):
        fill_rows(s_map, d, ((x_all, u_ref),), cap)

    rows_of(me)
    rows_of(links.left)
    rows_of(links.right)
    rows_of(links.opp)
    y_g.pass_on()
    x_g.wait_partner()
    rows_of(links.partner)
    x_g.wait_sides()
    side = 1 - 2 * links.core
    rows_of(links.left + side)
    rows_of(links.right + side)
    x_g.wait_last()
    rows_of(links.opp + side)
    forward_experts(pairs, w_sems, u_ref, o_ref, cap, 0, local)
    y_g.pass_far()
    stack = scatter_lhs(s_map, ga[...].reshape(local * n_dev, LANES), tok)
    red = Reduce(links, part, (near, mine, got))

    def sums_of(d):
        part[d] = token_sums(stack, d, o_ref[d].reshape(local * cap, width), tok, cap)

    for hop in (2, 1, 3, 0):
        sums_of(red.block(hop, 1 - links.core))
        red.start_side(hop)
    for hop in (2, 1, 3, 0):
        sums_of(red.block(hop, links.core))
    red.far()
    red.near_sends()
    red.relay()
    x_mid = (x_ref[...].astype(F32) + red.result()).astype(BF16)
    mid_buf[...] = x_mid
    mid_own[...] = x_mid
    m_all[me] = x_mid
    m_g = Gather(links, mid_buf, m_all)
    m_g.pass_on()
    m_g.pass_far()
    y_g.finish()
    dy_all[...] = y_all[...]
    m_g.finish()
    mid_all[...] = m_all[...]
    links.drain()


def backward_kernel(dims, x_all, dy_all, s_ref, g_ref, rel_ref, w1, w3, w2,
                    dw1, dw3, dw2, part, dgate,
                    u_ref, y_ref, du_ref, dg_ref, w1_v, w3_v, w2_v, dw1_v, dw3_v, dw2_v, w_sems, out_sems):
    n_dev, tok, width, local, cap, top_k = dims
    n_rows = n_dev * cap
    pairs = ((w1, w1_v), (w3, w3_v), (w2, w2_v))
    outs = ((dw1_v, dw1), (dw3_v, dw3), (dw2_v, dw2))
    load_weights(pairs, w_sems, local)
    s_map = s_ref[...].reshape(local * n_dev, LANES)

    def rows_of(d, carry):
        fill_rows(s_map, d, ((x_all, u_ref), (dy_all, y_ref)), cap)
        return carry
    lax.fori_loop(0, n_dev, rows_of, 0, unroll=2)

    def store(g, i, slot):
        src, dst = outs[i]
        return pltpu.make_async_copy(src.at[slot], dst.at[pl.ds(g * GROUPED, GROUPED)], out_sems.at[i, slot])

    def step(g, carry):
        slot = lax.rem(g, 2)
        experts = [g * GROUPED + i for i in range(GROUPED)]
        each = range(GROUPED)
        for e in experts:
            wait_weights(pairs, w_sems, e)

        @pl.when(g >= 2)
        def _():
            for i in range(3):
                store(g - 2, i, slot).wait()
        u = [u_ref[:, e].reshape(n_rows, width) for e in experts]
        dy = [y_ref[:, e].reshape(n_rows, width) for e in experts]
        holds = [s_ref[e][:, None, :] == iota((n_dev, cap, LANES), 1).astype(F32) for e in experts]
        gate_row = [jnp.sum(jnp.where(holds[i], g_ref[e][:, None, :], 0.0), axis=2, keepdims=True).reshape(n_rows, 1)
                    for i, e in enumerate(experts)]
        q = [(gate_row[i] * dy[i].astype(F32)).astype(BF16) for i in each]
        pre = [(mm(u[i], w1_v[e]), mm(u[i], w3_v[e])) for i, e in enumerate(experts)]
        d_hidden = [mm_nt(q[i], w2_v[e]) for i, e in enumerate(experts)]
        sig = [jax.nn.sigmoid(a) for a, _ in pre]
        act = [pre[i][0] * sig[i] for i in each]
        hidden = [(act[i] * pre[i][1]).astype(BF16) for i in each]
        out = [mm(hidden[i], w2_v[e]).astype(BF16) for i, e in enumerate(experts)]
        for i in each:
            dw2_v[slot, i] = mm_tn(hidden[i], q[i])
        d_gate = [(d_hidden[i] * pre[i][1] * sig[i] * (1.0 + pre[i][0] * (1.0 - sig[i]))).astype(BF16) for i in each]
        d_up = [(d_hidden[i] * act[i]).astype(BF16) for i in each]
        for i, e in enumerate(experts):
            dg_row = jnp.sum(dy[i].astype(F32) * out[i].astype(F32), axis=1, keepdims=True).reshape(n_dev, cap, 1)
            dg_ref[e] = jnp.sum(jnp.where(holds[i], dg_row, 0.0), axis=1)
        for i, e in enumerate(experts):
            du = (mm_nt(d_gate[i], w1_v[e]) + mm_nt(d_up[i], w3_v[e])).astype(BF16)
            du_ref[:, e] = du.reshape(n_dev, cap, width)
        for i in each:
            dw1_v[slot, i] = mm_tn(u[i], d_gate[i])
            dw3_v[slot, i] = mm_tn(u[i], d_up[i])
        for i in range(3):
            store(g, i, slot).start()
        return carry
    steps = local // GROUPED
    lax.fori_loop(0, steps, step, 0)

    stack = scatter_lhs(s_map, None, tok)

    def sums_of(d, carry):
        part[d] = token_sums(stack, d, du_ref[d].reshape(local * cap, width), tok, cap)
        return carry
    lax.fori_loop(0, n_dev, sums_of, 0, unroll=2)
    for d in range(n_dev):
        total = jnp.zeros((top_k, LANES), F32)
        for i in range(local):
            total = jnp.where(rel_ref[d] == float(i), dg_ref[i, d : d + 1, :], total)
        dgate[d] = total
    for g in (steps - 2, steps - 1):
        for i in range(3):
            store(g, i, g % 2).wait()


def middle_kernel(dims, part_b, dg_part, dy_ref, x_ref, mid_all, sb, gb, w1, w3, w2,
                  dmid_all, x_again, dmid_own, dgate, part_x,
                  d_all, x_all, u_ref, o_ref, near, mine, got, dg_near, dg_mine, dg_got, d_buf, w1_v, w3_v, w2_v,
                  w_sems, send_sems, recv_sems):
    n_dev, tok, width, local, cap, top_k = dims
    pairs = ((w1, w1_v), (w3, w3_v), (w2, w2_v))
    load_weights(pairs, w_sems, local)
    links = Links(n_dev, send_sems, recv_sems)
    me = links.me
    links.greet()
    red = Reduce(links, part_b, (near, mine, got))
    dg = Reduce(links, dg_part, (dg_near, dg_mine, dg_got), split=False)
    s_map = sb[...].reshape(local * n_dev, LANES)

    def rows_of(d, carry):
        fill_rows(s_map, d, ((mid_all, u_ref),), cap)
        return carry

    def sums_of(d, carry):
        part_x[d] = token_sums(stack, d, o_ref[d].reshape(local * cap, width), tok, cap)
        return carry

    red.start()
    dg.start()
    x_g = Gather(links, x_ref, x_all)
    x_all[me] = x_ref[...]
    lax.fori_loop(0, 2, rows_of, 0, unroll=2)
    red.far()
    red.near_sends()
    dg.far()
    dg.near_sends()
    lax.fori_loop(2, n_dev, rows_of, 0, unroll=2)
    x_g.pass_on()
    red.relay()
    dg.relay()
    half = local // 2 // GROUPED * GROUPED
    forward_experts(pairs, w_sems, u_ref, o_ref, cap, 0, half)
    x_g.pass_far()
    dx = (dy_ref[...].astype(F32) + red.result()).astype(BF16)
    d_buf[...] = dx
    dmid_own[...] = dx
    d_all[me] = dx
    d_g = Gather(links, d_buf, d_all)
    forward_experts(pairs, w_sems, u_ref, o_ref, cap, half, local)
    d_g.pass_on()
    stack = scatter_lhs(s_map, gb[...].reshape(local * n_dev, LANES), tok)
    lax.fori_loop(0, n_dev, sums_of, 0, unroll=2)
    d_g.pass_far()
    dgate[...] = dg.result()
    x_g.finish()
    x_again[...] = x_all[...]
    d_g.finish()
    dmid_all[...] = d_all[...]
    links.drain()


def final_kernel(x_ref, dx_ref, dga_ref, dgb_ref, x_out, dx_out, dga_out, dgb_out):
    x_out[...] = x_ref[...]
    dx_out[...] = dx_ref[...]
    tok = dga_out.shape[1]
    dga_out[...] = dga_ref[:, :tok]
    dgb_out[...] = dgb_ref[:, :tok]


def last_kernel(dims, part_a, dg_part, part_x, dmid_ref, mid_ref, dx_out, dgate, x_out,
                near, mine, got, dg_near, dg_mine, dg_got, x_near, x_mine, x_got, send_sems, recv_sems):
    links = Links(dims[0], send_sems, recv_sems)
    links.greet()
    reds = (Reduce(links, part_a, (near, mine, got)), Reduce(links, part_x, (x_near, x_mine, x_got)),
            Reduce(links, dg_part, (dg_near, dg_mine, dg_got), split=False))
    for red in reds:
        red.start()
    for red in reds:
        red.far()
        red.near_sends()
    for red in reds:
        red.relay()
    dx_out[...] = (dmid_ref[...].astype(F32) + reds[0].result()).astype(BF16)
    x_out[...] = (mid_ref[...].astype(F32) + reds[1].result()).astype(BF16)
    dgate[...] = reds[2].result()
    links.drain()


def remote_params(ident):
    return pltpu.CompilerParams(collective_id=ident, has_side_effects=True, vmem_limit_bytes=VMEM_LIMIT)


def dma_sems(count):
    return [pltpu.SemaphoreType.DMA((count,)), pltpu.SemaphoreType.DMA((count,))]


def solution(mesh):
    n_dev = mesh.shape["ep"]
    tok_spec = P(("dp", "ep"))
    w_spec = P("ep")

    def device_program(x_in, idx_a, idx_b, gate_a, gate_b, dy_out, w1_a, w3_a, w2_a, w1_b, w3_b, w2_b):
        tok, top_k = idx_a.shape
        width = x_in.shape[1]
        local, _, inner = w1_a.shape
        cap = CAP_FACTOR * tok * top_k // (local * n_dev)
        dims = (n_dev, tok, width, local, cap, top_k)
        sds = jax.ShapeDtypeStruct
        rows_all = sds((n_dev, tok, width), BF16)
        part_all = sds((n_dev, tok, width), F32)
        dg_all = sds((n_dev, top_k, LANES), F32)
        map_s = sds((local, n_dev, LANES), F32)
        own = sds((tok, width), BF16)

        weights_v = [pltpu.VMEM((local, width, inner), BF16)] * 2 + [pltpu.VMEM((local, inner, width), BF16)]
        w_sems = pltpu.SemaphoreType.DMA((3, local))
        rows_v = pltpu.VMEM((n_dev, tok, width), BF16)
        expert_v = pltpu.VMEM((n_dev, local, cap, width), BF16)

        count = 4 * Gather.COPIES + Reduce.COPIES
        mid_all, dy_all, mid_own, sa, ga, rela, sb, gb, relb = pl.pallas_call(
            functools.partial(first_kernel, dims),
            out_shape=(rows_all, rows_all, own, map_s, map_s, dg_all, map_s, map_s, dg_all),
            in_specs=[VMEM] * 6 + [ANY] * 3,
            out_specs=[VMEM] * 9,
            scratch_shapes=[rows_v, rows_v, rows_v, pltpu.VMEM((4 * top_k, LANES), F32), pltpu.VMEM((n_dev, 4 * top_k, LANES), F32), expert_v, expert_v,
                            pltpu.VMEM((n_dev, tok, width), F32), *Reduce.scratch(tok, width),
                            pltpu.VMEM((tok, width), BF16), *weights_v, w_sems, *dma_sems(count)],
            compiler_params=remote_params(0), name="first",
        )(x_in, dy_out, idx_a.T, gate_a.T, idx_b.T, gate_b.T, w1_a, w3_a, w2_a)

        def backward(x_all, d_all, s, g, rel, w1, w3, w2):
            return pl.pallas_call(
                functools.partial(backward_kernel, dims),
                out_shape=(sds((local, width, inner), F32), sds((local, width, inner), F32),
                           sds((local, inner, width), F32), part_all, dg_all),
                in_specs=[VMEM] * 5 + [ANY] * 3,
                out_specs=[ANY] * 3 + [VMEM] * 2,
                scratch_shapes=[expert_v, expert_v, expert_v, pltpu.VMEM((local, n_dev, LANES), F32), *weights_v,
                                *[pltpu.VMEM((2, GROUPED, width, inner), F32)] * 2,
                                pltpu.VMEM((2, GROUPED, inner, width), F32), w_sems, pltpu.SemaphoreType.DMA((3, 2))],
                compiler_params=pltpu.CompilerParams(vmem_limit_bytes=VMEM_LIMIT), name="backward",
            )(x_all, d_all, s, g, rel, w1, w3, w2)

        *grads_b, part_b, dg_b = backward(mid_all, dy_all, sb, gb, relb, w1_b, w3_b, w2_b)

        count = 2 * Gather.COPIES + 2 * Reduce.COPIES
        dmid_all, x_again, dmid_own, dgate_b, part_x = pl.pallas_call(
            functools.partial(middle_kernel, dims),
            out_shape=(rows_all, rows_all, own, sds((top_k, LANES), F32), part_all),
            in_specs=[VMEM] * 7 + [ANY] * 3,
            out_specs=[VMEM] * 5,
            scratch_shapes=[rows_v, rows_v, expert_v, expert_v, *Reduce.scratch(tok, width),
                            *Reduce.scratch(top_k, LANES), pltpu.VMEM((tok, width), BF16), *weights_v, w_sems,
                            *dma_sems(count)],
            compiler_params=remote_params(1), name="middle",
        )(part_b, dg_b, dy_out, x_in, mid_all, sb, gb, w1_b, w3_b, w2_b)

        *grads_a, part_a, dg_a = backward(x_again, dmid_all, sa, ga, rela, w1_a, w3_a, w2_a)

        count = 3 * Reduce.COPIES
        dx_in, dgate_a, x_out = pl.pallas_call(
            functools.partial(last_kernel, dims),
            out_shape=(own, sds((top_k, LANES), F32), own),
            in_specs=[VMEM] * 5,
            out_specs=[VMEM] * 3,
            scratch_shapes=[*Reduce.scratch(tok, width), *Reduce.scratch(top_k, LANES), *Reduce.scratch(tok, width),
                            *dma_sems(count)],
            compiler_params=remote_params(2), name="last",
        )(part_a, dg_a, part_x, dmid_own, mid_own)
        gates = sds((top_k, tok), F32)
        x_out, dx_in, dgate_a, dgate_b = pl.pallas_call(
            final_kernel, out_shape=(own, own, gates, gates), in_specs=[VMEM] * 4, out_specs=[VMEM] * 4, name="final",
        )(x_out, dx_in, dgate_a, dgate_b)
        return (x_out, dx_in, *grads_a, *grads_b, dgate_a.T, dgate_b.T)

    return jax.shard_map(device_program, mesh=mesh, in_specs=(tok_spec,) * 6 + (w_spec,) * 6, out_specs=(tok_spec,) * 10, check_vma=False)
```

```python
import functools

import jax
import jax.numpy as jnp
from jax import lax
from jax.experimental import pallas as pl
from jax.experimental.pallas import tpu as pltpu
from jax.sharding import PartitionSpec as P

BF16 = jnp.bfloat16
F32 = jnp.float32
MESH = pl.DeviceIdType.MESH
LANES = 128
CAP_FACTOR = 4
BF16_MAX = 3.3895313892515355e38
GROUPED = 2
FORWARD_GROUPED = 4
VMEM_LIMIT = 60 * 1024 * 1024
VMEM = pl.BlockSpec(memory_space=pltpu.VMEM)
ANY = pl.BlockSpec(memory_space=pl.ANY)


def mm(lhs, rhs):
    return jnp.dot(lhs, rhs, preferred_element_type=F32)


def mm_tn(lhs, rhs):
    return lax.dot_general(lhs, rhs, (((0,), (0,)), ((), ())), preferred_element_type=F32)


def mm_nt(lhs, rhs):
    return lax.dot_general(lhs, rhs, (((1,), (1,)), ((), ())), preferred_element_type=F32)


def iota(shape, dim):
    return lax.broadcasted_iota(jnp.int32, shape, dim)


def routing_maps(me, meta, layer, s_ref, g_ref, rel_ref, top_k, local):
    n_dev = meta.shape[0]
    base = (me * local).astype(F32)
    row = 2 * layer * top_k
    rel_ref[...] = meta[:, row : row + top_k, :] - base
    shape = (local, n_dev, LANES)
    expert = iota(shape, 0).astype(F32)
    hit, gate = jnp.zeros(shape, F32), jnp.zeros(shape, F32)
    for j in range(top_k):
        match = (meta[:, row + j, :] - base)[None] == expert
        hit = jnp.where(match, 1.0, hit)
        gate = jnp.where(match, meta[:, row + top_k + j, :][None], gate)
    hit = hit.reshape(local * n_dev, LANES)
    earlier = (iota((LANES, LANES), 0) < iota((LANES, LANES), 1)).astype(F32).astype(BF16)
    slot = jnp.where(hit > 0.0, mm(hit.astype(BF16), earlier), -1.0)
    s_ref[...] = slot.reshape(shape)
    g_ref[...] = gate


def row_picks(s_map, d, tok, n_dev, cap):
    pairs, lanes = s_map.shape
    n_rows = pairs // n_dev * cap
    spread = iota((n_rows, pairs), 1) == iota((n_rows, pairs), 0) // cap * n_dev + d
    slot = mm(spread.astype(F32).astype(BF16), s_map.astype(BF16))
    return jnp.where(slot == (iota((n_rows, lanes), 0) % cap).astype(F32), 1.0, 0.0).astype(BF16)[:, :tok]


def fill_rows(s_map, d, sources, cap):
    picks = row_picks(s_map, d, sources[0][0].shape[1], sources[0][0].shape[0], cap)
    for rows, out in sources:
        out[d] = mm(picks, rows[d]).astype(BF16).reshape(out.shape[1:])


def limbs(gate):
    hi = jnp.minimum(gate, BF16_MAX).astype(BF16)
    rest = gate - hi.astype(F32)
    mid = rest.astype(BF16)
    return hi, mid, (rest - mid.astype(F32)).astype(BF16)


def scatter_lhs(s_map, g_map, tok):
    stack = [s_map.T[:tok].astype(BF16)]
    if g_map is not None:
        stack += [limb.T[:tok].astype(BF16) for limb in (x.astype(F32) for x in limbs(g_map))]
    return jnp.concatenate(stack, axis=0)


def token_sums(stack, d, out_rows, tok, cap):
    pairs = stack.shape[1]
    n_rows = out_rows.shape[0]
    spread = iota((pairs, n_rows), 0) == iota((pairs, n_rows), 1) // cap * 8 + d
    maps = mm(stack, spread.astype(F32).astype(BF16))
    match = maps[:tok] == (iota((tok, n_rows), 1) % cap).astype(F32)
    if stack.shape[0] == tok:
        return mm(jnp.where(match, 1.0, 0.0).astype(BF16), out_rows)
    terms = (stack.shape[0] - tok) // tok
    lhs = [jnp.where(match, maps[(i + 1) * tok : (i + 2) * tok], 0.0).astype(BF16) for i in range(terms)]
    sums = mm(jnp.concatenate(lhs, axis=0), out_rows)
    total = sums[:tok]
    for i in range(1, terms):
        total = total + sums[i * tok : (i + 1) * tok]
    return total


class Links:
    def __init__(self, n_dev, send_sems, recv_sems):
        me = lax.axis_index("ep")
        self.n = n_dev
        self.me = me
        self.core = lax.rem(me, 2)
        self.partner = me + 1 - 2 * self.core
        self.right = lax.rem(me + 2, n_dev)
        self.left = lax.rem(me + n_dev - 2, n_dev)
        self.opp = lax.rem(me + 4, n_dev)
        self.send_sems, self.recv_sems = send_sems, recv_sems
        self.used = 0
        self.started = []

    def greet(self):
        barrier = pltpu.get_barrier_semaphore()
        for peer in (self.partner, self.left, self.right):
            pl.semaphore_signal(barrier, inc=1, device_id={"ep": peer}, device_id_type=MESH)
        pl.semaphore_wait(barrier, 3)

    def copy(self, src, dst, peer):
        slot = self.used
        self.used += 1
        rdma = pltpu.make_async_remote_copy(
            src_ref=src, dst_ref=dst, send_sem=self.send_sems.at[slot], recv_sem=self.recv_sems.at[slot],
            device_id={"ep": peer}, device_id_type=MESH)
        rdma.start()
        self.started.append(rdma)
        return rdma

    def drain(self):
        for rdma in self.started:
            rdma.wait_send()


class Gather:
    COPIES = 9

    def __init__(self, links, own, full):
        k, self.k, self.full = links, links, full
        self.half = own.shape[0] // 2
        self.to_right = k.copy(own, full.at[k.me], k.right)
        self.to_left = k.copy(own, full.at[k.me], k.left)
        self.to_partner = k.copy(own, full.at[k.me], k.partner)

    def pass_on(self):
        k, full, half = self.k, self.full, self.half
        self.to_right.wait_recv()
        self.far_a = k.copy(full.at[k.left, pl.ds(0, half)], full.at[k.left, pl.ds(0, half)], k.right)
        self.side_a = k.copy(full.at[k.left], full.at[k.left], k.partner)
        self.to_left.wait_recv()
        self.far_b = k.copy(full.at[k.right, pl.ds(half, half)], full.at[k.right, pl.ds(half, half)], k.left)
        self.side_b = k.copy(full.at[k.right], full.at[k.right], k.partner)

    def pass_far(self):
        k, full, half = self.k, self.full, self.half
        self.far_a.wait_recv()
        self.last_a = k.copy(full.at[k.opp, pl.ds(0, half)], full.at[k.opp, pl.ds(0, half)], k.partner)
        self.far_b.wait_recv()
        self.last_b = k.copy(full.at[k.opp, pl.ds(half, half)], full.at[k.opp, pl.ds(half, half)], k.partner)

    def wait_partner(self):
        self.to_partner.wait_recv()

    def wait_sides(self):
        self.side_a.wait_recv()
        self.side_b.wait_recv()

    def wait_last(self):
        self.last_a.wait_recv()
        self.last_b.wait_recv()

    def finish(self):
        self.wait_partner()
        self.wait_sides()
        self.wait_last()


class Reduce:
    COPIES = 10

    @staticmethod
    def scratch(rows, width):
        return [pltpu.VMEM((4, rows, width), F32), pltpu.VMEM((4, rows, width), F32), pltpu.VMEM((3, rows, width), F32)]

    def __init__(self, links, part, bufs, split=True):
        self.k, self.part = links, part
        self.near, self.mine, self.got = bufs
        rows = part.shape[1]
        self.rows = rows
        self.half = rows // 2 if split else rows
        self.side = {}

    def block(self, hop, core):
        k = self.k
        return lax.rem(k.me - k.core + 2 * hop, k.n) + core

    def start_side(self, hop):
        k = self.k
        self.side[hop] = k.copy(self.part.at[self.block(hop, 1 - k.core)], self.near.at[hop], k.partner)

    def start(self):
        for hop in (2, 1, 3, 0):
            self.start_side(hop)

    def add(self, hop, lo, hi, extra=None):
        own = self.part[self.block(hop, self.k.core), lo:hi, :]
        total = own + self.near[hop, lo:hi, :]
        if extra is not None:
            total = total + extra
        self.mine[hop, lo:hi, :] = total

    def far(self):
        k, half, rows = self.k, self.half, self.rows
        self.side[2].wait_recv()
        self.add(2, 0, rows)
        a = pl.ds(0, half)
        self.far_a = k.copy(self.mine.at[2, a], self.got.at[2, a], k.right)
        if half < rows:
            b = pl.ds(half, rows - half)
            self.far_b = k.copy(self.mine.at[2, b], self.got.at[2, b], k.left)

    def near_sends(self):
        k, half, rows = self.k, self.half, self.rows
        self.side[1].wait_recv()
        if half < rows:
            b = pl.ds(half, rows - half)
            self.add(1, half, rows)
            self.right_b = k.copy(self.mine.at[1, b], self.got.at[0, b], k.right)
        self.side[3].wait_recv()
        self.add(3, 0, half)
        a = pl.ds(0, half)
        self.left_a = k.copy(self.mine.at[3, a], self.got.at[1, a], k.left)

    def relay(self):
        k, half, rows = self.k, self.half, self.rows
        a = pl.ds(0, half)
        self.far_a.wait_recv()
        self.add(1, 0, half, self.got[2, :half, :])
        self.right_a = k.copy(self.mine.at[1, a], self.got.at[0, a], k.right)
        if half < rows:
            b = pl.ds(half, rows - half)
            self.far_b.wait_recv()
            self.add(3, half, rows, self.got[2, half:, :])
            self.left_b = k.copy(self.mine.at[3, b], self.got.at[1, b], k.left)

    def result(self):
        half, rows = self.half, self.rows
        self.side[0].wait_recv()
        if half < rows:
            self.right_b.wait_recv()
        self.left_a.wait_recv()
        self.right_a.wait_recv()
        if half < rows:
            self.left_b.wait_recv()
        return self.part[self.k.me] + self.near[0] + self.got[0] + self.got[1]


def load_weights(pairs, sems, local):
    def start(e, carry):
        for i, (src, dst) in enumerate(pairs):
            pltpu.make_async_copy(src.at[e], dst.at[e], sems.at[i, e]).start()
        return carry
    lax.fori_loop(0, local, start, 0)


def wait_weights(pairs, sems, e):
    for i, (src, dst) in enumerate(pairs):
        pltpu.make_async_copy(src.at[e], dst.at[e], sems.at[i, e]).wait()


def forward_experts(pairs, sems, u_ref, o_ref, cap, first, last):
    n_dev, _, _, width = u_ref.shape
    few = min(FORWARD_GROUPED, last - first)

    def step(g, carry):
        experts = [first + g * few + i for i in range(few)]
        for e in experts:
            wait_weights(pairs, sems, e)
        w_gate, w_up, w_down = (dst for _, dst in pairs)
        rows = [u_ref[:, e].reshape(n_dev * cap, width) for e in experts]
        pre = [(mm(u, w_gate[e]), mm(u, w_up[e])) for u, e in zip(rows, experts)]
        hidden = [(gate * jax.nn.sigmoid(gate) * up).astype(BF16) for gate, up in pre]
        for h, e in zip(hidden, experts):
            o_ref[:, e] = mm(h, w_down[e]).astype(BF16).reshape(n_dev, cap, width)
        return carry
    lax.fori_loop(0, (last - first) // few, step, 0)


def first_kernel(dims, x_ref, dy_ref, idx_a, gate_a, idx_b, gate_b, w1, w3, w2,
                 mid_all, dy_all, mid_own, sa, ga, rela, sb, gb, relb,
                 x_all, y_all, m_all, meta_ref, meta_all, u_ref, o_ref, part, near, mine, got, mid_buf, w1_v, w3_v, w2_v,
                 w_sems, send_sems, recv_sems):
    n_dev, tok, width, local, cap, top_k = dims
    pairs = ((w1, w1_v), (w3, w3_v), (w2, w2_v))
    load_weights(pairs, w_sems, local)
    meta_ref[...] = jnp.full(meta_ref.shape, -1.0, F32)
    for i, ref in enumerate((idx_a, gate_a, idx_b, gate_b)):
        meta_ref[i * top_k : (i + 1) * top_k, :tok] = ref[...].astype(F32)
    links = Links(n_dev, send_sems, recv_sems)
    me = links.me
    links.greet()
    meta_g = Gather(links, meta_ref, meta_all)
    x_g = Gather(links, x_ref, x_all)
    meta_all[me] = meta_ref[...]
    x_all[me] = x_ref[...]
    y_all[me] = dy_ref[...]
    meta_g.pass_on()
    x_g.pass_on()
    y_g = Gather(links, dy_ref, y_all)
    meta_g.pass_far()
    meta_g.finish()
    meta = meta_all[...]
    routing_maps(me, meta, 0, sa, ga, rela, top_k, local)
    routing_maps(me, meta, 1, sb, gb, relb, top_k, local)
    s_map = sa[...].reshape(local * n_dev, LANES)

    def rows_of(d):
        fill_rows(s_map, d, ((x_all, u_ref),), cap)

    rows_of(me)
    rows_of(links.left)
    rows_of(links.right)
    x_g.wait_partner()
    rows_of(links.partner)
    x_g.pass_far()
    x_g.wait_sides()
    side = 1 - 2 * links.core
    rows_of(links.left + side)
    rows_of(links.right + side)
    rows_of(links.opp)
    y_g.pass_on()
    x_g.wait_last()
    rows_of(links.opp + side)
    forward_experts(pairs, w_sems, u_ref, o_ref, cap, 0, local)
    y_g.pass_far()
    stack = scatter_lhs(s_map, ga[...].reshape(local * n_dev, LANES), tok)
    red = Reduce(links, part, (near, mine, got))

    def sums_of(d):
        part[d] = token_sums(stack, d, o_ref[d].reshape(local * cap, width), tok, cap)

    for hop in (2, 1, 3, 0):
        sums_of(red.block(hop, 1 - links.core))
        red.start_side(hop)
    for hop in (2, 1, 3, 0):
        sums_of(red.block(hop, links.core))
    red.far()
    red.near_sends()
    red.relay()
    x_mid = (x_ref[...].astype(F32) + red.result()).astype(BF16)
    mid_buf[...] = x_mid
    mid_own[...] = x_mid
    m_all[me] = x_mid
    m_g = Gather(links, mid_buf, m_all)
    m_g.pass_on()
    m_g.pass_far()
    y_g.finish()
    dy_all[...] = y_all[...]
    m_g.finish()
    mid_all[...] = m_all[...]
    links.drain()


def backward_kernel(dims, x_all, dy_all, s_ref, g_ref, rel_ref, w1, w3, w2,
                    dw1, dw3, dw2, part, dgate,
                    u_ref, y_ref, du_ref, dg_ref, w1_v, w3_v, w2_v, dw1_v, dw3_v, dw2_v, w_sems, out_sems):
    n_dev, tok, width, local, cap, top_k = dims
    n_rows = n_dev * cap
    pairs = ((w1, w1_v), (w3, w3_v), (w2, w2_v))
    outs = ((dw1_v, dw1), (dw3_v, dw3), (dw2_v, dw2))
    load_weights(pairs, w_sems, local)
    s_map = s_ref[...].reshape(local * n_dev, LANES)

    for d in range(n_dev):
        fill_rows(s_map, d, ((x_all, u_ref), (dy_all, y_ref)), cap)

    def store(g, i, slot):
        src, dst = outs[i]
        return pltpu.make_async_copy(src.at[slot], dst.at[pl.ds(g * GROUPED, GROUPED)], out_sems.at[i, slot])

    def step(g, carry):
        slot = lax.rem(g, 2)
        experts = [g * GROUPED + i for i in range(GROUPED)]
        each = range(GROUPED)
        for e in experts:
            wait_weights(pairs, w_sems, e)

        @pl.when(g >= 2)
        def _():
            for i in range(3):
                store(g - 2, i, slot).wait()
        u = [u_ref[:, e].reshape(n_rows, width) for e in experts]
        dy = [y_ref[:, e].reshape(n_rows, width) for e in experts]
        holds = [s_ref[e][:, None, :] == iota((n_dev, cap, LANES), 1).astype(F32) for e in experts]
        gate_row = [jnp.sum(jnp.where(holds[i], g_ref[e][:, None, :], 0.0), axis=2, keepdims=True).reshape(n_rows, 1)
                    for i, e in enumerate(experts)]
        q = [(gate_row[i] * dy[i].astype(F32)).astype(BF16) for i in each]
        pre = [(mm(u[i], w1_v[e]), mm(u[i], w3_v[e])) for i, e in enumerate(experts)]
        d_hidden = [mm_nt(q[i], w2_v[e]) for i, e in enumerate(experts)]
        sig = [jax.nn.sigmoid(a) for a, _ in pre]
        act = [pre[i][0] * sig[i] for i in each]
        hidden = [(act[i] * pre[i][1]).astype(BF16) for i in each]
        out = [mm(hidden[i], w2_v[e]).astype(BF16) for i, e in enumerate(experts)]
        for i in each:
            dw2_v[slot, i] = mm_tn(hidden[i], q[i])
        d_gate = [(d_hidden[i] * pre[i][1] * sig[i] * (1.0 + pre[i][0] * (1.0 - sig[i]))).astype(BF16) for i in each]
        d_up = [(d_hidden[i] * act[i]).astype(BF16) for i in each]
        for i, e in enumerate(experts):
            dg_row = jnp.sum(dy[i].astype(F32) * out[i].astype(F32), axis=1, keepdims=True).reshape(n_dev, cap, 1)
            dg_ref[e] = jnp.sum(jnp.where(holds[i], dg_row, 0.0), axis=1)
        for i, e in enumerate(experts):
            du = (mm_nt(d_gate[i], w1_v[e]) + mm_nt(d_up[i], w3_v[e])).astype(BF16)
            du_ref[:, e] = du.reshape(n_dev, cap, width)
        for i in each:
            dw1_v[slot, i] = mm_tn(u[i], d_gate[i])
            dw3_v[slot, i] = mm_tn(u[i], d_up[i])
        for i in range(3):
            store(g, i, slot).start()
        return carry
    steps = local // GROUPED
    lax.fori_loop(0, steps, step, 0)

    stack = scatter_lhs(s_map, None, tok)
    for d in range(n_dev):
        part[d] = token_sums(stack, d, du_ref[d].reshape(local * cap, width), tok, cap)
    for d in range(n_dev):
        total = jnp.zeros((top_k, LANES), F32)
        for i in range(local):
            total = jnp.where(rel_ref[d] == float(i), dg_ref[i, d : d + 1, :], total)
        dgate[d] = total
    for g in (steps - 2, steps - 1):
        for i in range(3):
            store(g, i, g % 2).wait()


def middle_kernel(dims, part_b, dg_part, dy_ref, x_ref, mid_all, sb, gb, w1, w3, w2,
                  dmid_all, x_again, dmid_own, dgate, part_x,
                  d_all, x_all, u_ref, o_ref, near, mine, got, dg_near, dg_mine, dg_got, d_buf, w1_v, w3_v, w2_v,
                  w_sems, send_sems, recv_sems):
    n_dev, tok, width, local, cap, top_k = dims
    pairs = ((w1, w1_v), (w3, w3_v), (w2, w2_v))
    load_weights(pairs, w_sems, local)
    links = Links(n_dev, send_sems, recv_sems)
    me = links.me
    links.greet()
    red = Reduce(links, part_b, (near, mine, got))
    dg = Reduce(links, dg_part, (dg_near, dg_mine, dg_got), split=False)
    s_map = sb[...].reshape(local * n_dev, LANES)

    def rows_of(d):
        fill_rows(s_map, d, ((mid_all, u_ref),), cap)

    red.start()
    dg.start()
    x_g = Gather(links, x_ref, x_all)
    x_all[me] = x_ref[...]
    for d in range(2):
        rows_of(d)
    red.far()
    red.near_sends()
    dg.far()
    dg.near_sends()
    for d in range(2, n_dev):
        rows_of(d)
    x_g.pass_on()
    red.relay()
    dg.relay()
    half = local // 2 // FORWARD_GROUPED * FORWARD_GROUPED
    forward_experts(pairs, w_sems, u_ref, o_ref, cap, 0, half)
    x_g.pass_far()
    dx = (dy_ref[...].astype(F32) + red.result()).astype(BF16)
    d_buf[...] = dx
    dmid_own[...] = dx
    d_all[me] = dx
    d_g = Gather(links, d_buf, d_all)
    forward_experts(pairs, w_sems, u_ref, o_ref, cap, half, local)
    d_g.pass_on()
    stack = scatter_lhs(s_map, gb[...].reshape(local * n_dev, LANES), tok)
    for d in range(n_dev):
        part_x[d] = token_sums(stack, d, o_ref[d].reshape(local * cap, width), tok, cap)
    d_g.pass_far()
    dgate[...] = dg.result()
    x_g.finish()
    x_again[...] = x_all[...]
    d_g.finish()
    dmid_all[...] = d_all[...]
    links.drain()


def final_kernel(x_ref, dx_ref, dga_ref, dgb_ref, x_out, dx_out, dga_out, dgb_out):
    x_out[...] = x_ref[...]
    dx_out[...] = dx_ref[...]
    tok = dga_out.shape[1]
    dga_out[...] = dga_ref[:, :tok]
    dgb_out[...] = dgb_ref[:, :tok]


def last_kernel(dims, part_a, dg_part, part_x, dmid_ref, mid_ref, dx_out, dgate, x_out,
                near, mine, got, dg_near, dg_mine, dg_got, x_near, x_mine, x_got, send_sems, recv_sems):
    links = Links(dims[0], send_sems, recv_sems)
    links.greet()
    reds = (Reduce(links, part_a, (near, mine, got)), Reduce(links, part_x, (x_near, x_mine, x_got)),
            Reduce(links, dg_part, (dg_near, dg_mine, dg_got), split=False))
    for red in reds:
        red.start()
    for red in reds:
        red.far()
        red.near_sends()
    for red in reds:
        red.relay()
    dx_out[...] = (dmid_ref[...].astype(F32) + reds[0].result()).astype(BF16)
    x_out[...] = (mid_ref[...].astype(F32) + reds[1].result()).astype(BF16)
    dgate[...] = reds[2].result()
    links.drain()


def remote_params(ident):
    return pltpu.CompilerParams(collective_id=ident, has_side_effects=True, vmem_limit_bytes=VMEM_LIMIT)


def dma_sems(count):
    return [pltpu.SemaphoreType.DMA((count,)), pltpu.SemaphoreType.DMA((count,))]


def solution(mesh):
    n_dev = mesh.shape["ep"]
    tok_spec = P(("dp", "ep"))
    w_spec = P("ep")

    def device_program(x_in, idx_a, idx_b, gate_a, gate_b, dy_out, w1_a, w3_a, w2_a, w1_b, w3_b, w2_b):
        tok, top_k = idx_a.shape
        width = x_in.shape[1]
        local, _, inner = w1_a.shape
        cap = CAP_FACTOR * tok * top_k // (local * n_dev)
        dims = (n_dev, tok, width, local, cap, top_k)
        sds = jax.ShapeDtypeStruct
        rows_all = sds((n_dev, tok, width), BF16)
        part_all = sds((n_dev, tok, width), F32)
        dg_all = sds((n_dev, top_k, LANES), F32)
        map_s = sds((local, n_dev, LANES), F32)
        own = sds((tok, width), BF16)

        weights_v = [pltpu.VMEM((local, width, inner), BF16)] * 2 + [pltpu.VMEM((local, inner, width), BF16)]
        w_sems = pltpu.SemaphoreType.DMA((3, local))
        rows_v = pltpu.VMEM((n_dev, tok, width), BF16)
        expert_v = pltpu.VMEM((n_dev, local, cap, width), BF16)

        count = 4 * Gather.COPIES + Reduce.COPIES
        mid_all, dy_all, mid_own, sa, ga, rela, sb, gb, relb = pl.pallas_call(
            functools.partial(first_kernel, dims),
            out_shape=(rows_all, rows_all, own, map_s, map_s, dg_all, map_s, map_s, dg_all),
            in_specs=[VMEM] * 6 + [ANY] * 3,
            out_specs=[VMEM] * 9,
            scratch_shapes=[rows_v, rows_v, rows_v, pltpu.VMEM((4 * top_k, LANES), F32), pltpu.VMEM((n_dev, 4 * top_k, LANES), F32), expert_v, expert_v,
                            pltpu.VMEM((n_dev, tok, width), F32), *Reduce.scratch(tok, width),
                            pltpu.VMEM((tok, width), BF16), *weights_v, w_sems, *dma_sems(count)],
            compiler_params=remote_params(0), name="first",
        )(x_in, dy_out, idx_a.T, gate_a.T, idx_b.T, gate_b.T, w1_a, w3_a, w2_a)

        def backward(x_all, d_all, s, g, rel, w1, w3, w2):
            return pl.pallas_call(
                functools.partial(backward_kernel, dims),
                out_shape=(sds((local, width, inner), F32), sds((local, width, inner), F32),
                           sds((local, inner, width), F32), part_all, dg_all),
                in_specs=[VMEM] * 5 + [ANY] * 3,
                out_specs=[ANY] * 3 + [VMEM] * 2,
                scratch_shapes=[expert_v, expert_v, expert_v, pltpu.VMEM((local, n_dev, LANES), F32), *weights_v,
                                *[pltpu.VMEM((2, GROUPED, width, inner), F32)] * 2,
                                pltpu.VMEM((2, GROUPED, inner, width), F32), w_sems, pltpu.SemaphoreType.DMA((3, 2))],
                compiler_params=pltpu.CompilerParams(vmem_limit_bytes=VMEM_LIMIT), name="backward",
            )(x_all, d_all, s, g, rel, w1, w3, w2)

        *grads_b, part_b, dg_b = backward(mid_all, dy_all, sb, gb, relb, w1_b, w3_b, w2_b)

        count = 2 * Gather.COPIES + 2 * Reduce.COPIES
        dmid_all, x_again, dmid_own, dgate_b, part_x = pl.pallas_call(
            functools.partial(middle_kernel, dims),
            out_shape=(rows_all, rows_all, own, sds((top_k, LANES), F32), part_all),
            in_specs=[VMEM] * 7 + [ANY] * 3,
            out_specs=[VMEM] * 5,
            scratch_shapes=[rows_v, rows_v, expert_v, expert_v, *Reduce.scratch(tok, width),
                            *Reduce.scratch(top_k, LANES), pltpu.VMEM((tok, width), BF16), *weights_v, w_sems,
                            *dma_sems(count)],
            compiler_params=remote_params(1), name="middle",
        )(part_b, dg_b, dy_out, x_in, mid_all, sb, gb, w1_b, w3_b, w2_b)

        *grads_a, part_a, dg_a = backward(x_again, dmid_all, sa, ga, rela, w1_a, w3_a, w2_a)

        count = 3 * Reduce.COPIES
        dx_in, dgate_a, x_out = pl.pallas_call(
            functools.partial(last_kernel, dims),
            out_shape=(own, sds((top_k, LANES), F32), own),
            in_specs=[VMEM] * 5,
            out_specs=[VMEM] * 3,
            scratch_shapes=[*Reduce.scratch(tok, width), *Reduce.scratch(top_k, LANES), *Reduce.scratch(tok, width),
                            *dma_sems(count)],
            compiler_params=remote_params(2), name="last",
        )(part_a, dg_a, part_x, dmid_own, mid_own)
        gates = sds((top_k, tok), F32)
        x_out, dx_in, dgate_a, dgate_b = pl.pallas_call(
            final_kernel, out_shape=(own, own, gates, gates), in_specs=[VMEM] * 4, out_specs=[VMEM] * 4, name="final",
        )(x_out, dx_in, dgate_a, dgate_b)
        return (x_out, dx_in, *grads_a, *grads_b, dgate_a.T, dgate_b.T)

    return jax.shard_map(device_program, mesh=mesh, in_specs=(tok_spec,) * 6 + (w_spec,) * 6, out_specs=(tok_spec,) * 10, check_vma=False)
```

```python
import functools

import jax
import jax.numpy as jnp
from jax import lax
from jax.experimental import pallas as pl
from jax.experimental.pallas import tpu as pltpu
from jax.sharding import PartitionSpec as P

BF16 = jnp.bfloat16
F32 = jnp.float32
MESH = pl.DeviceIdType.MESH
LANES = 128
CAP_FACTOR = 4
BF16_MAX = 3.3895313892515355e38
GROUPED = 2
FORWARD_GROUPED = 4
VMEM_LIMIT = 60 * 1024 * 1024
SMALL_VMEM_LIMIT = 16 * 1024 * 1024
VMEM = pl.BlockSpec(memory_space=pltpu.VMEM)
ANY = pl.BlockSpec(memory_space=pl.ANY)


def mm(lhs, rhs):
    return jnp.dot(lhs, rhs, preferred_element_type=F32)


def mm_tn(lhs, rhs):
    return lax.dot_general(lhs, rhs, (((0,), (0,)), ((), ())), preferred_element_type=F32)


def mm_nt(lhs, rhs):
    return lax.dot_general(lhs, rhs, (((1,), (1,)), ((), ())), preferred_element_type=F32)


def iota(shape, dim):
    return lax.broadcasted_iota(jnp.int32, shape, dim)


def routing_maps(me, meta, layer, s_ref, g_ref, rel_ref, top_k, local):
    n_dev = meta.shape[0]
    base = (me * local).astype(F32)
    row = 2 * layer * top_k
    rel_ref[...] = meta[:, row : row + top_k, :] - base
    shape = (local, n_dev, LANES)
    expert = iota(shape, 0).astype(F32)
    hit, gate = jnp.zeros(shape, F32), jnp.zeros(shape, F32)
    for j in range(top_k):
        match = (meta[:, row + j, :] - base)[None] == expert
        hit = jnp.where(match, 1.0, hit)
        gate = jnp.where(match, meta[:, row + top_k + j, :][None], gate)
    hit = hit.reshape(local * n_dev, LANES)
    earlier = (iota((LANES, LANES), 0) < iota((LANES, LANES), 1)).astype(F32).astype(BF16)
    slot = jnp.where(hit > 0.0, mm(hit.astype(BF16), earlier), -1.0)
    s_ref[...] = slot.reshape(shape)
    g_ref[...] = gate


def row_picks(s_map, d, tok, n_dev, cap):
    pairs, lanes = s_map.shape
    n_rows = pairs // n_dev * cap
    spread = iota((n_rows, pairs), 1) == iota((n_rows, pairs), 0) // cap * n_dev + d
    slot = mm(spread.astype(F32).astype(BF16), s_map.astype(BF16))
    return jnp.where(slot == (iota((n_rows, lanes), 0) % cap).astype(F32), 1.0, 0.0).astype(BF16)[:, :tok]


def fill_rows(s_map, d, sources, cap):
    picks = row_picks(s_map, d, sources[0][0].shape[1], sources[0][0].shape[0], cap)
    for rows, out in sources:
        out[d] = mm(picks, rows[d]).astype(BF16).reshape(out.shape[1:])


def limbs(gate):
    hi = jnp.minimum(gate, BF16_MAX).astype(BF16)
    rest = gate - hi.astype(F32)
    mid = rest.astype(BF16)
    return hi, mid, (rest - mid.astype(F32)).astype(BF16)


def scatter_lhs(s_map, g_map, tok):
    stack = [s_map.T[:tok].astype(BF16)]
    if g_map is not None:
        stack += [limb.T[:tok].astype(BF16) for limb in (x.astype(F32) for x in limbs(g_map))]
    return jnp.concatenate(stack, axis=0)


def token_sums(stack, d, out_rows, tok, cap):
    pairs = stack.shape[1]
    n_rows = out_rows.shape[0]
    spread = iota((pairs, n_rows), 0) == iota((pairs, n_rows), 1) // cap * 8 + d
    maps = mm(stack, spread.astype(F32).astype(BF16))
    match = maps[:tok] == (iota((tok, n_rows), 1) % cap).astype(F32)
    if stack.shape[0] == tok:
        return mm(jnp.where(match, 1.0, 0.0).astype(BF16), out_rows)
    terms = (stack.shape[0] - tok) // tok
    lhs = [jnp.where(match, maps[(i + 1) * tok : (i + 2) * tok], 0.0).astype(BF16) for i in range(terms)]
    sums = mm(jnp.concatenate(lhs, axis=0), out_rows)
    total = sums[:tok]
    for i in range(1, terms):
        total = total + sums[i * tok : (i + 1) * tok]
    return total


class Links:
    def __init__(self, n_dev, send_sems, recv_sems):
        me = lax.axis_index("ep")
        self.n = n_dev
        self.me = me
        self.core = lax.rem(me, 2)
        self.partner = me + 1 - 2 * self.core
        self.right = lax.rem(me + 2, n_dev)
        self.left = lax.rem(me + n_dev - 2, n_dev)
        self.opp = lax.rem(me + 4, n_dev)
        self.send_sems, self.recv_sems = send_sems, recv_sems
        self.used = 0
        self.started = []

    def greet(self):
        barrier = pltpu.get_barrier_semaphore()
        for peer in (self.partner, self.left, self.right):
            pl.semaphore_signal(barrier, inc=1, device_id={"ep": peer}, device_id_type=MESH)
        pl.semaphore_wait(barrier, 3)

    def copy(self, src, dst, peer):
        slot = self.used
        self.used += 1
        rdma = pltpu.make_async_remote_copy(
            src_ref=src, dst_ref=dst, send_sem=self.send_sems.at[slot], recv_sem=self.recv_sems.at[slot],
            device_id={"ep": peer}, device_id_type=MESH)
        rdma.start()
        self.started.append(rdma)
        return rdma

    def drain(self):
        for rdma in self.started:
            rdma.wait_send()


class Gather:
    COPIES = 9

    def __init__(self, links, own, full):
        k, self.k, self.full = links, links, full
        self.half = own.shape[0] // 2
        self.to_right = k.copy(own, full.at[k.me], k.right)
        self.to_left = k.copy(own, full.at[k.me], k.left)
        self.to_partner = k.copy(own, full.at[k.me], k.partner)

    def pass_on(self):
        k, full, half = self.k, self.full, self.half
        self.to_right.wait_recv()
        self.far_a = k.copy(full.at[k.left, pl.ds(0, half)], full.at[k.left, pl.ds(0, half)], k.right)
        self.side_a = k.copy(full.at[k.left], full.at[k.left], k.partner)
        self.to_left.wait_recv()
        self.far_b = k.copy(full.at[k.right, pl.ds(half, half)], full.at[k.right, pl.ds(half, half)], k.left)
        self.side_b = k.copy(full.at[k.right], full.at[k.right], k.partner)

    def pass_far(self):
        k, full, half = self.k, self.full, self.half
        self.far_a.wait_recv()
        self.last_a = k.copy(full.at[k.opp, pl.ds(0, half)], full.at[k.opp, pl.ds(0, half)], k.partner)
        self.far_b.wait_recv()
        self.last_b = k.copy(full.at[k.opp, pl.ds(half, half)], full.at[k.opp, pl.ds(half, half)], k.partner)

    def wait_partner(self):
        self.to_partner.wait_recv()

    def wait_sides(self):
        self.side_a.wait_recv()
        self.side_b.wait_recv()

    def wait_last(self):
        self.last_a.wait_recv()
        self.last_b.wait_recv()

    def finish(self):
        self.wait_partner()
        self.wait_sides()
        self.wait_last()


class Reduce:
    COPIES = 10

    @staticmethod
    def scratch(rows, width):
        return [pltpu.VMEM((4, rows, width), F32), pltpu.VMEM((4, rows, width), F32), pltpu.VMEM((3, rows, width), F32)]

    def __init__(self, links, part, bufs, split=True):
        self.k, self.part = links, part
        self.near, self.mine, self.got = bufs
        rows = part.shape[1]
        self.rows = rows
        self.half = rows // 2 if split else rows
        self.side = {}

    def block(self, hop, core):
        k = self.k
        return lax.rem(k.me - k.core + 2 * hop, k.n) + core

    def start_side(self, hop):
        k = self.k
        self.side[hop] = k.copy(self.part.at[self.block(hop, 1 - k.core)], self.near.at[hop], k.partner)

    def start(self):
        for hop in (2, 1, 3, 0):
            self.start_side(hop)

    def add(self, hop, lo, hi, extra=None):
        own = self.part[self.block(hop, self.k.core), lo:hi, :]
        total = own + self.near[hop, lo:hi, :]
        if extra is not None:
            total = total + extra
        self.mine[hop, lo:hi, :] = total

    def far(self):
        k, half, rows = self.k, self.half, self.rows
        self.side[2].wait_recv()
        self.add(2, 0, rows)
        a = pl.ds(0, half)
        self.far_a = k.copy(self.mine.at[2, a], self.got.at[2, a], k.right)
        if half < rows:
            b = pl.ds(half, rows - half)
            self.far_b = k.copy(self.mine.at[2, b], self.got.at[2, b], k.left)

    def near_sends(self):
        k, half, rows = self.k, self.half, self.rows
        self.side[1].wait_recv()
        if half < rows:
            b = pl.ds(half, rows - half)
            self.add(1, half, rows)
            self.right_b = k.copy(self.mine.at[1, b], self.got.at[0, b], k.right)
        self.side[3].wait_recv()
        self.add(3, 0, half)
        a = pl.ds(0, half)
        self.left_a = k.copy(self.mine.at[3, a], self.got.at[1, a], k.left)

    def relay(self):
        k, half, rows = self.k, self.half, self.rows
        a = pl.ds(0, half)
        self.far_a.wait_recv()
        self.add(1, 0, half, self.got[2, :half, :])
        self.right_a = k.copy(self.mine.at[1, a], self.got.at[0, a], k.right)
        if half < rows:
            b = pl.ds(half, rows - half)
            self.far_b.wait_recv()
            self.add(3, half, rows, self.got[2, half:, :])
            self.left_b = k.copy(self.mine.at[3, b], self.got.at[1, b], k.left)

    def result(self):
        half, rows = self.half, self.rows
        self.side[0].wait_recv()
        if half < rows:
            self.right_b.wait_recv()
        self.left_a.wait_recv()
        self.right_a.wait_recv()
        if half < rows:
            self.left_b.wait_recv()
        return self.part[self.k.me] + self.near[0] + self.got[0] + self.got[1]


def load_weights(pairs, sems, local):
    def start(e, carry):
        for i, (src, dst) in enumerate(pairs):
            pltpu.make_async_copy(src.at[e], dst.at[e], sems.at[i, e]).start()
        return carry
    lax.fori_loop(0, local, start, 0)


def wait_weights(pairs, sems, e):
    for i, (src, dst) in enumerate(pairs):
        pltpu.make_async_copy(src.at[e], dst.at[e], sems.at[i, e]).wait()


def forward_experts(pairs, sems, u_ref, o_ref, cap, first, last):
    n_dev, _, _, width = u_ref.shape
    few = min(FORWARD_GROUPED, last - first)

    def step(g, carry):
        experts = [first + g * few + i for i in range(few)]
        for e in experts:
            wait_weights(pairs, sems, e)
        w_gate, w_up, w_down = (dst for _, dst in pairs)
        rows = [u_ref[:, e].reshape(n_dev * cap, width) for e in experts]
        pre = [(mm(u, w_gate[e]), mm(u, w_up[e])) for u, e in zip(rows, experts)]
        hidden = [(gate * jax.nn.sigmoid(gate) * up).astype(BF16) for gate, up in pre]
        for h, e in zip(hidden, experts):
            o_ref[:, e] = mm(h, w_down[e]).astype(BF16).reshape(n_dev, cap, width)
        return carry
    lax.fori_loop(0, (last - first) // few, step, 0)


def first_kernel(dims, x_ref, dy_ref, idx_a, gate_a, idx_b, gate_b, w1, w3, w2,
                 mid_all, dy_all, mid_own, sa, ga, rela, sb, gb, relb,
                 x_all, y_all, m_all, meta_ref, meta_all, u_ref, o_ref, part, near, mine, got, mid_buf, w1_v, w3_v, w2_v,
                 w_sems, send_sems, recv_sems):
    n_dev, tok, width, local, cap, top_k = dims
    pairs = ((w1, w1_v), (w3, w3_v), (w2, w2_v))
    load_weights(pairs, w_sems, local)
    meta_ref[...] = jnp.full(meta_ref.shape, -1.0, F32)
    for i, ref in enumerate((idx_a, gate_a, idx_b, gate_b)):
        meta_ref[i * top_k : (i + 1) * top_k, :tok] = ref[...].astype(F32)
    links = Links(n_dev, send_sems, recv_sems)
    me = links.me
    links.greet()
    meta_g = Gather(links, meta_ref, meta_all)
    x_g = Gather(links, x_ref, x_all)
    meta_all[me] = meta_ref[...]
    x_all[me] = x_ref[...]
    y_all[me] = dy_ref[...]
    meta_g.pass_on()
    x_g.pass_on()
    y_g = Gather(links, dy_ref, y_all)
    meta_g.pass_far()
    meta_g.finish()
    meta = meta_all[...]
    routing_maps(me, meta, 0, sa, ga, rela, top_k, local)
    routing_maps(me, meta, 1, sb, gb, relb, top_k, local)
    s_map = sa[...].reshape(local * n_dev, LANES)

    def rows_of(d):
        fill_rows(s_map, d, ((x_all, u_ref),), cap)

    rows_of(me)
    rows_of(links.left)
    rows_of(links.right)
    x_g.wait_partner()
    rows_of(links.partner)
    x_g.pass_far()
    x_g.wait_sides()
    side = 1 - 2 * links.core
    rows_of(links.left + side)
    rows_of(links.right + side)
    rows_of(links.opp)
    y_g.pass_on()
    x_g.wait_last()
    rows_of(links.opp + side)
    forward_experts(pairs, w_sems, u_ref, o_ref, cap, 0, local)
    y_g.pass_far()
    stack = scatter_lhs(s_map, ga[...].reshape(local * n_dev, LANES), tok)
    red = Reduce(links, part, (near, mine, got))

    def sums_of(d):
        part[d] = token_sums(stack, d, o_ref[d].reshape(local * cap, width), tok, cap)

    for hop in (2, 1, 3, 0):
        sums_of(red.block(hop, 1 - links.core))
        red.start_side(hop)
    for hop in (2, 1, 3, 0):
        sums_of(red.block(hop, links.core))
    red.far()
    red.near_sends()
    red.relay()
    x_mid = (x_ref[...].astype(F32) + red.result()).astype(BF16)
    mid_buf[...] = x_mid
    mid_own[...] = x_mid
    m_all[me] = x_mid
    m_g = Gather(links, mid_buf, m_all)
    m_g.pass_on()
    m_g.pass_far()
    y_g.finish()
    dy_all[...] = y_all[...]
    m_g.finish()
    mid_all[...] = m_all[...]
    links.drain()


def backward_kernel(dims, x_all, dy_all, s_ref, g_ref, rel_ref, w1, w3, w2,
                    dw1, dw3, dw2, part, dgate,
                    u_ref, y_ref, du_ref, dg_ref, w1_v, w3_v, w2_v, dw1_v, dw3_v, dw2_v, w_sems, out_sems):
    n_dev, tok, width, local, cap, top_k = dims
    n_rows = n_dev * cap
    pairs = ((w1, w1_v), (w3, w3_v), (w2, w2_v))
    outs = ((dw1_v, dw1), (dw3_v, dw3), (dw2_v, dw2))
    load_weights(pairs, w_sems, local)
    s_map = s_ref[...].reshape(local * n_dev, LANES)

    for d in range(n_dev):
        fill_rows(s_map, d, ((x_all, u_ref), (dy_all, y_ref)), cap)

    def store(g, i, slot):
        src, dst = outs[i]
        return pltpu.make_async_copy(src.at[slot], dst.at[pl.ds(g * GROUPED, GROUPED)], out_sems.at[i, slot])

    def step(g, carry):
        slot = lax.rem(g, 2)
        experts = [g * GROUPED + i for i in range(GROUPED)]
        each = range(GROUPED)
        for e in experts:
            wait_weights(pairs, w_sems, e)

        @pl.when(g >= 2)
        def _():
            for i in range(3):
                store(g - 2, i, slot).wait()
        u = [u_ref[:, e].reshape(n_rows, width) for e in experts]
        dy = [y_ref[:, e].reshape(n_rows, width) for e in experts]
        holds = [s_ref[e][:, None, :] == iota((n_dev, cap, LANES), 1).astype(F32) for e in experts]
        gate_row = [jnp.sum(jnp.where(holds[i], g_ref[e][:, None, :], 0.0), axis=2, keepdims=True).reshape(n_rows, 1)
                    for i, e in enumerate(experts)]
        q = [(gate_row[i] * dy[i].astype(F32)).astype(BF16) for i in each]
        pre = [(mm(u[i], w1_v[e]), mm(u[i], w3_v[e])) for i, e in enumerate(experts)]
        d_hidden = [mm_nt(q[i], w2_v[e]) for i, e in enumerate(experts)]
        sig = [jax.nn.sigmoid(a) for a, _ in pre]
        act = [pre[i][0] * sig[i] for i in each]
        hidden = [(act[i] * pre[i][1]).astype(BF16) for i in each]
        out = [mm(hidden[i], w2_v[e]).astype(BF16) for i, e in enumerate(experts)]
        for i in each:
            dw2_v[slot, i] = mm_tn(hidden[i], q[i])
        d_gate = [(d_hidden[i] * pre[i][1] * sig[i] * (1.0 + pre[i][0] * (1.0 - sig[i]))).astype(BF16) for i in each]
        d_up = [(d_hidden[i] * act[i]).astype(BF16) for i in each]
        for i, e in enumerate(experts):
            dg_row = jnp.sum(dy[i].astype(F32) * out[i].astype(F32), axis=1, keepdims=True).reshape(n_dev, cap, 1)
            dg_ref[e] = jnp.sum(jnp.where(holds[i], dg_row, 0.0), axis=1)
        for i, e in enumerate(experts):
            du = (mm_nt(d_gate[i], w1_v[e]) + mm_nt(d_up[i], w3_v[e])).astype(BF16)
            du_ref[:, e] = du.reshape(n_dev, cap, width)
        for i in each:
            dw1_v[slot, i] = mm_tn(u[i], d_gate[i])
            dw3_v[slot, i] = mm_tn(u[i], d_up[i])
        for i in range(3):
            store(g, i, slot).start()
        return carry
    steps = local // GROUPED
    lax.fori_loop(0, steps, step, 0)

    stack = scatter_lhs(s_map, None, tok)
    for d in range(n_dev):
        part[d] = token_sums(stack, d, du_ref[d].reshape(local * cap, width), tok, cap)
    for d in range(n_dev):
        total = jnp.zeros((top_k, LANES), F32)
        for i in range(local):
            total = jnp.where(rel_ref[d] == float(i), dg_ref[i, d : d + 1, :], total)
        dgate[d] = total
    for g in (steps - 2, steps - 1):
        for i in range(3):
            store(g, i, g % 2).wait()


def middle_kernel(dims, part_b, dg_part, dy_ref, x_ref, mid_all, sb, gb, w1, w3, w2,
                  dmid_all, x_again, dmid_own, dgate, own_x, right_x, opp_x, left_x,
                  part_x, near_x, d_all, x_all, u_ref, o_ref, near, mine, got, dg_near, dg_mine, dg_got, d_buf, w1_v, w3_v, w2_v,
                  w_sems, send_sems, recv_sems):
    n_dev, tok, width, local, cap, top_k = dims
    pairs = ((w1, w1_v), (w3, w3_v), (w2, w2_v))
    load_weights(pairs, w_sems, local)
    links = Links(n_dev, send_sems, recv_sems)
    me = links.me
    links.greet()
    red = Reduce(links, part_b, (near, mine, got))
    dg = Reduce(links, dg_part, (dg_near, dg_mine, dg_got), split=False)
    s_map = sb[...].reshape(local * n_dev, LANES)

    def rows_of(d):
        fill_rows(s_map, d, ((mid_all, u_ref),), cap)

    red.start()
    dg.start()
    x_g = Gather(links, x_ref, x_all)
    x_all[me] = x_ref[...]
    for d in range(2):
        rows_of(d)
    red.far()
    red.near_sends()
    dg.far()
    dg.near_sends()
    for d in range(2, n_dev):
        rows_of(d)
    x_g.pass_on()
    red.relay()
    dg.relay()
    half = local // 2 // FORWARD_GROUPED * FORWARD_GROUPED
    forward_experts(pairs, w_sems, u_ref, o_ref, cap, 0, half)
    x_g.pass_far()
    dx = (dy_ref[...].astype(F32) + red.result()).astype(BF16)
    d_buf[...] = dx
    dmid_own[...] = dx
    d_all[me] = dx
    d_g = Gather(links, d_buf, d_all)
    forward_experts(pairs, w_sems, u_ref, o_ref, cap, half, local)
    d_g.pass_on()
    stack = scatter_lhs(s_map, gb[...].reshape(local * n_dev, LANES), tok)
    for d in range(n_dev):
        part_x[d % 2, d // 2] = token_sums(stack, d, o_ref[d].reshape(local * cap, width), tok, cap)
    side_x = links.copy(part_x.at[1 - links.core], near_x, links.partner)
    d_g.pass_far()
    side_x.wait_recv()
    for hop, out in enumerate((own_x, right_x, opp_x, left_x)):
        chip = lax.rem((me - links.core) // 2 + hop, n_dev // 2)
        out[...] = part_x[links.core, chip] + near_x[chip]
    dgate[...] = dg.result()
    x_g.finish()
    x_again[...] = x_all[...]
    d_g.finish()
    dmid_all[...] = d_all[...]
    links.drain()


def final_kernel(x_ref, dx_ref, dga_ref, dgb_ref, x_out, dx_out, dga_out, dgb_out):
    x_out[...] = x_ref[...]
    dx_out[...] = dx_ref[...]
    tok = dga_out.shape[1]
    dga_out[...] = dga_ref[:, :tok]
    dgb_out[...] = dgb_ref[:, :tok]


def last_kernel(dims, part_a, dg_part, dmid_ref, mid_ref, own_x, left_x, opp_x, right_x, dx_out, dgate, x_out,
                near, mine, got, dg_near, dg_mine, dg_got, send_sems, recv_sems):
    links = Links(dims[0], send_sems, recv_sems)
    links.greet()
    red = Reduce(links, part_a, (near, mine, got))
    dg = Reduce(links, dg_part, (dg_near, dg_mine, dg_got), split=False)
    red.start()
    dg.start()
    red.far()
    red.near_sends()
    dg.far()
    dg.near_sends()
    total = own_x[...] + left_x[...] + opp_x[...] + right_x[...]
    x_out[...] = (mid_ref[...].astype(F32) + total).astype(BF16)
    red.relay()
    dg.relay()
    dx_out[...] = (dmid_ref[...].astype(F32) + red.result()).astype(BF16)
    dgate[...] = dg.result()
    links.drain()


def remote_params(ident, limit=VMEM_LIMIT):
    return pltpu.CompilerParams(collective_id=ident, has_side_effects=True, vmem_limit_bytes=limit)


def dma_sems(count):
    return [pltpu.SemaphoreType.DMA((count,)), pltpu.SemaphoreType.DMA((count,))]


def solution(mesh):
    n_dev = mesh.shape["ep"]
    tok_spec = P(("dp", "ep"))
    w_spec = P("ep")

    def device_program(x_in, idx_a, idx_b, gate_a, gate_b, dy_out, w1_a, w3_a, w2_a, w1_b, w3_b, w2_b):
        tok, top_k = idx_a.shape
        width = x_in.shape[1]
        local, _, inner = w1_a.shape
        cap = CAP_FACTOR * tok * top_k // (local * n_dev)
        dims = (n_dev, tok, width, local, cap, top_k)
        sds = jax.ShapeDtypeStruct
        rows_all = sds((n_dev, tok, width), BF16)
        part_all = sds((n_dev, tok, width), F32)
        dg_all = sds((n_dev, top_k, LANES), F32)
        map_s = sds((local, n_dev, LANES), F32)
        own = sds((tok, width), BF16)

        weights_v = [pltpu.VMEM((local, width, inner), BF16)] * 2 + [pltpu.VMEM((local, inner, width), BF16)]
        w_sems = pltpu.SemaphoreType.DMA((3, local))
        rows_v = pltpu.VMEM((n_dev, tok, width), BF16)
        expert_v = pltpu.VMEM((n_dev, local, cap, width), BF16)

        count = 4 * Gather.COPIES + Reduce.COPIES
        mid_all, dy_all, mid_own, sa, ga, rela, sb, gb, relb = pl.pallas_call(
            functools.partial(first_kernel, dims),
            out_shape=(rows_all, rows_all, own, map_s, map_s, dg_all, map_s, map_s, dg_all),
            in_specs=[VMEM] * 6 + [ANY] * 3,
            out_specs=[VMEM] * 9,
            scratch_shapes=[rows_v, rows_v, rows_v, pltpu.VMEM((4 * top_k, LANES), F32), pltpu.VMEM((n_dev, 4 * top_k, LANES), F32), expert_v, expert_v,
                            pltpu.VMEM((n_dev, tok, width), F32), *Reduce.scratch(tok, width),
                            pltpu.VMEM((tok, width), BF16), *weights_v, w_sems, *dma_sems(count)],
            compiler_params=remote_params(0), name="first",
        )(x_in, dy_out, idx_a.T, gate_a.T, idx_b.T, gate_b.T, w1_a, w3_a, w2_a)

        def backward(x_all, d_all, s, g, rel, w1, w3, w2):
            return pl.pallas_call(
                functools.partial(backward_kernel, dims),
                out_shape=(sds((local, width, inner), F32), sds((local, width, inner), F32),
                           sds((local, inner, width), F32), part_all, dg_all),
                in_specs=[VMEM] * 5 + [ANY] * 3,
                out_specs=[ANY] * 3 + [VMEM] * 2,
                scratch_shapes=[expert_v, expert_v, expert_v, pltpu.VMEM((local, n_dev, LANES), F32), *weights_v,
                                *[pltpu.VMEM((2, GROUPED, width, inner), F32)] * 2,
                                pltpu.VMEM((2, GROUPED, inner, width), F32), w_sems, pltpu.SemaphoreType.DMA((3, 2))],
                compiler_params=pltpu.CompilerParams(vmem_limit_bytes=VMEM_LIMIT), name="backward",
                cost_estimate=pl.CostEstimate(flops=18 * local * n_dev * cap * width * inner, transcendentals=0,
                                              bytes_accessed=18 * local * width * inner),
            )(x_all, d_all, s, g, rel, w1, w3, w2)

        *grads_b, part_b, dg_b = backward(mid_all, dy_all, sb, gb, relb, w1_b, w3_b, w2_b)

        count = 2 * Gather.COPIES + 2 * Reduce.COPIES + 1
        sums = sds((tok, width), F32)
        chip_sums = pltpu.VMEM((n_dev // 2, tok, width), F32)
        dmid_all, x_again, dmid_own, dgate_b, own_x, right_x, opp_x, left_x = pl.pallas_call(
            functools.partial(middle_kernel, dims),
            out_shape=(rows_all, rows_all, own, sds((top_k, LANES), F32), sums, sums, sums, sums),
            in_specs=[VMEM] * 7 + [ANY] * 3,
            out_specs=[VMEM] * 8,
            scratch_shapes=[pltpu.VMEM((2, n_dev // 2, tok, width), F32), chip_sums, rows_v, rows_v, expert_v, expert_v,
                            *Reduce.scratch(tok, width), *Reduce.scratch(top_k, LANES), pltpu.VMEM((tok, width), BF16),
                            *weights_v, w_sems, *dma_sems(count)],
            compiler_params=remote_params(1), name="middle",
        )(part_b, dg_b, dy_out, x_in, mid_all, sb, gb, w1_b, w3_b, w2_b)

        def shift(rows, hop):
            return lax.ppermute(rows, "ep", [(i, (i + 2 * hop) % n_dev) for i in range(n_dev)])

        left_x, opp_x, right_x = shift(right_x, 1), shift(opp_x, 2), shift(left_x, 3)
        *grads_a, part_a, dg_a = backward(x_again, dmid_all, sa, ga, rela, w1_a, w3_a, w2_a)

        dx_in, dgate_a, x_out = pl.pallas_call(
            functools.partial(last_kernel, dims),
            out_shape=(own, sds((top_k, LANES), F32), own),
            in_specs=[VMEM] * 8,
            out_specs=[VMEM] * 3,
            scratch_shapes=[*Reduce.scratch(tok, width), *Reduce.scratch(top_k, LANES), *dma_sems(2 * Reduce.COPIES)],
            compiler_params=remote_params(2, SMALL_VMEM_LIMIT), name="last",
        )(part_a, dg_a, dmid_own, mid_own, own_x, left_x, opp_x, right_x)
        gates = sds((top_k, tok), F32)
        x_out, dx_in, dgate_a, dgate_b = pl.pallas_call(
            final_kernel, out_shape=(own, own, gates, gates), in_specs=[VMEM] * 4, out_specs=[VMEM] * 4, name="final",
        )(x_out, dx_in, dgate_a, dgate_b)
        return (x_out, dx_in, *grads_a, *grads_b, dgate_a.T, dgate_b.T)

    return jax.shard_map(device_program, mesh=mesh, in_specs=(tok_spec,) * 6 + (w_spec,) * 6, out_specs=(tok_spec,) * 10, check_vma=False)
```

```python
import functools

import jax
import jax.numpy as jnp
from jax import lax
from jax.experimental import pallas as pl
from jax.experimental.pallas import tpu as pltpu
from jax.sharding import PartitionSpec as P

BF16 = jnp.bfloat16
F32 = jnp.float32
MESH = pl.DeviceIdType.MESH
LANES = 128
CAP_FACTOR = 4
BF16_MAX = 3.3895313892515355e38
GROUPED = 2
FORWARD_GROUPED = 4
VMEM_LIMIT = 60 * 1024 * 1024
SMALL_VMEM_LIMIT = 8 * 1024 * 1024
VMEM = pl.BlockSpec(memory_space=pltpu.VMEM)
ANY = pl.BlockSpec(memory_space=pl.ANY)


def mm(lhs, rhs):
    return jnp.dot(lhs, rhs, preferred_element_type=F32)


def mm_tn(lhs, rhs):
    return lax.dot_general(lhs, rhs, (((0,), (0,)), ((), ())), preferred_element_type=F32)


def iota(shape, dim):
    return lax.broadcasted_iota(jnp.int32, shape, dim)


def routing_maps(me, meta, layer, s_ref, g_ref, rel_ref, top_k, local):
    n_dev = meta.shape[0]
    base = (me * local).astype(F32)
    row = 2 * layer * top_k
    rel_ref[...] = meta[:, row : row + top_k, :] - base
    shape = (local, n_dev, LANES)
    expert = iota(shape, 0).astype(F32)
    hit, gate = jnp.zeros(shape, F32), jnp.zeros(shape, F32)
    for j in range(top_k):
        match = (meta[:, row + j, :] - base)[None] == expert
        hit = jnp.where(match, 1.0, hit)
        gate = jnp.where(match, meta[:, row + top_k + j, :][None], gate)
    hit = hit.reshape(local * n_dev, LANES)
    earlier = (iota((LANES, LANES), 0) < iota((LANES, LANES), 1)).astype(F32).astype(BF16)
    slot = jnp.where(hit > 0.0, mm(hit.astype(BF16), earlier), -1.0)
    s_ref[...] = slot.reshape(shape)
    g_ref[...] = gate


def row_picks(s_map, d, tok, n_dev, cap):
    pairs, lanes = s_map.shape
    n_rows = pairs // n_dev * cap
    spread = iota((n_rows, pairs), 1) == iota((n_rows, pairs), 0) // cap * n_dev + d
    slot = mm(spread.astype(F32).astype(BF16), s_map.astype(BF16))
    return jnp.where(slot == (iota((n_rows, lanes), 0) % cap).astype(F32), 1.0, 0.0).astype(BF16)[:, :tok]


def fill_rows(s_map, d, sources, cap):
    picks = row_picks(s_map, d, sources[0][0].shape[1], sources[0][0].shape[0], cap)
    for rows, out in sources:
        out[d] = mm(picks, rows[d]).astype(BF16).reshape(out.shape[1:])


def limbs(gate):
    hi = jnp.minimum(gate, BF16_MAX).astype(BF16)
    rest = gate - hi.astype(F32)
    mid = rest.astype(BF16)
    return hi, mid, (rest - mid.astype(F32)).astype(BF16)


def scatter_lhs(s_map, g_map, tok):
    stack = [s_map.T[:tok].astype(BF16)]
    if g_map is not None:
        stack += [limb.T[:tok].astype(BF16) for limb in (x.astype(F32) for x in limbs(g_map))]
    return jnp.concatenate(stack, axis=0)


def token_sums(stack, d, out_rows, tok, cap):
    pairs = stack.shape[1]
    n_rows = out_rows.shape[0]
    spread = iota((pairs, n_rows), 0) == iota((pairs, n_rows), 1) // cap * 8 + d
    maps = mm(stack, spread.astype(F32).astype(BF16))
    match = maps[:tok] == (iota((tok, n_rows), 1) % cap).astype(F32)
    if stack.shape[0] == tok:
        return mm(jnp.where(match, 1.0, 0.0).astype(BF16), out_rows)
    terms = (stack.shape[0] - tok) // tok
    lhs = [jnp.where(match, maps[(i + 1) * tok : (i + 2) * tok], 0.0).astype(BF16) for i in range(terms)]
    sums = mm(jnp.concatenate(lhs, axis=0), out_rows)
    total = sums[:tok]
    for i in range(1, terms):
        total = total + sums[i * tok : (i + 1) * tok]
    return total


class Links:
    def __init__(self, n_dev, send_sems, recv_sems):
        me = lax.axis_index("ep")
        self.n = n_dev
        self.me = me
        self.core = lax.rem(me, 2)
        self.partner = me + 1 - 2 * self.core
        self.right = lax.rem(me + 2, n_dev)
        self.left = lax.rem(me + n_dev - 2, n_dev)
        self.opp = lax.rem(me + 4, n_dev)
        self.send_sems, self.recv_sems = send_sems, recv_sems
        self.used = 0
        self.started = []

    def greet(self):
        barrier = pltpu.get_barrier_semaphore()
        for peer in (self.partner, self.left, self.right):
            pl.semaphore_signal(barrier, inc=1, device_id={"ep": peer}, device_id_type=MESH)
        pl.semaphore_wait(barrier, 3)

    def copy(self, src, dst, peer):
        slot = self.used
        self.used += 1
        rdma = pltpu.make_async_remote_copy(
            src_ref=src, dst_ref=dst, send_sem=self.send_sems.at[slot], recv_sem=self.recv_sems.at[slot],
            device_id={"ep": peer}, device_id_type=MESH)
        rdma.start()
        self.started.append(rdma)
        return rdma

    def drain(self):
        for rdma in self.started:
            rdma.wait_send()


class Gather:
    COPIES = 9

    def __init__(self, links, own, full):
        k, self.k, self.full = links, links, full
        self.half = own.shape[0] // 2
        self.to_right = k.copy(own, full.at[k.me], k.right)
        self.to_left = k.copy(own, full.at[k.me], k.left)
        self.to_partner = k.copy(own, full.at[k.me], k.partner)

    def pass_on(self):
        k, full, half = self.k, self.full, self.half
        self.to_right.wait_recv()
        self.far_a = k.copy(full.at[k.left, pl.ds(0, half)], full.at[k.left, pl.ds(0, half)], k.right)
        self.side_a = k.copy(full.at[k.left], full.at[k.left], k.partner)
        self.to_left.wait_recv()
        self.far_b = k.copy(full.at[k.right, pl.ds(half, half)], full.at[k.right, pl.ds(half, half)], k.left)
        self.side_b = k.copy(full.at[k.right], full.at[k.right], k.partner)

    def pass_far(self):
        k, full, half = self.k, self.full, self.half
        self.far_a.wait_recv()
        self.last_a = k.copy(full.at[k.opp, pl.ds(0, half)], full.at[k.opp, pl.ds(0, half)], k.partner)
        self.far_b.wait_recv()
        self.last_b = k.copy(full.at[k.opp, pl.ds(half, half)], full.at[k.opp, pl.ds(half, half)], k.partner)

    def wait_partner(self):
        self.to_partner.wait_recv()

    def wait_sides(self):
        self.side_a.wait_recv()
        self.side_b.wait_recv()

    def wait_last(self):
        self.last_a.wait_recv()
        self.last_b.wait_recv()

    def finish(self):
        self.wait_partner()
        self.wait_sides()
        self.wait_last()


class Reduce:
    COPIES = 10

    @staticmethod
    def scratch(rows, width):
        return [pltpu.VMEM((4, rows, width), F32), pltpu.VMEM((4, rows, width), F32), pltpu.VMEM((3, rows, width), F32)]

    def __init__(self, links, part, bufs, split=True):
        self.k, self.part = links, part
        self.near, self.mine, self.got = bufs
        rows = part.shape[1]
        self.rows = rows
        self.half = rows // 2 if split else rows
        self.side = {}

    def block(self, hop, core):
        k = self.k
        return lax.rem(k.me - k.core + 2 * hop, k.n) + core

    def start_side(self, hop):
        k = self.k
        self.side[hop] = k.copy(self.part.at[self.block(hop, 1 - k.core)], self.near.at[hop], k.partner)

    def start(self):
        for hop in (2, 1, 3, 0):
            self.start_side(hop)

    def add(self, hop, lo, hi, extra=None):
        own = self.part[self.block(hop, self.k.core), lo:hi, :]
        total = own + self.near[hop, lo:hi, :]
        if extra is not None:
            total = total + extra
        self.mine[hop, lo:hi, :] = total

    def far(self):
        k, half, rows = self.k, self.half, self.rows
        self.side[2].wait_recv()
        self.add(2, 0, rows)
        a = pl.ds(0, half)
        self.far_a = k.copy(self.mine.at[2, a], self.got.at[2, a], k.right)
        if half < rows:
            b = pl.ds(half, rows - half)
            self.far_b = k.copy(self.mine.at[2, b], self.got.at[2, b], k.left)

    def near_sends(self):
        k, half, rows = self.k, self.half, self.rows
        self.side[1].wait_recv()
        if half < rows:
            b = pl.ds(half, rows - half)
            self.add(1, half, rows)
            self.right_b = k.copy(self.mine.at[1, b], self.got.at[0, b], k.right)
        self.side[3].wait_recv()
        self.add(3, 0, half)
        a = pl.ds(0, half)
        self.left_a = k.copy(self.mine.at[3, a], self.got.at[1, a], k.left)

    def relay(self):
        k, half, rows = self.k, self.half, self.rows
        a = pl.ds(0, half)
        self.far_a.wait_recv()
        self.add(1, 0, half, self.got[2, :half, :])
        self.right_a = k.copy(self.mine.at[1, a], self.got.at[0, a], k.right)
        if half < rows:
            b = pl.ds(half, rows - half)
            self.far_b.wait_recv()
            self.add(3, half, rows, self.got[2, half:, :])
            self.left_b = k.copy(self.mine.at[3, b], self.got.at[1, b], k.left)

    def result(self):
        half, rows = self.half, self.rows
        self.side[0].wait_recv()
        if half < rows:
            self.right_b.wait_recv()
        self.left_a.wait_recv()
        self.right_a.wait_recv()
        if half < rows:
            self.left_b.wait_recv()
        return self.part[self.k.me] + self.near[0] + self.got[0] + self.got[1]


def load_weights(pairs, sems, local):
    def start(e, carry):
        for i, (src, dst) in enumerate(pairs):
            pltpu.make_async_copy(src.at[e], dst.at[e], sems.at[i, e]).start()
        return carry
    lax.fori_loop(0, local, start, 0)


def wait_weights(pairs, sems, e):
    for i, (src, dst) in enumerate(pairs):
        pltpu.make_async_copy(src.at[e], dst.at[e], sems.at[i, e]).wait()


def forward_experts(pairs, sems, u_ref, o_ref, cap, first, last):
    n_dev, _, _, width = u_ref.shape
    few = min(FORWARD_GROUPED, last - first)

    def step(g, carry):
        experts = [first + g * few + i for i in range(few)]
        for e in experts:
            wait_weights(pairs, sems, e)
        w_gate, w_up, w_down = (dst for _, dst in pairs)
        rows = [u_ref[:, e].reshape(n_dev * cap, width) for e in experts]
        pre = [(mm(u, w_gate[e]), mm(u, w_up[e])) for u, e in zip(rows, experts)]
        hidden = [(gate * jax.nn.sigmoid(gate) * up).astype(BF16) for gate, up in pre]
        for h, e in zip(hidden, experts):
            o_ref[:, e] = mm(h, w_down[e]).astype(BF16).reshape(n_dev, cap, width)
        return carry
    lax.fori_loop(0, (last - first) // few, step, 0)


def first_kernel(dims, x_ref, dy_ref, idx_a, gate_a, idx_b, gate_b, w1, w3, w2,
                 mid_all, dy_all, mid_own, sa, ga, rela, sb, gb, relb,
                 x_all, y_all, m_all, meta_ref, meta_all, u_ref, o_ref, part, near, mine, got, mid_buf, w1_v, w3_v, w2_v,
                 w_sems, send_sems, recv_sems):
    n_dev, tok, width, local, cap, top_k = dims
    pairs = ((w1, w1_v), (w3, w3_v), (w2, w2_v))
    load_weights(pairs, w_sems, local)
    meta_ref[...] = jnp.full(meta_ref.shape, -1.0, F32)
    for i, ref in enumerate((idx_a, gate_a, idx_b, gate_b)):
        meta_ref[i * top_k : (i + 1) * top_k, :tok] = ref[...].astype(F32)
    links = Links(n_dev, send_sems, recv_sems)
    me = links.me
    links.greet()
    meta_g = Gather(links, meta_ref, meta_all)
    x_g = Gather(links, x_ref, x_all)
    meta_all[me] = meta_ref[...]
    x_all[me] = x_ref[...]
    y_all[me] = dy_ref[...]
    meta_g.pass_on()
    x_g.pass_on()
    y_g = Gather(links, dy_ref, y_all)
    meta_g.pass_far()
    meta_g.finish()
    meta = meta_all[...]
    routing_maps(me, meta, 0, sa, ga, rela, top_k, local)
    routing_maps(me, meta, 1, sb, gb, relb, top_k, local)
    s_map = sa[...].reshape(local * n_dev, LANES)

    def rows_of(d):
        fill_rows(s_map, d, ((x_all, u_ref),), cap)

    rows_of(me)
    rows_of(links.left)
    rows_of(links.right)
    x_g.wait_partner()
    rows_of(links.partner)
    x_g.pass_far()
    x_g.wait_sides()
    side = 1 - 2 * links.core
    rows_of(links.left + side)
    rows_of(links.right + side)
    rows_of(links.opp)
    y_g.pass_on()
    x_g.wait_last()
    rows_of(links.opp + side)
    forward_experts(pairs, w_sems, u_ref, o_ref, cap, 0, local)
    y_g.pass_far()
    stack = scatter_lhs(s_map, ga[...].reshape(local * n_dev, LANES), tok)
    red = Reduce(links, part, (near, mine, got))

    def sums_of(d):
        part[d] = token_sums(stack, d, o_ref[d].reshape(local * cap, width), tok, cap)

    for hop in (2, 1, 3, 0):
        sums_of(red.block(hop, 1 - links.core))
        red.start_side(hop)
    for hop in (2, 1, 3, 0):
        sums_of(red.block(hop, links.core))
    red.far()
    red.near_sends()
    red.relay()
    x_mid = (x_ref[...].astype(F32) + red.result()).astype(BF16)
    mid_buf[...] = x_mid
    mid_own[...] = x_mid
    m_all[me] = x_mid
    m_g = Gather(links, mid_buf, m_all)
    m_g.pass_on()
    m_g.pass_far()
    y_g.finish()
    dy_all[...] = y_all[...]
    m_g.finish()
    mid_all[...] = m_all[...]
    links.drain()


def backward_kernel(dims, x_all, dy_all, s_ref, g_ref, rel_ref, w1, w3, w2,
                    dw1, dw3, dw2, part, dgate,
                    u_ref, y_ref, du_ref, dg_ref, w1_v, w3_v, w2_v, w1_t, w3_t, w2_t, dw1_v, dw3_v, dw2_v, part_v,
                    w_sems, out_sems, part_sems):
    n_dev, tok, width, local, cap, top_k = dims
    n_rows = n_dev * cap
    pairs = ((w1, w1_v), (w3, w3_v), (w2, w2_v))
    outs = ((dw1_v, dw1), (dw3_v, dw3), (dw2_v, dw2))
    load_weights(pairs, w_sems, local)
    s_map = s_ref[...].reshape(local * n_dev, LANES)

    for d in range(n_dev):
        fill_rows(s_map, d, ((x_all, u_ref), (dy_all, y_ref)), cap)

    def store(g, i, slot):
        src, dst = outs[i]
        return pltpu.make_async_copy(src.at[slot], dst.at[pl.ds(g * GROUPED, GROUPED)], out_sems.at[i, slot])

    def step(g, carry):
        slot = lax.rem(g, 2)
        experts = [g * GROUPED + i for i in range(GROUPED)]
        each = range(GROUPED)
        for e in experts:
            wait_weights(pairs, w_sems, e)

        @pl.when(g >= 2)
        def _():
            for i in range(3):
                store(g - 2, i, slot).wait()
        for i, e in enumerate(experts):
            w2_t[i] = w2_v[e].T
        u = [u_ref[:, e].reshape(n_rows, width) for e in experts]
        dy = [y_ref[:, e].reshape(n_rows, width) for e in experts]
        holds = [s_ref[e][:, None, :] == iota((n_dev, cap, LANES), 1).astype(F32) for e in experts]
        gate_row = [jnp.sum(jnp.where(holds[i], g_ref[e][:, None, :], 0.0), axis=2, keepdims=True).reshape(n_rows, 1)
                    for i, e in enumerate(experts)]
        q = [(gate_row[i] * dy[i].astype(F32)).astype(BF16) for i in each]
        pre = [(mm(u[i], w1_v[e]), mm(u[i], w3_v[e])) for i, e in enumerate(experts)]
        for i, e in enumerate(experts):
            w1_t[i] = w1_v[e].T
            w3_t[i] = w3_v[e].T
        d_hidden = [mm(q[i], w2_t[i]) for i in each]
        sig = [jax.nn.sigmoid(a) for a, _ in pre]
        act = [pre[i][0] * sig[i] for i in each]
        hidden = [(act[i] * pre[i][1]).astype(BF16) for i in each]
        out = [mm(hidden[i], w2_v[e]).astype(BF16) for i, e in enumerate(experts)]
        for i in each:
            dw2_v[slot, i] = mm_tn(hidden[i], q[i])
        d_gate = [(d_hidden[i] * pre[i][1] * sig[i] * (1.0 + pre[i][0] * (1.0 - sig[i]))).astype(BF16) for i in each]
        d_up = [(d_hidden[i] * act[i]).astype(BF16) for i in each]
        for i, e in enumerate(experts):
            dg_row = jnp.sum(dy[i].astype(F32) * out[i].astype(F32), axis=1, keepdims=True).reshape(n_dev, cap, 1)
            dg_ref[e] = jnp.sum(jnp.where(holds[i], dg_row, 0.0), axis=1)
        for i, e in enumerate(experts):
            du = (mm(d_gate[i], w1_t[i]) + mm(d_up[i], w3_t[i])).astype(BF16)
            du_ref[:, e] = du.reshape(n_dev, cap, width)
        for i in each:
            dw1_v[slot, i] = mm_tn(u[i], d_gate[i])
            dw3_v[slot, i] = mm_tn(u[i], d_up[i])
        for i in range(3):
            store(g, i, slot).start()
        return carry
    steps = local // GROUPED
    lax.fori_loop(0, steps, step, 0)

    stack = scatter_lhs(s_map, None, tok)
    for d in range(n_dev):
        part_v[d] = token_sums(stack, d, du_ref[d].reshape(local * cap, width), tok, cap)
        pltpu.make_async_copy(part_v.at[d], part.at[d], part_sems.at[d]).start()
    for d in range(n_dev):
        total = jnp.zeros((top_k, LANES), F32)
        for i in range(local):
            total = jnp.where(rel_ref[d] == float(i), dg_ref[i, d : d + 1, :], total)
        dgate[d] = total
    for g in (steps - 2, steps - 1):
        for i in range(3):
            store(g, i, g % 2).wait()
    for d in range(n_dev):
        pltpu.make_async_copy(part_v.at[d], part.at[d], part_sems.at[d]).wait()


def middle_kernel(dims, dg_part, dy_ref, x_ref, sb, gb, part_in, mid_in, w1, w3, w2,
                  x_again, dmid_all, dmid_own, dgate, own_x, right_x, opp_x, left_x,
                  part_b, mid_all, in_sems, part_x, near_x, d_all, x_all, u_ref, o_ref, near, mine, got, dg_near, dg_mine, dg_got, d_buf, w1_v, w3_v, w2_v,
                  w_sems, send_sems, recv_sems):
    n_dev, tok, width, local, cap, top_k = dims
    pairs = ((w1, w1_v), (w3, w3_v), (w2, w2_v))
    part_load = pltpu.make_async_copy(part_in, part_b, in_sems.at[0])
    mid_load = pltpu.make_async_copy(mid_in, mid_all, in_sems.at[1])
    part_load.start()
    mid_load.start()
    load_weights(pairs, w_sems, local)
    links = Links(n_dev, send_sems, recv_sems)
    me = links.me
    links.greet()
    part_load.wait()
    red = Reduce(links, part_b, (near, mine, got))
    dg = Reduce(links, dg_part, (dg_near, dg_mine, dg_got), split=False)
    s_map = sb[...].reshape(local * n_dev, LANES)

    def rows_of(d):
        fill_rows(s_map, d, ((mid_all, u_ref),), cap)

    red.start()
    dg.start()
    x_g = Gather(links, x_ref, x_all)
    x_all[me] = x_ref[...]
    mid_load.wait()
    for d in range(2):
        rows_of(d)
    red.far()
    red.near_sends()
    dg.far()
    dg.near_sends()
    for d in range(2, n_dev):
        rows_of(d)
    x_g.pass_on()
    red.relay()
    dg.relay()
    half = local // 2 // FORWARD_GROUPED * FORWARD_GROUPED
    forward_experts(pairs, w_sems, u_ref, o_ref, cap, 0, half)
    x_g.pass_far()
    dx = (dy_ref[...].astype(F32) + red.result()).astype(BF16)
    d_buf[...] = dx
    dmid_own[...] = dx
    d_all[me] = dx
    d_g = Gather(links, d_buf, d_all)
    forward_experts(pairs, w_sems, u_ref, o_ref, cap, half, local)
    d_g.pass_on()
    x_g.finish()
    x_store = pltpu.make_async_copy(x_all, x_again, in_sems.at[2])
    x_store.start()
    stack = scatter_lhs(s_map, gb[...].reshape(local * n_dev, LANES), tok)
    for d in range(n_dev):
        part_x[d % 2, d // 2] = token_sums(stack, d, o_ref[d].reshape(local * cap, width), tok, cap)
    side_x = links.copy(part_x.at[1 - links.core], near_x, links.partner)
    d_g.pass_far()
    side_x.wait_recv()
    for hop, out in enumerate((own_x, right_x, opp_x, left_x)):
        chip = lax.rem((me - links.core) // 2 + hop, n_dev // 2)
        out[...] = part_x[links.core, chip] + near_x[chip]
    dgate[...] = dg.result()
    d_g.finish()
    dmid_all[...] = d_all[...]
    x_store.wait()
    links.drain()


def final_kernel(mid_ref, own_x, left_x, opp_x, right_x, dx_ref, dga_ref, dgb_ref, x_out, dx_out, dga_out, dgb_out):
    total = own_x[...] + left_x[...] + opp_x[...] + right_x[...]
    x_out[...] = (mid_ref[...].astype(F32) + total).astype(BF16)
    dx_out[...] = dx_ref[...]
    tok = dga_out.shape[1]
    dga_out[...] = dga_ref[:, :tok]
    dgb_out[...] = dgb_ref[:, :tok]


def last_kernel(dims, dg_part, dmid_ref, part_in, dx_out, dgate,
                part_a, in_sem, near, mine, got, dg_near, dg_mine, dg_got, send_sems, recv_sems):
    part_load = pltpu.make_async_copy(part_in, part_a, in_sem.at[0])
    part_load.start()
    links = Links(dims[0], send_sems, recv_sems)
    links.greet()
    part_load.wait()
    red = Reduce(links, part_a, (near, mine, got))
    dg = Reduce(links, dg_part, (dg_near, dg_mine, dg_got), split=False)
    red.start()
    dg.start()
    red.far()
    red.near_sends()
    dg.far()
    dg.near_sends()
    red.relay()
    dg.relay()
    dx_out[...] = (dmid_ref[...].astype(F32) + red.result()).astype(BF16)
    dgate[...] = dg.result()
    links.drain()


def remote_params(ident):
    return pltpu.CompilerParams(collective_id=ident, has_side_effects=True, vmem_limit_bytes=VMEM_LIMIT)


def dma_sems(count):
    return [pltpu.SemaphoreType.DMA((count,)), pltpu.SemaphoreType.DMA((count,))]


def solution(mesh):
    n_dev = mesh.shape["ep"]
    tok_spec = P(("dp", "ep"))
    w_spec = P("ep")

    def device_program(x_in, idx_a, idx_b, gate_a, gate_b, dy_out, w1_a, w3_a, w2_a, w1_b, w3_b, w2_b):
        tok, top_k = idx_a.shape
        width = x_in.shape[1]
        local, _, inner = w1_a.shape
        cap = CAP_FACTOR * tok * top_k // (local * n_dev)
        dims = (n_dev, tok, width, local, cap, top_k)
        sds = jax.ShapeDtypeStruct
        rows_all = sds((n_dev, tok, width), BF16)
        part_all = sds((n_dev, tok, width), F32)
        dg_all = sds((n_dev, top_k, LANES), F32)
        map_s = sds((local, n_dev, LANES), F32)
        own = sds((tok, width), BF16)

        weights_v = [pltpu.VMEM((local, width, inner), BF16)] * 2 + [pltpu.VMEM((local, inner, width), BF16)]
        w_sems = pltpu.SemaphoreType.DMA((3, local))
        rows_v = pltpu.VMEM((n_dev, tok, width), BF16)
        expert_v = pltpu.VMEM((n_dev, local, cap, width), BF16)

        count = 4 * Gather.COPIES + Reduce.COPIES
        mid_all, dy_all, mid_own, sa, ga, rela, sb, gb, relb = pl.pallas_call(
            functools.partial(first_kernel, dims),
            out_shape=(rows_all, rows_all, own, map_s, map_s, dg_all, map_s, map_s, dg_all),
            in_specs=[VMEM] * 6 + [ANY] * 3,
            out_specs=[VMEM] * 9,
            scratch_shapes=[rows_v, rows_v, rows_v, pltpu.VMEM((4 * top_k, LANES), F32), pltpu.VMEM((n_dev, 4 * top_k, LANES), F32), expert_v, expert_v,
                            pltpu.VMEM((n_dev, tok, width), F32), *Reduce.scratch(tok, width),
                            pltpu.VMEM((tok, width), BF16), *weights_v, w_sems, *dma_sems(count)],
            compiler_params=remote_params(0), name="first",
        )(x_in, dy_out, idx_a.T, gate_a.T, idx_b.T, gate_b.T, w1_a, w3_a, w2_a)

        part_v = pltpu.VMEM((n_dev, tok, width), F32)

        def backward(x_all, d_all, s, g, rel, w1, w3, w2):
            return pl.pallas_call(
                functools.partial(backward_kernel, dims),
                out_shape=(sds((local, width, inner), F32), sds((local, width, inner), F32),
                           sds((local, inner, width), F32), part_all, dg_all),
                in_specs=[VMEM] * 5 + [ANY] * 3,
                out_specs=[ANY] * 4 + [VMEM],
                scratch_shapes=[expert_v, expert_v, expert_v, pltpu.VMEM((local, n_dev, LANES), F32), *weights_v,
                                *[pltpu.VMEM((GROUPED, inner, width), BF16)] * 2, pltpu.VMEM((GROUPED, width, inner), BF16),
                                *[pltpu.VMEM((2, GROUPED, width, inner), F32)] * 2,
                                pltpu.VMEM((2, GROUPED, inner, width), F32), part_v, w_sems,
                                pltpu.SemaphoreType.DMA((3, 2)), pltpu.SemaphoreType.DMA((n_dev,))],
                compiler_params=pltpu.CompilerParams(vmem_limit_bytes=VMEM_LIMIT), name="backward",
                cost_estimate=pl.CostEstimate(flops=18 * local * n_dev * cap * width * inner, transcendentals=0,
                                              bytes_accessed=18 * local * width * inner),
            )(x_all, d_all, s, g, rel, w1, w3, w2)

        *grads_b, part_b, dg_b = backward(mid_all, dy_all, sb, gb, relb, w1_b, w3_b, w2_b)

        count = 2 * Gather.COPIES + 2 * Reduce.COPIES + 1
        sums = sds((tok, width), F32)
        chip_sums = pltpu.VMEM((n_dev // 2, tok, width), F32)
        x_again, dmid_all, dmid_own, dgate_b, own_x, right_x, opp_x, left_x = pl.pallas_call(
            functools.partial(middle_kernel, dims),
            out_shape=(rows_all, rows_all, own, sds((top_k, LANES), F32), sums, sums, sums, sums),
            in_specs=[VMEM] * 5 + [ANY] * 5,
            out_specs=[ANY] + [VMEM] * 7,
            scratch_shapes=[part_v, rows_v, pltpu.SemaphoreType.DMA((3,)),
                            pltpu.VMEM((2, n_dev // 2, tok, width), F32), chip_sums, rows_v, rows_v, expert_v, expert_v,
                            *Reduce.scratch(tok, width), *Reduce.scratch(top_k, LANES), pltpu.VMEM((tok, width), BF16),
                            *weights_v, w_sems, *dma_sems(count)],
            compiler_params=remote_params(1), name="middle",
        )(dg_b, dy_out, x_in, sb, gb, part_b, mid_all, w1_b, w3_b, w2_b)

        def shift(rows, hop):
            return lax.ppermute(rows, "ep", [(i, (i + 2 * hop) % n_dev) for i in range(n_dev)])

        left_x, opp_x, right_x = shift(right_x, 1), shift(opp_x, 2), shift(left_x, 3)
        *grads_a, part_a, dg_a = backward(x_again, dmid_all, sa, ga, rela, w1_a, w3_a, w2_a)

        dx_in, dgate_a = pl.pallas_call(
            functools.partial(last_kernel, dims),
            out_shape=(own, sds((top_k, LANES), F32)),
            in_specs=[VMEM] * 2 + [ANY],
            out_specs=[VMEM] * 2,
            scratch_shapes=[part_v, pltpu.SemaphoreType.DMA((1,)), *Reduce.scratch(tok, width),
                            *Reduce.scratch(top_k, LANES), *dma_sems(2 * Reduce.COPIES)],
            compiler_params=remote_params(2), name="last",
        )(dg_a, dmid_own, part_a)
        gates = sds((top_k, tok), F32)
        x_out, dx_in, dgate_a, dgate_b = pl.pallas_call(
            final_kernel, out_shape=(own, own, gates, gates), in_specs=[VMEM] * 8, out_specs=[VMEM] * 4, name="final",
            compiler_params=pltpu.CompilerParams(vmem_limit_bytes=SMALL_VMEM_LIMIT),
        )(mid_own, own_x, left_x, opp_x, right_x, dx_in, dgate_a, dgate_b)
        return (x_out, dx_in, *grads_a, *grads_b, dgate_a.T, dgate_b.T)

    return jax.shard_map(device_program, mesh=mesh, in_specs=(tok_spec,) * 6 + (w_spec,) * 6, out_specs=(tok_spec,) * 10, check_vma=False)
```

```python
import functools

import jax
import jax.numpy as jnp
from jax import lax
from jax.experimental import pallas as pl
from jax.experimental.pallas import tpu as pltpu
from jax.sharding import PartitionSpec as P

BF16 = jnp.bfloat16
F32 = jnp.float32
MESH = pl.DeviceIdType.MESH
LANES = 128
CAP_FACTOR = 4
BF16_MAX = 3.3895313892515355e38
GROUPED = 2
FORWARD_GROUPED = 4
MIB = 1024 * 1024
ALL_VMEM = 64 * MIB - 64 * 1024
VMEM = pl.BlockSpec(memory_space=pltpu.VMEM)
HBM = pl.BlockSpec(memory_space=pltpu.HBM)


def mm(lhs, rhs):
    return jnp.dot(lhs, rhs, preferred_element_type=F32)


def mm_tn(lhs, rhs):
    return lax.dot_general(lhs, rhs, (((0,), (0,)), ((), ())), preferred_element_type=F32)


def iota(shape, dim):
    return lax.broadcasted_iota(jnp.int32, shape, dim)


def routing_maps(me, meta, layer, s_ref, g_ref, rel_ref, top_k, local):
    n_dev = meta.shape[0]
    base = (me * local).astype(F32)
    row = 2 * layer * top_k
    rel_ref[...] = meta[:, row : row + top_k, :] - base
    shape = (local, n_dev, LANES)
    expert = iota(shape, 0).astype(F32)
    hit, gate = jnp.zeros(shape, F32), jnp.zeros(shape, F32)
    for j in range(top_k):
        match = (meta[:, row + j, :] - base)[None] == expert
        hit = jnp.where(match, 1.0, hit)
        gate = jnp.where(match, meta[:, row + top_k + j, :][None], gate)
    hit = hit.reshape(local * n_dev, LANES)
    earlier = (iota((LANES, LANES), 0) < iota((LANES, LANES), 1)).astype(F32).astype(BF16)
    slot = jnp.where(hit > 0.0, mm(hit.astype(BF16), earlier), -1.0)
    s_ref[...] = slot.reshape(shape)
    g_ref[...] = gate


def row_picks(s_map, d, tok, n_dev, cap):
    pairs, lanes = s_map.shape
    n_rows = pairs // n_dev * cap
    spread = iota((n_rows, pairs), 1) == iota((n_rows, pairs), 0) // cap * n_dev + d
    slot = mm(spread.astype(F32).astype(BF16), s_map.astype(BF16))
    return jnp.where(slot == (iota((n_rows, lanes), 0) % cap).astype(F32), 1.0, 0.0).astype(BF16)[:, :tok]


def fill_rows(s_map, d, sources, cap):
    picks = row_picks(s_map, d, sources[0][0].shape[1], sources[0][0].shape[0], cap)
    for rows, out in sources:
        out[d] = mm(picks, rows[d]).astype(BF16).reshape(out.shape[1:])


def limbs(gate):
    hi = jnp.minimum(gate, BF16_MAX).astype(BF16)
    rest = gate - hi.astype(F32)
    mid = rest.astype(BF16)
    return hi, mid, (rest - mid.astype(F32)).astype(BF16)


def scatter_lhs(s_map, g_map, tok):
    stack = [s_map.T[:tok].astype(BF16)]
    if g_map is not None:
        stack += [limb.T[:tok].astype(BF16) for limb in (x.astype(F32) for x in limbs(g_map))]
    return jnp.concatenate(stack, axis=0)


def token_sums(stack, d, out_rows, tok, cap):
    pairs = stack.shape[1]
    n_rows = out_rows.shape[0]
    spread = iota((pairs, n_rows), 0) == iota((pairs, n_rows), 1) // cap * 8 + d
    maps = mm(stack, spread.astype(F32).astype(BF16))
    match = maps[:tok] == (iota((tok, n_rows), 1) % cap).astype(F32)
    if stack.shape[0] == tok:
        return mm(jnp.where(match, 1.0, 0.0).astype(BF16), out_rows)
    terms = (stack.shape[0] - tok) // tok
    lhs = [jnp.where(match, maps[(i + 1) * tok : (i + 2) * tok], 0.0).astype(BF16) for i in range(terms)]
    sums = mm(jnp.concatenate(lhs, axis=0), out_rows)
    total = sums[:tok]
    for i in range(1, terms):
        total = total + sums[i * tok : (i + 1) * tok]
    return total


class Links:
    def __init__(self, n_dev, send_sems, recv_sems):
        me = lax.axis_index("ep")
        self.n = n_dev
        self.me = me
        self.core = lax.rem(me, 2)
        self.partner = me + 1 - 2 * self.core
        self.right = lax.rem(me + 2, n_dev)
        self.left = lax.rem(me + n_dev - 2, n_dev)
        self.opp = lax.rem(me + 4, n_dev)
        self.send_sems, self.recv_sems = send_sems, recv_sems
        self.used = 0
        self.started = []

    def greet(self):
        barrier = pltpu.get_barrier_semaphore()
        for peer in (self.partner, self.left, self.right):
            pl.semaphore_signal(barrier, inc=1, device_id={"ep": peer}, device_id_type=MESH)
        pl.semaphore_wait(barrier, 3)

    def copy(self, src, dst, peer):
        slot = self.used
        self.used += 1
        rdma = pltpu.make_async_remote_copy(
            src_ref=src, dst_ref=dst, send_sem=self.send_sems.at[slot], recv_sem=self.recv_sems.at[slot],
            device_id={"ep": peer}, device_id_type=MESH)
        rdma.start()
        self.started.append(rdma)
        return rdma

    def drain(self):
        for rdma in self.started:
            rdma.wait_send()


class Gather:
    COPIES = 9

    def __init__(self, links, own, full):
        k, self.k, self.full = links, links, full
        self.half = own.shape[0] // 2
        self.to_right = k.copy(own, full.at[k.me], k.right)
        self.to_left = k.copy(own, full.at[k.me], k.left)
        self.to_partner = k.copy(own, full.at[k.me], k.partner)

    def pass_on(self):
        k, full, half = self.k, self.full, self.half
        self.to_right.wait_recv()
        self.far_a = k.copy(full.at[k.left, pl.ds(0, half)], full.at[k.left, pl.ds(0, half)], k.right)
        self.side_a = k.copy(full.at[k.left], full.at[k.left], k.partner)
        self.to_left.wait_recv()
        self.far_b = k.copy(full.at[k.right, pl.ds(half, half)], full.at[k.right, pl.ds(half, half)], k.left)
        self.side_b = k.copy(full.at[k.right], full.at[k.right], k.partner)

    def pass_far(self):
        k, full, half = self.k, self.full, self.half
        self.far_a.wait_recv()
        self.last_a = k.copy(full.at[k.opp, pl.ds(0, half)], full.at[k.opp, pl.ds(0, half)], k.partner)
        self.far_b.wait_recv()
        self.last_b = k.copy(full.at[k.opp, pl.ds(half, half)], full.at[k.opp, pl.ds(half, half)], k.partner)

    def wait_partner(self):
        self.to_partner.wait_recv()

    def wait_sides(self):
        self.side_a.wait_recv()
        self.side_b.wait_recv()

    def wait_last(self):
        self.last_a.wait_recv()
        self.last_b.wait_recv()

    def finish(self):
        self.wait_partner()
        self.wait_sides()
        self.wait_last()


class Reduce:
    COPIES = 10

    @staticmethod
    def scratch(rows, width):
        return [pltpu.VMEM((4, rows, width), F32), pltpu.VMEM((4, rows, width), F32), pltpu.VMEM((3, rows, width), F32)]

    def __init__(self, links, part, bufs, split=True):
        self.k, self.part = links, part
        self.near, self.mine, self.got = bufs
        rows = part.shape[1]
        self.rows = rows
        self.half = rows // 2 if split else rows
        self.side = {}

    def block(self, hop, core):
        k = self.k
        return lax.rem(k.me - k.core + 2 * hop, k.n) + core

    def start_side(self, hop):
        k = self.k
        self.side[hop] = k.copy(self.part.at[self.block(hop, 1 - k.core)], self.near.at[hop], k.partner)

    def start(self):
        for hop in (2, 1, 3, 0):
            self.start_side(hop)

    def add(self, hop, lo, hi, extra=None):
        own = self.part[self.block(hop, self.k.core), lo:hi, :]
        total = own + self.near[hop, lo:hi, :]
        if extra is not None:
            total = total + extra
        self.mine[hop, lo:hi, :] = total

    def far(self):
        k, half, rows = self.k, self.half, self.rows
        self.side[2].wait_recv()
        self.add(2, 0, rows)
        a = pl.ds(0, half)
        self.far_a = k.copy(self.mine.at[2, a], self.got.at[2, a], k.right)
        if half < rows:
            b = pl.ds(half, rows - half)
            self.far_b = k.copy(self.mine.at[2, b], self.got.at[2, b], k.left)

    def near_sends(self):
        k, half, rows = self.k, self.half, self.rows
        self.side[1].wait_recv()
        if half < rows:
            b = pl.ds(half, rows - half)
            self.add(1, half, rows)
            self.right_b = k.copy(self.mine.at[1, b], self.got.at[0, b], k.right)
        self.side[3].wait_recv()
        self.add(3, 0, half)
        a = pl.ds(0, half)
        self.left_a = k.copy(self.mine.at[3, a], self.got.at[1, a], k.left)

    def relay(self):
        k, half, rows = self.k, self.half, self.rows
        a = pl.ds(0, half)
        self.far_a.wait_recv()
        self.add(1, 0, half, self.got[2, :half, :])
        self.right_a = k.copy(self.mine.at[1, a], self.got.at[0, a], k.right)
        if half < rows:
            b = pl.ds(half, rows - half)
            self.far_b.wait_recv()
            self.add(3, half, rows, self.got[2, half:, :])
            self.left_b = k.copy(self.mine.at[3, b], self.got.at[1, b], k.left)

    def result(self):
        half, rows = self.half, self.rows
        self.side[0].wait_recv()
        if half < rows:
            self.right_b.wait_recv()
        self.left_a.wait_recv()
        self.right_a.wait_recv()
        if half < rows:
            self.left_b.wait_recv()
        return self.part[self.k.me] + self.near[0] + self.got[0] + self.got[1]


def load_weights(pairs, sems, local):
    def start(e, carry):
        for i, (src, dst) in enumerate(pairs):
            pltpu.make_async_copy(src.at[e], dst.at[e], sems.at[i, e]).start()
        return carry
    lax.fori_loop(0, local, start, 0)


def wait_weights(pairs, sems, e):
    for i, (src, dst) in enumerate(pairs):
        pltpu.make_async_copy(src.at[e], dst.at[e], sems.at[i, e]).wait()


def forward_experts(weights, ready, u_ref, o_ref, cap, first, last):
    n_dev, _, _, width = u_ref.shape
    few = min(FORWARD_GROUPED, last - first)

    def step(g, carry):
        experts = [first + g * few + i for i in range(few)]
        for e in experts:
            ready(e)
        w_gate, w_up, w_down = weights
        rows = [u_ref[:, e].reshape(n_dev * cap, width) for e in experts]
        pre = [(mm(u, w_gate[e]), mm(u, w_up[e])) for u, e in zip(rows, experts)]
        hidden = [(gate * jax.nn.sigmoid(gate) * up).astype(BF16) for gate, up in pre]
        for h, e in zip(hidden, experts):
            o_ref[:, e] = mm(h, w_down[e]).astype(BF16).reshape(n_dev, cap, width)
        return carry
    lax.fori_loop(0, (last - first) // few, step, 0)


def first_kernel(dims, x_ref, dy_ref, idx_a, gate_a, idx_b, gate_b, w1, w3, w2,
                 dy_all, mid_all, mid_own, sa, ga, rela, sb, gb, relb,
                 x_all, y_all, m_all, meta_ref, meta_all, u_ref, o_ref, part, near, mine, got, mid_buf, w1_v, w3_v, w2_v,
                 w_sems, out_sem, send_sems, recv_sems):
    n_dev, tok, width, local, cap, top_k = dims
    pairs = ((w1, w1_v), (w3, w3_v), (w2, w2_v))
    load_weights(pairs, w_sems, local)
    meta_ref[...] = jnp.full(meta_ref.shape, -1.0, F32)
    for i, ref in enumerate((idx_a, gate_a, idx_b, gate_b)):
        meta_ref[i * top_k : (i + 1) * top_k, :tok] = ref[...].astype(F32)
    links = Links(n_dev, send_sems, recv_sems)
    me = links.me
    links.greet()
    meta_g = Gather(links, meta_ref, meta_all)
    x_g = Gather(links, x_ref, x_all)
    meta_all[me] = meta_ref[...]
    x_all[me] = x_ref[...]
    y_all[me] = dy_ref[...]
    meta_g.pass_on()
    x_g.pass_on()
    y_g = Gather(links, dy_ref, y_all)
    meta_g.pass_far()
    meta_g.finish()
    meta = meta_all[...]
    routing_maps(me, meta, 0, sa, ga, rela, top_k, local)
    s_map = sa[...].reshape(local * n_dev, LANES)

    def rows_of(d):
        fill_rows(s_map, d, ((x_all, u_ref),), cap)

    rows_of(me)
    rows_of(links.left)
    rows_of(links.right)
    x_g.wait_partner()
    rows_of(links.partner)
    x_g.pass_far()
    x_g.wait_sides()
    side = 1 - 2 * links.core
    rows_of(links.left + side)
    rows_of(links.right + side)
    rows_of(links.opp)
    y_g.pass_on()
    routing_maps(me, meta, 1, sb, gb, relb, top_k, local)
    x_g.wait_last()
    rows_of(links.opp + side)
    forward_experts((w1_v, w3_v, w2_v), lambda e: wait_weights(pairs, w_sems, e), u_ref, o_ref, cap, 0, local)
    y_g.pass_far()
    stack = scatter_lhs(s_map, ga[...].reshape(local * n_dev, LANES), tok)
    red = Reduce(links, part, (near, mine, got))

    def sums_of(d):
        part[d] = token_sums(stack, d, o_ref[d].reshape(local * cap, width), tok, cap)

    sums_of(red.block(2, 1 - links.core))
    red.start_side(2)
    sums_of(red.block(2, links.core))
    for hop in (1, 3, 0):
        sums_of(red.block(hop, 1 - links.core))
        red.start_side(hop)
    red.far()
    sums_of(red.block(1, links.core))
    sums_of(red.block(3, links.core))
    red.near_sends()
    sums_of(red.block(0, links.core))
    red.relay()
    y_g.finish()
    y_store = pltpu.make_async_copy(y_all, dy_all, out_sem.at[0])
    y_store.start()
    x_mid = (x_ref[...].astype(F32) + red.result()).astype(BF16)
    mid_buf[...] = x_mid
    mid_own[...] = x_mid
    m_all[me] = x_mid
    m_g = Gather(links, mid_buf, m_all)
    m_g.pass_on()
    m_g.pass_far()
    m_g.finish()
    mid_all[...] = m_all[...]
    y_store.wait()
    links.drain()


def backward_kernel(dims, x_all, dy_all, s_ref, g_ref, rel_ref, w1, w3, w2,
                    dw1, dw3, dw2, part, dgate,
                    u_ref, y_ref, dg_ref, w1_v, w3_v, w2_v, w1_t, w3_t, w2_t, dw1_v, dw3_v, dw2_v, part_v,
                    w_sems, out_sems, part_sems):
    n_dev, tok, width, local, cap, top_k = dims
    pairs = ((w1, w1_v), (w3, w3_v), (w2, w2_v))
    load_weights(pairs, w_sems, local)
    n_rows = n_dev * cap
    outs = ((dw1_v, dw1), (dw3_v, dw3), (dw2_v, dw2))
    s_map = s_ref[...].reshape(local * n_dev, LANES)

    for d in range(n_dev):
        fill_rows(s_map, d, ((x_all, u_ref), (dy_all, y_ref)), cap)

    def store(g, i, slot):
        src, dst = outs[i]
        return pltpu.make_async_copy(src.at[slot], dst.at[pl.ds(g * GROUPED, GROUPED)], out_sems.at[i, slot])

    def step(g, carry):
        slot = lax.rem(g, 2)
        experts = [g * GROUPED + i for i in range(GROUPED)]
        each = range(GROUPED)
        for e in experts:
            wait_weights(pairs, w_sems, e)

        @pl.when(g >= 2)
        def _():
            for i in range(3):
                store(g - 2, i, slot).wait()
        for i, e in enumerate(experts):
            w2_t[i] = w2_v[e].T
        u = [u_ref[:, e].reshape(n_rows, width) for e in experts]
        dy = [y_ref[:, e].reshape(n_rows, width) for e in experts]
        holds = [s_ref[e][:, None, :] == iota((n_dev, cap, LANES), 1).astype(F32) for e in experts]
        gate_row = [jnp.sum(jnp.where(holds[i], g_ref[e][:, None, :], 0.0), axis=2, keepdims=True).reshape(n_rows, 1)
                    for i, e in enumerate(experts)]
        q = [(gate_row[i] * dy[i].astype(F32)).astype(BF16) for i in each]
        pre = [(mm(u[i], w1_v[e]), mm(u[i], w3_v[e])) for i, e in enumerate(experts)]
        for i, e in enumerate(experts):
            w1_t[i] = w1_v[e].T
            w3_t[i] = w3_v[e].T
        d_hidden = [mm(q[i], w2_t[i]) for i in each]
        sig = [jax.nn.sigmoid(a) for a, _ in pre]
        act = [pre[i][0] * sig[i] for i in each]
        hidden = [(act[i] * pre[i][1]).astype(BF16) for i in each]
        out = [mm(hidden[i], w2_v[e]).astype(BF16) for i, e in enumerate(experts)]
        for i in each:
            dw2_v[slot, i] = mm_tn(hidden[i], q[i])
        d_gate = [(d_hidden[i] * pre[i][1] * sig[i] * (1.0 + pre[i][0] * (1.0 - sig[i]))).astype(BF16) for i in each]
        d_up = [(d_hidden[i] * act[i]).astype(BF16) for i in each]
        for i, e in enumerate(experts):
            dg_row = jnp.sum(dy[i].astype(F32) * out[i].astype(F32), axis=1, keepdims=True).reshape(n_dev, cap, 1)
            dg_ref[e] = jnp.sum(jnp.where(holds[i], dg_row, 0.0), axis=1)
        for i, e in enumerate(experts):
            du = (mm(d_gate[i], w1_t[i]) + mm(d_up[i], w3_t[i])).astype(BF16)
            y_ref[:, e] = du.reshape(n_dev, cap, width)
        for i in each:
            dw1_v[slot, i] = mm_tn(u[i], d_gate[i])
            dw3_v[slot, i] = mm_tn(u[i], d_up[i])
        for i in range(3):
            store(g, i, slot).start()
        return carry
    steps = local // GROUPED
    lax.fori_loop(0, steps, step, 0)

    stack = scatter_lhs(s_map, None, tok)
    for d in range(n_dev):
        part_v[d] = token_sums(stack, d, y_ref[d].reshape(local * cap, width), tok, cap)
        pltpu.make_async_copy(part_v.at[d], part.at[d], part_sems.at[d]).start()
    for d in range(n_dev):
        total = jnp.zeros((top_k, LANES), F32)
        for i in range(local):
            total = jnp.where(rel_ref[d] == float(i), dg_ref[i, d : d + 1, :], total)
        dgate[d] = total
    for g in (steps - 2, steps - 1):
        for i in range(3):
            store(g, i, g % 2).wait()
    for d in range(n_dev):
        pltpu.make_async_copy(part_v.at[d], part.at[d], part_sems.at[d]).wait()


def middle_kernel(dims, dg_part, dy_ref, x_ref, sb, gb, part_in, mid_in, w1, w3, w2,
                  x_again, dmid_all, dmid_own, dgate, own_x, right_x, opp_x, left_x,
                  part_b, mid_all, in_sems, part_x, near_x, d_all, x_all, u_ref, near, mine, got, dg_near, dg_mine, dg_got, d_buf, w1_v, w3_v, w2_v,
                  w_sems, send_sems, recv_sems):
    n_dev, tok, width, local, cap, top_k = dims
    pairs = ((w1, w1_v), (w3, w3_v), (w2, w2_v))
    part_load = pltpu.make_async_copy(part_in, part_b, in_sems.at[0])
    mid_load = pltpu.make_async_copy(mid_in, mid_all, in_sems.at[1])
    part_load.start()
    mid_load.start()
    load_weights(pairs, w_sems, local)
    links = Links(n_dev, send_sems, recv_sems)
    me = links.me
    links.greet()
    part_load.wait()
    red = Reduce(links, part_b, (near, mine, got))
    dg = Reduce(links, dg_part, (dg_near, dg_mine, dg_got), split=False)
    s_map = sb[...].reshape(local * n_dev, LANES)

    def rows_of(d):
        fill_rows(s_map, d, ((mid_all, u_ref),), cap)

    red.start()
    dg.start()
    mid_load.wait()
    for d in range(2):
        rows_of(d)
    red.far()
    red.near_sends()
    dg.far()
    dg.near_sends()
    for d in range(2, n_dev):
        rows_of(d)
    red.relay()
    dg.relay()
    x_g = Gather(links, x_ref, x_all)
    x_all[me] = x_ref[...]
    half = local // 2 // FORWARD_GROUPED * FORWARD_GROUPED
    forward_experts((w1_v, w3_v, w2_v), lambda e: wait_weights(pairs, w_sems, e), u_ref, u_ref, cap, 0, half)
    dx = (dy_ref[...].astype(F32) + red.result()).astype(BF16)
    d_buf[...] = dx
    dmid_own[...] = dx
    d_all[me] = dx
    d_g = Gather(links, d_buf, d_all)
    x_g.pass_on()
    forward_experts((w1_v, w3_v, w2_v), lambda e: wait_weights(pairs, w_sems, e), u_ref, u_ref, cap, half, local)
    d_g.pass_on()
    x_g.pass_far()
    stack = scatter_lhs(s_map, gb[...].reshape(local * n_dev, LANES), tok)
    for d in range(n_dev):
        part_x[d % 2, d // 2] = token_sums(stack, d, u_ref[d].reshape(local * cap, width), tok, cap)
    side_x = links.copy(part_x.at[1 - links.core], near_x, links.partner)
    d_g.pass_far()
    x_g.finish()
    x_store = pltpu.make_async_copy(x_all, x_again, in_sems.at[2])
    x_store.start()
    side_x.wait_recv()
    for hop, out in enumerate((own_x, right_x, opp_x, left_x)):
        chip = lax.rem((me - links.core) // 2 + hop, n_dev // 2)
        out[...] = part_x[links.core, chip] + near_x[chip]
    dgate[...] = dg.result()
    d_g.finish()
    dmid_all[...] = d_all[...]
    x_store.wait()
    links.drain()


def final_kernel(mid_ref, own_x, left_x, opp_x, right_x, dx_ref, dga_ref, dgb_ref, x_out, dx_out, dga_out, dgb_out):
    total = own_x[...] + left_x[...] + opp_x[...] + right_x[...]
    x_out[...] = (mid_ref[...].astype(F32) + total).astype(BF16)
    dx_out[...] = dx_ref[...]
    tok = dga_out.shape[1]
    dga_out[...] = dga_ref[:, :tok]
    dgb_out[...] = dgb_ref[:, :tok]


def last_kernel(dims, dg_part, dmid_ref, part_in, dx_out, dgate,
                part_a, in_sem, near, mine, got, dg_near, dg_mine, dg_got, send_sems, recv_sems):
    part_load = pltpu.make_async_copy(part_in, part_a, in_sem.at[0])
    part_load.start()
    links = Links(dims[0], send_sems, recv_sems)
    links.greet()
    part_load.wait()
    red = Reduce(links, part_a, (near, mine, got))
    dg = Reduce(links, dg_part, (dg_near, dg_mine, dg_got), split=False)
    red.start()
    dg.start()
    red.far()
    red.near_sends()
    dg.far()
    dg.near_sends()
    red.relay()
    dg.relay()
    dx_out[...] = (dmid_ref[...].astype(F32) + red.result()).astype(BF16)
    dgate[...] = dg.result()
    links.drain()


def remote_params(ident):
    return pltpu.CompilerParams(collective_id=ident, has_side_effects=True, vmem_limit_bytes=ALL_VMEM)


def dma_sems(count):
    return [pltpu.SemaphoreType.DMA((count,)), pltpu.SemaphoreType.DMA((count,))]


def solution(mesh):
    n_dev = mesh.shape["ep"]
    tok_spec = P(("dp", "ep"))
    w_spec = P("ep")

    def device_program(x_in, idx_a, idx_b, gate_a, gate_b, dy_out, w1_a, w3_a, w2_a, w1_b, w3_b, w2_b):
        tok, top_k = idx_a.shape
        width = x_in.shape[1]
        local, _, inner = w1_a.shape
        cap = CAP_FACTOR * tok * top_k // (local * n_dev)
        dims = (n_dev, tok, width, local, cap, top_k)
        sds = jax.ShapeDtypeStruct
        rows_all = sds((n_dev, tok, width), BF16)
        part_all = sds((n_dev, tok, width), F32)
        dg_all = sds((n_dev, top_k, LANES), F32)
        map_s = sds((local, n_dev, LANES), F32)
        own = sds((tok, width), BF16)

        weights_v = [pltpu.VMEM((local, width, inner), BF16)] * 2 + [pltpu.VMEM((local, inner, width), BF16)]
        w_sems = pltpu.SemaphoreType.DMA((3, local))
        rows_v = pltpu.VMEM((n_dev, tok, width), BF16)
        expert_v = pltpu.VMEM((n_dev, local, cap, width), BF16)

        count = 4 * Gather.COPIES + Reduce.COPIES
        dy_all, mid_all, mid_own, sa, ga, rela, sb, gb, relb = pl.pallas_call(
            functools.partial(first_kernel, dims),
            out_shape=(rows_all, rows_all, own, map_s, map_s, dg_all, map_s, map_s, dg_all),
            in_specs=[VMEM] * 6 + [HBM] * 3,
            out_specs=[HBM] + [VMEM] * 8,
            scratch_shapes=[rows_v, rows_v, rows_v, pltpu.VMEM((4 * top_k, LANES), F32), pltpu.VMEM((n_dev, 4 * top_k, LANES), F32), expert_v, expert_v,
                            pltpu.VMEM((n_dev, tok, width), F32), *Reduce.scratch(tok, width),
                            pltpu.VMEM((tok, width), BF16), *weights_v, w_sems, pltpu.SemaphoreType.DMA((1,)), *dma_sems(count)],
            compiler_params=remote_params(0), name="first",
        )(x_in, dy_out, idx_a.T, gate_a.T, idx_b.T, gate_b.T, w1_a, w3_a, w2_a)

        part_v = pltpu.VMEM((n_dev, tok, width), F32)

        def backward(x_all, d_all, s, g, rel, w1, w3, w2):
            return pl.pallas_call(
                functools.partial(backward_kernel, dims),
                out_shape=(sds((local, width, inner), F32), sds((local, width, inner), F32),
                           sds((local, inner, width), F32), part_all, dg_all),
                in_specs=[VMEM] * 5 + [HBM] * 3,
                out_specs=[HBM] * 4 + [VMEM],
                scratch_shapes=[expert_v, expert_v, pltpu.VMEM((local, n_dev, LANES), F32), *weights_v,
                                *[pltpu.VMEM((GROUPED, inner, width), BF16)] * 2, pltpu.VMEM((GROUPED, width, inner), BF16),
                                *[pltpu.VMEM((2, GROUPED, width, inner), F32)] * 2,
                                pltpu.VMEM((2, GROUPED, inner, width), F32), part_v, w_sems,
                                pltpu.SemaphoreType.DMA((3, 2)), pltpu.SemaphoreType.DMA((n_dev,))],
                compiler_params=pltpu.CompilerParams(vmem_limit_bytes=ALL_VMEM), name="backward",
                cost_estimate=pl.CostEstimate(flops=18 * local * n_dev * cap * width * inner, transcendentals=0,
                                              bytes_accessed=18 * local * width * inner),
            )(x_all, d_all, s, g, rel, w1, w3, w2)

        *grads_b, part_b, dg_b = backward(mid_all, dy_all, sb, gb, relb, w1_b, w3_b, w2_b)

        count = 2 * Gather.COPIES + 2 * Reduce.COPIES + 1
        sums = sds((tok, width), F32)
        chip_sums = pltpu.VMEM((n_dev // 2, tok, width), F32)
        x_again, dmid_all, dmid_own, dgate_b, own_x, right_x, opp_x, left_x = pl.pallas_call(
            functools.partial(middle_kernel, dims),
            out_shape=(rows_all, rows_all, own, sds((top_k, LANES), F32), sums, sums, sums, sums),
            in_specs=[VMEM] * 5 + [HBM] * 5,
            out_specs=[HBM] + [VMEM] * 7,
            scratch_shapes=[part_v, rows_v, pltpu.SemaphoreType.DMA((3,)),
                            pltpu.VMEM((2, n_dev // 2, tok, width), F32), chip_sums, rows_v, rows_v, expert_v,
                            *Reduce.scratch(tok, width), *Reduce.scratch(top_k, LANES), pltpu.VMEM((tok, width), BF16),
                            *weights_v, w_sems, *dma_sems(count)],
            compiler_params=remote_params(1), name="middle",
        )(dg_b, dy_out, x_in, sb, gb, part_b, mid_all, w1_b, w3_b, w2_b)

        def shift(rows, hop):
            return lax.ppermute(rows, "ep", [(i, (i + 2 * hop) % n_dev) for i in range(n_dev)])

        left_x, opp_x, right_x = shift(right_x, 1), shift(opp_x, 2), shift(left_x, 3)
        *grads_a, part_a, dg_a = backward(x_again, dmid_all, sa, ga, rela, w1_a, w3_a, w2_a)

        dx_in, dgate_a = pl.pallas_call(
            functools.partial(last_kernel, dims),
            out_shape=(own, sds((top_k, LANES), F32)),
            in_specs=[VMEM] * 2 + [HBM],
            out_specs=[VMEM] * 2,
            scratch_shapes=[part_v, pltpu.SemaphoreType.DMA((1,)), *Reduce.scratch(tok, width),
                            *Reduce.scratch(top_k, LANES), *dma_sems(2 * Reduce.COPIES)],
            compiler_params=remote_params(2), name="last",
        )(dg_a, dmid_own, part_a)
        gates = sds((top_k, tok), F32)
        x_out, dx_in, dgate_a, dgate_b = pl.pallas_call(
            final_kernel, out_shape=(own, own, gates, gates), in_specs=[VMEM] * 8, out_specs=[VMEM] * 4, name="final",
            compiler_params=pltpu.CompilerParams(vmem_limit_bytes=60 * MIB),
        )(mid_own, own_x, left_x, opp_x, right_x, dx_in, dgate_a, dgate_b)
        return (x_out, dx_in, *grads_a, *grads_b, dgate_a.T, dgate_b.T)

    return jax.shard_map(device_program, mesh=mesh, in_specs=(tok_spec,) * 6 + (w_spec,) * 6, out_specs=(tok_spec,) * 10, check_vma=False)
```

```python
import functools

import jax
import jax.numpy as jnp
from jax import lax
from jax.experimental import pallas as pl
from jax.experimental.pallas import tpu as pltpu
from jax.sharding import PartitionSpec as P

BF16 = jnp.bfloat16
F32 = jnp.float32
MESH = pl.DeviceIdType.MESH
LANES = 128
CAP_FACTOR = 4
BF16_MAX = 3.3895313892515355e38
GROUPED = 2
SLOTS = 3
FORWARD_GROUPED = 4
MIB = 1024 * 1024
ALL_VMEM = 64 * MIB - 64 * 1024
VMEM = pl.BlockSpec(memory_space=pltpu.VMEM)
HBM = pl.BlockSpec(memory_space=pltpu.HBM)


def mm(lhs, rhs):
    return jnp.dot(lhs, rhs, preferred_element_type=F32)


def mm_tn(lhs, rhs):
    return lax.dot_general(lhs, rhs, (((0,), (0,)), ((), ())), preferred_element_type=F32)


def iota(shape, dim):
    return lax.broadcasted_iota(jnp.int32, shape, dim)


def routing_maps(me, meta, layer, s_ref, g_ref, rel_ref, top_k, local):
    n_dev = meta.shape[0]
    base = (me * local).astype(F32)
    row = 2 * layer * top_k
    rel_ref[...] = meta[:, row : row + top_k, :] - base
    shape = (local, n_dev, LANES)
    expert = iota(shape, 0).astype(F32)
    hit, gate = jnp.zeros(shape, F32), jnp.zeros(shape, F32)
    for j in range(top_k):
        match = (meta[:, row + j, :] - base)[None] == expert
        hit = jnp.where(match, 1.0, hit)
        gate = jnp.where(match, meta[:, row + top_k + j, :][None], gate)
    hit = hit.reshape(local * n_dev, LANES)
    earlier = (iota((LANES, LANES), 0) < iota((LANES, LANES), 1)).astype(F32).astype(BF16)
    slot = jnp.where(hit > 0.0, mm(hit.astype(BF16), earlier), -1.0)
    s_ref[...] = slot.reshape(shape)
    g_ref[...] = gate


def row_picks(s_map, d, tok, n_dev, cap):
    pairs, lanes = s_map.shape
    n_rows = pairs // n_dev * cap
    spread = iota((n_rows, pairs), 1) == iota((n_rows, pairs), 0) // cap * n_dev + d
    slot = mm(spread.astype(F32).astype(BF16), s_map.astype(BF16))
    return jnp.where(slot == (iota((n_rows, lanes), 0) % cap).astype(F32), 1.0, 0.0).astype(BF16)[:, :tok]


def fill_rows(s_map, d, sources, cap):
    picks = row_picks(s_map, d, sources[0][0].shape[1], sources[0][0].shape[0], cap)
    for rows, out in sources:
        out[d] = mm(picks, rows[d]).astype(BF16).reshape(out.shape[1:])


def limbs(gate):
    hi = jnp.minimum(gate, BF16_MAX).astype(BF16)
    rest = gate - hi.astype(F32)
    mid = rest.astype(BF16)
    return hi, mid, (rest - mid.astype(F32)).astype(BF16)


def scatter_lhs(s_map, g_map, tok):
    stack = [s_map.T[:tok].astype(BF16)]
    if g_map is not None:
        stack += [limb.T[:tok].astype(BF16) for limb in (x.astype(F32) for x in limbs(g_map))]
    return jnp.concatenate(stack, axis=0)


def token_sums(stack, d, out_rows, tok, cap):
    pairs = stack.shape[1]
    n_rows = out_rows.shape[0]
    spread = iota((pairs, n_rows), 0) == iota((pairs, n_rows), 1) // cap * 8 + d
    maps = mm(stack, spread.astype(F32).astype(BF16))
    match = maps[:tok] == (iota((tok, n_rows), 1) % cap).astype(F32)
    if stack.shape[0] == tok:
        return mm(jnp.where(match, 1.0, 0.0).astype(BF16), out_rows)
    terms = (stack.shape[0] - tok) // tok
    lhs = [jnp.where(match, maps[(i + 1) * tok : (i + 2) * tok], 0.0).astype(BF16) for i in range(terms)]
    sums = mm(jnp.concatenate(lhs, axis=0), out_rows)
    total = sums[:tok]
    for i in range(1, terms):
        total = total + sums[i * tok : (i + 1) * tok]
    return total


class Links:
    def __init__(self, n_dev, send_sems, recv_sems):
        me = lax.axis_index("ep")
        self.n = n_dev
        self.me = me
        self.core = lax.rem(me, 2)
        self.partner = me + 1 - 2 * self.core
        self.right = lax.rem(me + 2, n_dev)
        self.left = lax.rem(me + n_dev - 2, n_dev)
        self.opp = lax.rem(me + 4, n_dev)
        self.send_sems, self.recv_sems = send_sems, recv_sems
        self.used = 0
        self.started = []

    def greet(self):
        barrier = pltpu.get_barrier_semaphore()
        for peer in (self.partner, self.left, self.right):
            pl.semaphore_signal(barrier, inc=1, device_id={"ep": peer}, device_id_type=MESH)
        pl.semaphore_wait(barrier, 3)

    def copy(self, src, dst, peer):
        slot = self.used
        self.used += 1
        rdma = pltpu.make_async_remote_copy(
            src_ref=src, dst_ref=dst, send_sem=self.send_sems.at[slot], recv_sem=self.recv_sems.at[slot],
            device_id={"ep": peer}, device_id_type=MESH)
        rdma.start()
        self.started.append(rdma)
        return rdma

    def drain(self):
        for rdma in self.started:
            rdma.wait_send()


class Gather:
    COPIES = 9

    def __init__(self, links, own, full):
        k, self.k, self.full = links, links, full
        self.half = own.shape[0] // 2
        self.to_right = k.copy(own, full.at[k.me], k.right)
        self.to_left = k.copy(own, full.at[k.me], k.left)
        self.to_partner = k.copy(own, full.at[k.me], k.partner)

    def pass_on(self):
        k, full, half = self.k, self.full, self.half
        self.to_right.wait_recv()
        self.far_a = k.copy(full.at[k.left, pl.ds(0, half)], full.at[k.left, pl.ds(0, half)], k.right)
        self.side_a = k.copy(full.at[k.left], full.at[k.left], k.partner)
        self.to_left.wait_recv()
        self.far_b = k.copy(full.at[k.right, pl.ds(half, half)], full.at[k.right, pl.ds(half, half)], k.left)
        self.side_b = k.copy(full.at[k.right], full.at[k.right], k.partner)

    def pass_far(self):
        k, full, half = self.k, self.full, self.half
        self.far_a.wait_recv()
        self.last_a = k.copy(full.at[k.opp, pl.ds(0, half)], full.at[k.opp, pl.ds(0, half)], k.partner)
        self.far_b.wait_recv()
        self.last_b = k.copy(full.at[k.opp, pl.ds(half, half)], full.at[k.opp, pl.ds(half, half)], k.partner)

    def wait_partner(self):
        self.to_partner.wait_recv()

    def wait_sides(self):
        self.side_a.wait_recv()
        self.side_b.wait_recv()

    def wait_last(self):
        self.last_a.wait_recv()
        self.last_b.wait_recv()

    def finish(self):
        self.wait_partner()
        self.wait_sides()
        self.wait_last()


class Reduce:
    COPIES = 10

    @staticmethod
    def scratch(rows, width):
        return [pltpu.VMEM((4, rows, width), F32), pltpu.VMEM((4, rows, width), F32), pltpu.VMEM((3, rows, width), F32)]

    def __init__(self, links, part, bufs, split=True):
        self.k, self.part = links, part
        self.near, self.mine, self.got = bufs
        rows = part.shape[1]
        self.rows = rows
        self.half = rows // 2 if split else rows
        self.side = {}

    def block(self, hop, core):
        k = self.k
        return lax.rem(k.me - k.core + 2 * hop, k.n) + core

    def start_side(self, hop):
        k = self.k
        self.side[hop] = k.copy(self.part.at[self.block(hop, 1 - k.core)], self.near.at[hop], k.partner)

    def start(self):
        for hop in (2, 1, 3, 0):
            self.start_side(hop)

    def add(self, hop, lo, hi, extra=None):
        own = self.part[self.block(hop, self.k.core), lo:hi, :]
        total = own + self.near[hop, lo:hi, :]
        if extra is not None:
            total = total + extra
        self.mine[hop, lo:hi, :] = total

    def far(self):
        k, half, rows = self.k, self.half, self.rows
        self.side[2].wait_recv()
        self.add(2, 0, rows)
        a = pl.ds(0, half)
        self.far_a = k.copy(self.mine.at[2, a], self.got.at[2, a], k.right)
        if half < rows:
            b = pl.ds(half, rows - half)
            self.far_b = k.copy(self.mine.at[2, b], self.got.at[2, b], k.left)

    def near_sends(self):
        k, half, rows = self.k, self.half, self.rows
        self.side[1].wait_recv()
        if half < rows:
            b = pl.ds(half, rows - half)
            self.add(1, half, rows)
            self.right_b = k.copy(self.mine.at[1, b], self.got.at[0, b], k.right)
        self.side[3].wait_recv()
        self.add(3, 0, half)
        a = pl.ds(0, half)
        self.left_a = k.copy(self.mine.at[3, a], self.got.at[1, a], k.left)

    def relay(self):
        k, half, rows = self.k, self.half, self.rows
        a = pl.ds(0, half)
        self.far_a.wait_recv()
        self.add(1, 0, half, self.got[2, :half, :])
        self.right_a = k.copy(self.mine.at[1, a], self.got.at[0, a], k.right)
        if half < rows:
            b = pl.ds(half, rows - half)
            self.far_b.wait_recv()
            self.add(3, half, rows, self.got[2, half:, :])
            self.left_b = k.copy(self.mine.at[3, b], self.got.at[1, b], k.left)

    def result(self):
        half, rows = self.half, self.rows
        self.side[0].wait_recv()
        if half < rows:
            self.right_b.wait_recv()
        self.left_a.wait_recv()
        self.right_a.wait_recv()
        if half < rows:
            self.left_b.wait_recv()
        return self.part[self.k.me] + self.near[0] + self.got[0] + self.got[1]


def load_weights(pairs, sems, local):
    def start(e, carry):
        for i, (src, dst) in enumerate(pairs):
            pltpu.make_async_copy(src.at[e], dst.at[e], sems.at[i, e]).start()
        return carry
    lax.fori_loop(0, local, start, 0)


def wait_weights(pairs, sems, e):
    for i, (src, dst) in enumerate(pairs):
        pltpu.make_async_copy(src.at[e], dst.at[e], sems.at[i, e]).wait()


def forward_experts(weights, ready, u_ref, o_ref, cap, first, last):
    n_dev, _, _, width = u_ref.shape
    few = min(FORWARD_GROUPED, last - first)

    def step(g, carry):
        experts = [first + g * few + i for i in range(few)]
        for e in experts:
            ready(e)
        w_gate, w_up, w_down = weights
        rows = [u_ref[:, e].reshape(n_dev * cap, width) for e in experts]
        pre = [(mm(u, w_gate[e]), mm(u, w_up[e])) for u, e in zip(rows, experts)]
        hidden = [(gate * jax.nn.sigmoid(gate) * up).astype(BF16) for gate, up in pre]
        for h, e in zip(hidden, experts):
            o_ref[:, e] = mm(h, w_down[e]).astype(BF16).reshape(n_dev, cap, width)
        return carry
    lax.fori_loop(0, (last - first) // few, step, 0)


def first_kernel(dims, x_ref, dy_ref, idx_a, gate_a, idx_b, gate_b, w1, w3, w2,
                 dy_all, mid_all, mid_own, sa, ga, rela, sb, gb, relb,
                 x_all, y_all, m_all, meta_ref, meta_all, u_ref, o_ref, part, near, mine, got, mid_buf, w1_v, w3_v, w2_v,
                 w_sems, out_sem, send_sems, recv_sems):
    n_dev, tok, width, local, cap, top_k = dims
    pairs = ((w1, w1_v), (w3, w3_v), (w2, w2_v))
    load_weights(pairs, w_sems, local)
    meta_ref[...] = jnp.full(meta_ref.shape, -1.0, F32)
    for i, ref in enumerate((idx_a, gate_a, idx_b, gate_b)):
        meta_ref[i * top_k : (i + 1) * top_k, :tok] = ref[...].astype(F32)
    links = Links(n_dev, send_sems, recv_sems)
    me = links.me
    links.greet()
    meta_g = Gather(links, meta_ref, meta_all)
    x_g = Gather(links, x_ref, x_all)
    meta_all[me] = meta_ref[...]
    x_all[me] = x_ref[...]
    y_all[me] = dy_ref[...]
    meta_g.pass_on()
    x_g.pass_on()
    y_g = Gather(links, dy_ref, y_all)
    meta_g.pass_far()
    meta_g.finish()
    meta = meta_all[...]
    routing_maps(me, meta, 0, sa, ga, rela, top_k, local)
    s_map = sa[...].reshape(local * n_dev, LANES)

    def rows_of(d):
        fill_rows(s_map, d, ((x_all, u_ref),), cap)

    rows_of(me)
    rows_of(links.left)
    rows_of(links.right)
    x_g.wait_partner()
    rows_of(links.partner)
    x_g.pass_far()
    x_g.wait_sides()
    side = 1 - 2 * links.core
    rows_of(links.left + side)
    rows_of(links.right + side)
    rows_of(links.opp)
    y_g.pass_on()
    routing_maps(me, meta, 1, sb, gb, relb, top_k, local)
    x_g.wait_last()
    rows_of(links.opp + side)
    forward_experts((w1_v, w3_v, w2_v), lambda e: wait_weights(pairs, w_sems, e), u_ref, o_ref, cap, 0, local)
    y_g.pass_far()
    stack = scatter_lhs(s_map, ga[...].reshape(local * n_dev, LANES), tok)
    red = Reduce(links, part, (near, mine, got))

    def sums_of(d):
        part[d] = token_sums(stack, d, o_ref[d].reshape(local * cap, width), tok, cap)

    sums_of(red.block(2, 1 - links.core))
    red.start_side(2)
    sums_of(red.block(2, links.core))
    for hop in (1, 3, 0):
        sums_of(red.block(hop, 1 - links.core))
        red.start_side(hop)
    red.far()
    sums_of(red.block(1, links.core))
    sums_of(red.block(3, links.core))
    red.near_sends()
    sums_of(red.block(0, links.core))
    red.relay()
    y_g.finish()
    y_store = pltpu.make_async_copy(y_all, dy_all, out_sem.at[0])
    y_store.start()
    x_mid = (x_ref[...].astype(F32) + red.result()).astype(BF16)
    mid_buf[...] = x_mid
    mid_own[...] = x_mid
    m_all[me] = x_mid
    m_g = Gather(links, mid_buf, m_all)
    m_g.pass_on()
    m_g.pass_far()
    m_g.finish()
    mid_all[...] = m_all[...]
    y_store.wait()
    links.drain()


def backward_kernel(dims, x_all, dy_all, s_ref, g_ref, rel_ref, w1, w3, w2,
                    dw1, dw3, dw2, part, dgate,
                    u_ref, y_ref, dg_ref, w1_v, w3_v, w2_v, w1_t, w3_t, w2_t, dw1_v, dw3_v, dw2_v, part_v,
                    w_sems, out_sems, part_sems):
    n_dev, tok, width, local, cap, top_k = dims
    pairs = ((w1, w1_v), (w3, w3_v), (w2, w2_v))
    load_weights(pairs, w_sems, local)
    n_rows = n_dev * cap
    outs = ((dw1_v, dw1), (dw3_v, dw3), (dw2_v, dw2))
    s_map = s_ref[...].reshape(local * n_dev, LANES)

    for d in range(n_dev):
        fill_rows(s_map, d, ((x_all, u_ref), (dy_all, y_ref)), cap)

    def store(g, i, slot):
        src, dst = outs[i]
        return pltpu.make_async_copy(src.at[slot], dst.at[pl.ds(g * GROUPED, GROUPED)], out_sems.at[i, slot])

    def step(g, carry):
        slot = lax.rem(g, SLOTS)
        experts = [g * GROUPED + i for i in range(GROUPED)]
        each = range(GROUPED)
        for e in experts:
            wait_weights(pairs, w_sems, e)

        @pl.when(g >= SLOTS)
        def _():
            for i in range(3):
                store(g - SLOTS, i, slot).wait()
        for i, e in enumerate(experts):
            w2_t[i] = w2_v[e].T
        u = [u_ref[:, e].reshape(n_rows, width) for e in experts]
        dy = [y_ref[:, e].reshape(n_rows, width) for e in experts]
        holds = [s_ref[e][:, None, :] == iota((n_dev, cap, LANES), 1).astype(F32) for e in experts]
        gate_row = [jnp.sum(jnp.where(holds[i], g_ref[e][:, None, :], 0.0), axis=2, keepdims=True).reshape(n_rows, 1)
                    for i, e in enumerate(experts)]
        q = [(gate_row[i] * dy[i].astype(F32)).astype(BF16) for i in each]
        pre = [(mm(u[i], w1_v[e]), mm(u[i], w3_v[e])) for i, e in enumerate(experts)]
        for i, e in enumerate(experts):
            w1_t[i] = w1_v[e].T
            w3_t[i] = w3_v[e].T
        d_hidden = [mm(q[i], w2_t[i]) for i in each]
        sig = [jax.nn.sigmoid(a) for a, _ in pre]
        act = [pre[i][0] * sig[i] for i in each]
        hidden = [(act[i] * pre[i][1]).astype(BF16) for i in each]
        out = [mm(hidden[i], w2_v[e]).astype(BF16) for i, e in enumerate(experts)]
        for i in each:
            dw2_v[slot, i] = mm_tn(hidden[i], q[i])
        d_gate = [(d_hidden[i] * pre[i][1] * sig[i] * (1.0 + pre[i][0] * (1.0 - sig[i]))).astype(BF16) for i in each]
        d_up = [(d_hidden[i] * act[i]).astype(BF16) for i in each]
        for i, e in enumerate(experts):
            dg_row = jnp.sum(dy[i].astype(F32) * out[i].astype(F32), axis=1, keepdims=True).reshape(n_dev, cap, 1)
            dg_ref[e] = jnp.sum(jnp.where(holds[i], dg_row, 0.0), axis=1)
        for i, e in enumerate(experts):
            du = (mm(d_gate[i], w1_t[i]) + mm(d_up[i], w3_t[i])).astype(BF16)
            y_ref[:, e] = du.reshape(n_dev, cap, width)
        for i in each:
            dw1_v[slot, i] = mm_tn(u[i], d_gate[i])
            dw3_v[slot, i] = mm_tn(u[i], d_up[i])
        for i in range(3):
            store(g, i, slot).start()
        return carry
    steps = local // GROUPED
    lax.fori_loop(0, steps, step, 0)

    stack = scatter_lhs(s_map, None, tok)
    for d in range(n_dev):
        part_v[d] = token_sums(stack, d, y_ref[d].reshape(local * cap, width), tok, cap)
        pltpu.make_async_copy(part_v.at[d], part.at[d], part_sems.at[d]).start()
    for d in range(n_dev):
        total = jnp.zeros((top_k, LANES), F32)
        for i in range(local):
            total = jnp.where(rel_ref[d] == float(i), dg_ref[i, d : d + 1, :], total)
        dgate[d] = total
    for g in range(max(steps - SLOTS, 0), steps):
        for i in range(3):
            store(g, i, g % SLOTS).wait()
    for d in range(n_dev):
        pltpu.make_async_copy(part_v.at[d], part.at[d], part_sems.at[d]).wait()


def middle_kernel(dims, dy_ref, x_ref, sb, gb, part_in, mid_in, w1, w3, w2,
                  x_again, dmid_all, dmid_own, own_x, right_x, opp_x, left_x,
                  part_b, mid_all, in_sems, part_x, near_x, d_all, x_all, u_ref, near, mine, got, d_buf, w1_v, w3_v, w2_v,
                  w_sems, send_sems, recv_sems):
    n_dev, tok, width, local, cap, top_k = dims
    pairs = ((w1, w1_v), (w3, w3_v), (w2, w2_v))
    part_load = pltpu.make_async_copy(part_in, part_b, in_sems.at[0])
    mid_load = pltpu.make_async_copy(mid_in, mid_all, in_sems.at[1])
    part_load.start()
    mid_load.start()
    load_weights(pairs, w_sems, local)
    links = Links(n_dev, send_sems, recv_sems)
    me = links.me
    links.greet()
    part_load.wait()
    red = Reduce(links, part_b, (near, mine, got))
    s_map = sb[...].reshape(local * n_dev, LANES)

    def rows_of(d):
        fill_rows(s_map, d, ((mid_all, u_ref),), cap)

    red.start()
    mid_load.wait()
    for d in range(2):
        rows_of(d)
    red.far()
    red.near_sends()
    for d in range(2, n_dev):
        rows_of(d)
    red.relay()
    x_g = Gather(links, x_ref, x_all)
    x_all[me] = x_ref[...]
    half = local // 2 // FORWARD_GROUPED * FORWARD_GROUPED
    forward_experts((w1_v, w3_v, w2_v), lambda e: wait_weights(pairs, w_sems, e), u_ref, u_ref, cap, 0, half)
    dx = (dy_ref[...].astype(F32) + red.result()).astype(BF16)
    d_buf[...] = dx
    dmid_own[...] = dx
    d_all[me] = dx
    d_g = Gather(links, d_buf, d_all)
    x_g.pass_on()
    forward_experts((w1_v, w3_v, w2_v), lambda e: wait_weights(pairs, w_sems, e), u_ref, u_ref, cap, half, local)
    d_g.pass_on()
    x_g.pass_far()
    stack = scatter_lhs(s_map, gb[...].reshape(local * n_dev, LANES), tok)
    for d in range(n_dev):
        part_x[d % 2, d // 2] = token_sums(stack, d, u_ref[d].reshape(local * cap, width), tok, cap)
    side_x = links.copy(part_x.at[1 - links.core], near_x, links.partner)
    d_g.pass_far()
    x_g.finish()
    x_store = pltpu.make_async_copy(x_all, x_again, in_sems.at[2])
    x_store.start()
    side_x.wait_recv()
    for hop, out in enumerate((own_x, right_x, opp_x, left_x)):
        chip = lax.rem((me - links.core) // 2 + hop, n_dev // 2)
        out[...] = part_x[links.core, chip] + near_x[chip]
    d_g.finish()
    dmid_all[...] = d_all[...]
    x_store.wait()
    links.drain()


def final_kernel(mid_ref, own_x, left_x, opp_x, right_x, dx_ref, dgate_ref, x_out, dx_out, dga_out, dgb_out):
    total = own_x[...] + left_x[...] + opp_x[...] + right_x[...]
    x_out[...] = (mid_ref[...].astype(F32) + total).astype(BF16)
    dx_out[...] = dx_ref[...]
    top_k, tok = dga_out.shape
    dga_out[...] = dgate_ref[:top_k, :tok]
    dgb_out[...] = dgate_ref[top_k:, :tok]


def last_kernel(dims, dg_a, dg_b, dmid_ref, part_in, dx_out, dgate,
                part_a, in_sem, dg_part, near, mine, got, dg_near, dg_mine, dg_got, send_sems, recv_sems):
    part_load = pltpu.make_async_copy(part_in, part_a, in_sem.at[0])
    part_load.start()
    top_k = dims[-1]
    dg_part[:, :top_k, :] = dg_a[...]
    dg_part[:, top_k:, :] = dg_b[...]
    links = Links(dims[0], send_sems, recv_sems)
    links.greet()
    part_load.wait()
    red = Reduce(links, part_a, (near, mine, got))
    dg = Reduce(links, dg_part, (dg_near, dg_mine, dg_got), split=False)
    red.start()
    dg.start()
    red.far()
    red.near_sends()
    dg.far()
    dg.near_sends()
    red.relay()
    dg.relay()
    dx_out[...] = (dmid_ref[...].astype(F32) + red.result()).astype(BF16)
    dgate[...] = dg.result()
    links.drain()


def remote_params(ident):
    return pltpu.CompilerParams(collective_id=ident, has_side_effects=True, vmem_limit_bytes=ALL_VMEM)


def dma_sems(count):
    return [pltpu.SemaphoreType.DMA((count,)), pltpu.SemaphoreType.DMA((count,))]


def solution(mesh):
    n_dev = mesh.shape["ep"]
    tok_spec = P(("dp", "ep"))
    w_spec = P("ep")

    def device_program(x_in, idx_a, idx_b, gate_a, gate_b, dy_out, w1_a, w3_a, w2_a, w1_b, w3_b, w2_b):
        tok, top_k = idx_a.shape
        width = x_in.shape[1]
        local, _, inner = w1_a.shape
        cap = CAP_FACTOR * tok * top_k // (local * n_dev)
        dims = (n_dev, tok, width, local, cap, top_k)
        sds = jax.ShapeDtypeStruct
        rows_all = sds((n_dev, tok, width), BF16)
        part_all = sds((n_dev, tok, width), F32)
        dg_all = sds((n_dev, top_k, LANES), F32)
        map_s = sds((local, n_dev, LANES), F32)
        own = sds((tok, width), BF16)

        weights_v = [pltpu.VMEM((local, width, inner), BF16)] * 2 + [pltpu.VMEM((local, inner, width), BF16)]
        w_sems = pltpu.SemaphoreType.DMA((3, local))
        rows_v = pltpu.VMEM((n_dev, tok, width), BF16)
        expert_v = pltpu.VMEM((n_dev, local, cap, width), BF16)

        count = 4 * Gather.COPIES + Reduce.COPIES
        dy_all, mid_all, mid_own, sa, ga, rela, sb, gb, relb = pl.pallas_call(
            functools.partial(first_kernel, dims),
            out_shape=(rows_all, rows_all, own, map_s, map_s, dg_all, map_s, map_s, dg_all),
            in_specs=[VMEM] * 6 + [HBM] * 3,
            out_specs=[HBM] + [VMEM] * 8,
            scratch_shapes=[rows_v, rows_v, rows_v, pltpu.VMEM((4 * top_k, LANES), F32), pltpu.VMEM((n_dev, 4 * top_k, LANES), F32), expert_v, expert_v,
                            pltpu.VMEM((n_dev, tok, width), F32), *Reduce.scratch(tok, width),
                            pltpu.VMEM((tok, width), BF16), *weights_v, w_sems, pltpu.SemaphoreType.DMA((1,)), *dma_sems(count)],
            compiler_params=remote_params(0), name="first",
        )(x_in, dy_out, idx_a.T, gate_a.T, idx_b.T, gate_b.T, w1_a, w3_a, w2_a)

        part_v = pltpu.VMEM((n_dev, tok, width), F32)

        def backward(x_all, d_all, s, g, rel, w1, w3, w2):
            return pl.pallas_call(
                functools.partial(backward_kernel, dims),
                out_shape=(sds((local, width, inner), F32), sds((local, width, inner), F32),
                           sds((local, inner, width), F32), part_all, dg_all),
                in_specs=[VMEM] * 5 + [HBM] * 3,
                out_specs=[HBM] * 4 + [VMEM],
                scratch_shapes=[expert_v, expert_v, pltpu.VMEM((local, n_dev, LANES), F32), *weights_v,
                                *[pltpu.VMEM((GROUPED, inner, width), BF16)] * 2, pltpu.VMEM((GROUPED, width, inner), BF16),
                                *[pltpu.VMEM((SLOTS, GROUPED, width, inner), F32)] * 2,
                                pltpu.VMEM((SLOTS, GROUPED, inner, width), F32), part_v, w_sems,
                                pltpu.SemaphoreType.DMA((3, SLOTS)), pltpu.SemaphoreType.DMA((n_dev,))],
                compiler_params=pltpu.CompilerParams(vmem_limit_bytes=ALL_VMEM), name="backward",
                cost_estimate=pl.CostEstimate(flops=18 * local * n_dev * cap * width * inner, transcendentals=0,
                                              bytes_accessed=18 * local * width * inner),
            )(x_all, d_all, s, g, rel, w1, w3, w2)

        *grads_b, part_b, dg_b = backward(mid_all, dy_all, sb, gb, relb, w1_b, w3_b, w2_b)

        count = 2 * Gather.COPIES + Reduce.COPIES + 1
        sums = sds((tok, width), F32)
        chip_sums = pltpu.VMEM((n_dev // 2, tok, width), F32)
        x_again, dmid_all, dmid_own, own_x, right_x, opp_x, left_x = pl.pallas_call(
            functools.partial(middle_kernel, dims),
            out_shape=(rows_all, rows_all, own, sums, sums, sums, sums),
            in_specs=[VMEM] * 4 + [HBM] * 5,
            out_specs=[HBM] + [VMEM] * 6,
            scratch_shapes=[part_v, rows_v, pltpu.SemaphoreType.DMA((3,)),
                            pltpu.VMEM((2, n_dev // 2, tok, width), F32), chip_sums, rows_v, rows_v, expert_v,
                            *Reduce.scratch(tok, width), pltpu.VMEM((tok, width), BF16),
                            *weights_v, w_sems, *dma_sems(count)],
            compiler_params=remote_params(1), name="middle",
        )(dy_out, x_in, sb, gb, part_b, mid_all, w1_b, w3_b, w2_b)

        def shift(rows, hop):
            return lax.ppermute(rows, "ep", [(i, (i + 2 * hop) % n_dev) for i in range(n_dev)])

        left_x, opp_x, right_x = shift(right_x, 1), shift(opp_x, 2), shift(left_x, 3)
        *grads_a, part_a, dg_a = backward(x_again, dmid_all, sa, ga, rela, w1_a, w3_a, w2_a)

        dx_in, dgates = pl.pallas_call(
            functools.partial(last_kernel, dims),
            out_shape=(own, sds((2 * top_k, LANES), F32)),
            in_specs=[VMEM] * 3 + [HBM],
            out_specs=[VMEM] * 2,
            scratch_shapes=[part_v, pltpu.SemaphoreType.DMA((1,)), pltpu.VMEM((n_dev, 2 * top_k, LANES), F32),
                            *Reduce.scratch(tok, width), *Reduce.scratch(2 * top_k, LANES), *dma_sems(2 * Reduce.COPIES)],
            compiler_params=remote_params(2), name="last",
        )(dg_a, dg_b, dmid_own, part_a)
        gates = sds((top_k, tok), F32)
        x_out, dx_in, dgate_a, dgate_b = pl.pallas_call(
            final_kernel, out_shape=(own, own, gates, gates), in_specs=[VMEM] * 7, out_specs=[VMEM] * 4, name="final",
            compiler_params=pltpu.CompilerParams(vmem_limit_bytes=60 * MIB),
        )(mid_own, own_x, left_x, opp_x, right_x, dx_in, dgates)
        return (x_out, dx_in, *grads_a, *grads_b, dgate_a.T, dgate_b.T)

    return jax.shard_map(device_program, mesh=mesh, in_specs=(tok_spec,) * 6 + (w_spec,) * 6, out_specs=(tok_spec,) * 10, check_vma=False)
```

```python
import functools

import jax
import jax.numpy as jnp
from jax import lax
from jax.experimental import pallas as pl
from jax.experimental.pallas import tpu as pltpu
from jax.sharding import PartitionSpec as P

BF16 = jnp.bfloat16
F32 = jnp.float32
MESH = pl.DeviceIdType.MESH
LANES = 128
CAP_FACTOR = 4
BF16_MAX = 3.3895313892515355e38
GROUPED = 2
SLOTS = 3
FORWARD_GROUPED = 4
MIB = 1024 * 1024
ALL_VMEM = 64 * MIB - 64 * 1024
VMEM = pl.BlockSpec(memory_space=pltpu.VMEM)
HBM = pl.BlockSpec(memory_space=pltpu.HBM)


def mm(lhs, rhs):
    return jnp.dot(lhs, rhs, preferred_element_type=F32)


def mm_tn(lhs, rhs):
    return lax.dot_general(lhs, rhs, (((0,), (0,)), ((), ())), preferred_element_type=F32)


def iota(shape, dim):
    return lax.broadcasted_iota(jnp.int32, shape, dim)


def routing_maps(me, meta, layer, s_ref, g_ref, rel_ref, top_k, local):
    n_dev = meta.shape[0]
    base = (me * local).astype(F32)
    row = 2 * layer * top_k
    rel_ref[...] = meta[:, row : row + top_k, :] - base
    shape = (local, n_dev, LANES)
    expert = iota(shape, 0).astype(F32)
    hit, gate = jnp.zeros(shape, F32), jnp.zeros(shape, F32)
    for j in range(top_k):
        match = (meta[:, row + j, :] - base)[None] == expert
        hit = jnp.where(match, 1.0, hit)
        gate = jnp.where(match, meta[:, row + top_k + j, :][None], gate)
    hit = hit.reshape(local * n_dev, LANES)
    earlier = (iota((LANES, LANES), 0) < iota((LANES, LANES), 1)).astype(F32).astype(BF16)
    slot = jnp.where(hit > 0.0, mm(hit.astype(BF16), earlier), -1.0)
    s_ref[...] = slot.reshape(shape)
    g_ref[...] = gate


def row_picks(s_map, d, tok, n_dev, cap):
    pairs, lanes = s_map.shape
    n_rows = pairs // n_dev * cap
    spread = iota((n_rows, pairs), 1) == iota((n_rows, pairs), 0) // cap * n_dev + d
    slot = mm(spread.astype(F32).astype(BF16), s_map.astype(BF16))
    return jnp.where(slot == (iota((n_rows, lanes), 0) % cap).astype(F32), 1.0, 0.0).astype(BF16)[:, :tok]


def fill_rows(s_map, d, sources, cap):
    picks = row_picks(s_map, d, sources[0][0].shape[1], sources[0][0].shape[0], cap)
    for rows, out in sources:
        out[d] = mm(picks, rows[d]).astype(BF16).reshape(out.shape[1:])


def limbs(gate):
    hi = jnp.minimum(gate, BF16_MAX).astype(BF16)
    rest = gate - hi.astype(F32)
    mid = rest.astype(BF16)
    return hi, mid, (rest - mid.astype(F32)).astype(BF16)


def scatter_lhs(s_map, g_map, tok):
    stack = [s_map.T[:tok].astype(BF16)]
    if g_map is not None:
        stack += [limb.T[:tok].astype(BF16) for limb in (x.astype(F32) for x in limbs(g_map))]
    return jnp.concatenate(stack, axis=0)


def token_sums(stack, d, out_rows, tok, cap):
    pairs = stack.shape[1]
    n_rows = out_rows.shape[0]
    spread = iota((pairs, n_rows), 0) == iota((pairs, n_rows), 1) // cap * 8 + d
    maps = mm(stack, spread.astype(F32).astype(BF16))
    match = maps[:tok] == (iota((tok, n_rows), 1) % cap).astype(F32)
    if stack.shape[0] == tok:
        return mm(jnp.where(match, 1.0, 0.0).astype(BF16), out_rows)
    terms = (stack.shape[0] - tok) // tok
    lhs = [jnp.where(match, maps[(i + 1) * tok : (i + 2) * tok], 0.0).astype(BF16) for i in range(terms)]
    sums = mm(jnp.concatenate(lhs, axis=0), out_rows)
    total = sums[:tok]
    for i in range(1, terms):
        total = total + sums[i * tok : (i + 1) * tok]
    return total


class Links:
    def __init__(self, n_dev, send_sems, recv_sems):
        me = lax.axis_index("ep")
        self.n = n_dev
        self.me = me
        self.core = lax.rem(me, 2)
        self.partner = me + 1 - 2 * self.core
        self.right = lax.rem(me + 2, n_dev)
        self.left = lax.rem(me + n_dev - 2, n_dev)
        self.opp = lax.rem(me + 4, n_dev)
        side = self.partner - me
        self.right_side, self.left_side = self.right + side, self.left + side
        self.send_sems, self.recv_sems = send_sems, recv_sems
        self.used = 0
        self.started = []

    def greet(self):
        barrier = pltpu.get_barrier_semaphore()
        peers = (self.partner, self.left, self.right, self.left_side, self.right_side)
        for peer in peers:
            pl.semaphore_signal(barrier, inc=1, device_id={"ep": peer}, device_id_type=MESH)
        pl.semaphore_wait(barrier, len(peers))

    def copy(self, src, dst, peer):
        slot = self.used
        self.used += 1
        rdma = pltpu.make_async_remote_copy(
            src_ref=src, dst_ref=dst, send_sem=self.send_sems.at[slot], recv_sem=self.recv_sems.at[slot],
            device_id={"ep": peer}, device_id_type=MESH)
        rdma.start()
        self.started.append(rdma)
        return rdma

    def drain(self):
        for rdma in self.started:
            rdma.wait_send()


class Gather:
    COPIES = 9

    def __init__(self, links, own, full):
        k, self.k, self.full = links, links, full
        self.half = own.shape[0] // 2
        self.to_right = k.copy(own, full.at[k.me], k.right)
        self.to_left = k.copy(own, full.at[k.me], k.left)
        self.to_partner = k.copy(own, full.at[k.me], k.partner)

    def pass_on(self):
        k, half = self.k, self.half
        upper, lower = pl.ds(0, half), pl.ds(half, half)
        self.to_right.wait_recv()
        self.far = [self.forward(k.left, upper, k.right), self.forward(k.left, upper, k.right_side)]
        side_a = self.forward(k.left, pl.ds(0, 2 * half), k.partner)
        self.to_left.wait_recv()
        self.far += [self.forward(k.right, lower, k.left), self.forward(k.right, lower, k.left_side)]
        self.sides = [side_a, self.forward(k.right, pl.ds(0, 2 * half), k.partner)]

    def forward(self, block, at, peer):
        return self.k.copy(self.full.at[block, at], self.full.at[block, at], peer)

    def wait_partner(self):
        self.to_partner.wait_recv()

    def wait_sides(self):
        for copy in self.sides:
            copy.wait_recv()

    def wait_far(self):
        for copy in self.far:
            copy.wait_recv()

    def finish(self):
        self.wait_partner()
        self.wait_sides()
        self.wait_far()


class Reduce:
    COPIES = 10

    @staticmethod
    def scratch(rows, width):
        return [pltpu.VMEM((4, rows, width), F32), pltpu.VMEM((4, rows, width), F32), pltpu.VMEM((3, rows, width), F32)]

    def __init__(self, links, part, bufs, split=True):
        self.k, self.part = links, part
        self.near, self.mine, self.got = bufs
        rows = part.shape[1]
        self.rows = rows
        self.half = rows // 2 if split else rows
        self.side = {}

    def block(self, hop, core):
        k = self.k
        return lax.rem(k.me - k.core + 2 * hop, k.n) + core

    def start_side(self, hop):
        k = self.k
        self.side[hop] = k.copy(self.part.at[self.block(hop, 1 - k.core)], self.near.at[hop], k.partner)

    def start(self):
        for hop in (2, 1, 3, 0):
            self.start_side(hop)

    def add(self, hop, lo, hi, extra=None):
        own = self.part[self.block(hop, self.k.core), lo:hi, :]
        total = own + self.near[hop, lo:hi, :]
        if extra is not None:
            total = total + extra
        self.mine[hop, lo:hi, :] = total

    def far(self):
        k, half, rows = self.k, self.half, self.rows
        self.side[2].wait_recv()
        self.add(2, 0, rows)
        a = pl.ds(0, half)
        self.far_a = k.copy(self.mine.at[2, a], self.got.at[2, a], k.right)
        if half < rows:
            b = pl.ds(half, rows - half)
            self.far_b = k.copy(self.mine.at[2, b], self.got.at[2, b], k.left)

    def near_sends(self):
        k, half, rows = self.k, self.half, self.rows
        self.side[1].wait_recv()
        if half < rows:
            b = pl.ds(half, rows - half)
            self.add(1, half, rows)
            self.right_b = k.copy(self.mine.at[1, b], self.got.at[0, b], k.right)
        self.side[3].wait_recv()
        self.add(3, 0, half)
        a = pl.ds(0, half)
        self.left_a = k.copy(self.mine.at[3, a], self.got.at[1, a], k.left)

    def relay(self):
        k, half, rows = self.k, self.half, self.rows
        a = pl.ds(0, half)
        self.far_a.wait_recv()
        self.add(1, 0, half, self.got[2, :half, :])
        self.right_a = k.copy(self.mine.at[1, a], self.got.at[0, a], k.right)
        if half < rows:
            b = pl.ds(half, rows - half)
            self.far_b.wait_recv()
            self.add(3, half, rows, self.got[2, half:, :])
            self.left_b = k.copy(self.mine.at[3, b], self.got.at[1, b], k.left)

    def result(self):
        half, rows = self.half, self.rows
        self.side[0].wait_recv()
        if half < rows:
            self.right_b.wait_recv()
        self.left_a.wait_recv()
        self.right_a.wait_recv()
        if half < rows:
            self.left_b.wait_recv()
        return self.part[self.k.me] + self.near[0] + self.got[0] + self.got[1]


def load_weights(pairs, sems, local):
    def start(e, carry):
        for i, (src, dst) in enumerate(pairs):
            pltpu.make_async_copy(src.at[e], dst.at[e], sems.at[i, e]).start()
        return carry
    lax.fori_loop(0, local, start, 0)


def wait_weights(pairs, sems, e):
    for i, (src, dst) in enumerate(pairs):
        pltpu.make_async_copy(src.at[e], dst.at[e], sems.at[i, e]).wait()


def forward_experts(weights, ready, u_ref, o_ref, cap, first, last):
    n_dev, _, _, width = u_ref.shape
    few = min(FORWARD_GROUPED, last - first)

    def step(g, carry):
        experts = [first + g * few + i for i in range(few)]
        for e in experts:
            ready(e)
        w_gate, w_up, w_down = weights
        rows = [u_ref[:, e].reshape(n_dev * cap, width) for e in experts]
        pre = [(mm(u, w_gate[e]), mm(u, w_up[e])) for u, e in zip(rows, experts)]
        hidden = [(gate * jax.nn.sigmoid(gate) * up).astype(BF16) for gate, up in pre]
        for h, e in zip(hidden, experts):
            o_ref[:, e] = mm(h, w_down[e]).astype(BF16).reshape(n_dev, cap, width)
        return carry
    lax.fori_loop(0, (last - first) // few, step, 0)


def first_kernel(dims, x_ref, dy_ref, idx_a, gate_a, idx_b, gate_b, w1, w3, w2,
                 dy_all, mid_all, mid_own, sa, ga, rela, sb, gb, relb,
                 x_all, y_all, m_all, meta_ref, meta_all, u_ref, o_ref, part, near, mine, got, mid_buf, w1_v, w3_v, w2_v,
                 w_sems, out_sem, send_sems, recv_sems):
    n_dev, tok, width, local, cap, top_k = dims
    pairs = ((w1, w1_v), (w3, w3_v), (w2, w2_v))
    load_weights(pairs, w_sems, local)
    meta_ref[...] = jnp.full(meta_ref.shape, -1.0, F32)
    for i, ref in enumerate((idx_a, gate_a, idx_b, gate_b)):
        meta_ref[i * top_k : (i + 1) * top_k, :tok] = ref[...].astype(F32)
    links = Links(n_dev, send_sems, recv_sems)
    me = links.me
    links.greet()
    meta_g = Gather(links, meta_ref, meta_all)
    x_g = Gather(links, x_ref, x_all)
    meta_all[me] = meta_ref[...]
    x_all[me] = x_ref[...]
    y_all[me] = dy_ref[...]
    meta_g.pass_on()
    x_g.pass_on()
    y_g = Gather(links, dy_ref, y_all)
    meta_g.finish()
    meta = meta_all[...]
    routing_maps(me, meta, 0, sa, ga, rela, top_k, local)
    s_map = sa[...].reshape(local * n_dev, LANES)

    def rows_of(d):
        fill_rows(s_map, d, ((x_all, u_ref),), cap)

    rows_of(me)
    rows_of(links.left)
    rows_of(links.right)
    x_g.wait_partner()
    rows_of(links.partner)
    x_g.wait_sides()
    side = 1 - 2 * links.core
    rows_of(links.left + side)
    rows_of(links.right + side)
    y_g.pass_on()
    routing_maps(me, meta, 1, sb, gb, relb, top_k, local)
    x_g.wait_far()
    rows_of(links.opp)
    rows_of(links.opp + side)
    forward_experts((w1_v, w3_v, w2_v), lambda e: wait_weights(pairs, w_sems, e), u_ref, o_ref, cap, 0, local)
    stack = scatter_lhs(s_map, ga[...].reshape(local * n_dev, LANES), tok)
    red = Reduce(links, part, (near, mine, got))

    def sums_of(d):
        part[d] = token_sums(stack, d, o_ref[d].reshape(local * cap, width), tok, cap)

    sums_of(red.block(2, 1 - links.core))
    red.start_side(2)
    sums_of(red.block(2, links.core))
    for hop in (1, 3, 0):
        sums_of(red.block(hop, 1 - links.core))
        red.start_side(hop)
    red.far()
    sums_of(red.block(1, links.core))
    sums_of(red.block(3, links.core))
    red.near_sends()
    sums_of(red.block(0, links.core))
    red.relay()
    y_g.finish()
    y_store = pltpu.make_async_copy(y_all, dy_all, out_sem.at[0])
    y_store.start()
    x_mid = (x_ref[...].astype(F32) + red.result()).astype(BF16)
    mid_buf[...] = x_mid
    mid_own[...] = x_mid
    m_all[me] = x_mid
    m_g = Gather(links, mid_buf, m_all)
    m_g.pass_on()
    m_g.finish()
    mid_all[...] = m_all[...]
    y_store.wait()
    links.drain()


def backward_kernel(dims, x_all, dy_all, s_ref, g_ref, rel_ref, w1, w3, w2,
                    dw1, dw3, dw2, part, dgate,
                    u_ref, y_ref, dg_ref, w1_v, w3_v, w2_v, w1_t, w3_t, w2_t, dw1_v, dw3_v, dw2_v, part_v,
                    w_sems, out_sems, part_sems):
    n_dev, tok, width, local, cap, top_k = dims
    pairs = ((w1, w1_v), (w3, w3_v), (w2, w2_v))
    load_weights(pairs, w_sems, local)
    n_rows = n_dev * cap
    outs = ((dw1_v, dw1), (dw3_v, dw3), (dw2_v, dw2))
    s_map = s_ref[...].reshape(local * n_dev, LANES)

    for d in range(n_dev):
        fill_rows(s_map, d, ((x_all, u_ref), (dy_all, y_ref)), cap)

    def store(g, i, slot):
        src, dst = outs[i]
        return pltpu.make_async_copy(src.at[slot], dst.at[pl.ds(g * GROUPED, GROUPED)], out_sems.at[i, slot])

    def step(g, carry):
        slot = lax.rem(g, SLOTS)
        experts = [g * GROUPED + i for i in range(GROUPED)]
        each = range(GROUPED)
        for e in experts:
            wait_weights(pairs, w_sems, e)

        @pl.when(g >= SLOTS)
        def _():
            for i in range(3):
                store(g - SLOTS, i, slot).wait()
        for i, e in enumerate(experts):
            w2_t[i] = w2_v[e].T
        u = [u_ref[:, e].reshape(n_rows, width) for e in experts]
        dy = [y_ref[:, e].reshape(n_rows, width) for e in experts]
        holds = [s_ref[e][:, None, :] == iota((n_dev, cap, LANES), 1).astype(F32) for e in experts]
        gate_row = [jnp.sum(jnp.where(holds[i], g_ref[e][:, None, :], 0.0), axis=2, keepdims=True).reshape(n_rows, 1)
                    for i, e in enumerate(experts)]
        q = [(gate_row[i] * dy[i].astype(F32)).astype(BF16) for i in each]
        pre = [(mm(u[i], w1_v[e]), mm(u[i], w3_v[e])) for i, e in enumerate(experts)]
        for i, e in enumerate(experts):
            w1_t[i] = w1_v[e].T
            w3_t[i] = w3_v[e].T
        d_hidden = [mm(q[i], w2_t[i]) for i in each]
        sig = [jax.nn.sigmoid(a) for a, _ in pre]
        act = [pre[i][0] * sig[i] for i in each]
        hidden = [(act[i] * pre[i][1]).astype(BF16) for i in each]
        out = [mm(hidden[i], w2_v[e]).astype(BF16) for i, e in enumerate(experts)]
        for i in each:
            dw2_v[slot, i] = mm_tn(hidden[i], q[i])
        d_gate = [(d_hidden[i] * pre[i][1] * sig[i] * (1.0 + pre[i][0] * (1.0 - sig[i]))).astype(BF16) for i in each]
        d_up = [(d_hidden[i] * act[i]).astype(BF16) for i in each]
        for i, e in enumerate(experts):
            dg_row = jnp.sum(dy[i].astype(F32) * out[i].astype(F32), axis=1, keepdims=True).reshape(n_dev, cap, 1)
            dg_ref[e] = jnp.sum(jnp.where(holds[i], dg_row, 0.0), axis=1)
        for i, e in enumerate(experts):
            du = (mm(d_gate[i], w1_t[i]) + mm(d_up[i], w3_t[i])).astype(BF16)
            y_ref[:, e] = du.reshape(n_dev, cap, width)
        for i in each:
            dw1_v[slot, i] = mm_tn(u[i], d_gate[i])
            dw3_v[slot, i] = mm_tn(u[i], d_up[i])
        for i in range(3):
            store(g, i, slot).start()
        return carry
    steps = local // GROUPED
    lax.fori_loop(0, steps, step, 0)

    stack = scatter_lhs(s_map, None, tok)
    for d in range(n_dev):
        part_v[d] = token_sums(stack, d, y_ref[d].reshape(local * cap, width), tok, cap)
        pltpu.make_async_copy(part_v.at[d], part.at[d], part_sems.at[d]).start()
    for d in range(n_dev):
        total = jnp.zeros((top_k, LANES), F32)
        for i in range(local):
            total = jnp.where(rel_ref[d] == float(i), dg_ref[i, d : d + 1, :], total)
        dgate[d] = total
    for g in range(max(steps - SLOTS, 0), steps):
        for i in range(3):
            store(g, i, g % SLOTS).wait()
    for d in range(n_dev):
        pltpu.make_async_copy(part_v.at[d], part.at[d], part_sems.at[d]).wait()


def middle_kernel(dims, dy_ref, x_ref, sb, gb, part_in, mid_in, w1, w3, w2,
                  x_again, dmid_all, dmid_own, own_x, right_x, opp_x, left_x,
                  part_b, mid_all, in_sems, part_x, near_x, d_all, x_all, u_ref, near, mine, got, d_buf, w1_v, w3_v, w2_v,
                  w_sems, send_sems, recv_sems):
    n_dev, tok, width, local, cap, top_k = dims
    pairs = ((w1, w1_v), (w3, w3_v), (w2, w2_v))
    part_load = pltpu.make_async_copy(part_in, part_b, in_sems.at[0])
    mid_load = pltpu.make_async_copy(mid_in, mid_all, in_sems.at[1])
    part_load.start()
    mid_load.start()
    load_weights(pairs, w_sems, local)
    links = Links(n_dev, send_sems, recv_sems)
    me = links.me
    links.greet()
    part_load.wait()
    red = Reduce(links, part_b, (near, mine, got))
    s_map = sb[...].reshape(local * n_dev, LANES)

    def rows_of(d):
        fill_rows(s_map, d, ((mid_all, u_ref),), cap)

    red.start()
    mid_load.wait()
    for d in range(2):
        rows_of(d)
    red.far()
    red.near_sends()
    for d in range(2, n_dev):
        rows_of(d)
    red.relay()
    x_g = Gather(links, x_ref, x_all)
    x_all[me] = x_ref[...]
    half = local // 2 // FORWARD_GROUPED * FORWARD_GROUPED
    forward_experts((w1_v, w3_v, w2_v), lambda e: wait_weights(pairs, w_sems, e), u_ref, u_ref, cap, 0, half)
    dx = (dy_ref[...].astype(F32) + red.result()).astype(BF16)
    d_buf[...] = dx
    dmid_own[...] = dx
    d_all[me] = dx
    d_g = Gather(links, d_buf, d_all)
    x_g.pass_on()
    forward_experts((w1_v, w3_v, w2_v), lambda e: wait_weights(pairs, w_sems, e), u_ref, u_ref, cap, half, local)
    d_g.pass_on()
    stack = scatter_lhs(s_map, gb[...].reshape(local * n_dev, LANES), tok)
    for d in range(n_dev):
        part_x[d % 2, d // 2] = token_sums(stack, d, u_ref[d].reshape(local * cap, width), tok, cap)
    side_x = links.copy(part_x.at[1 - links.core], near_x, links.partner)
    x_g.finish()
    x_store = pltpu.make_async_copy(x_all, x_again, in_sems.at[2])
    x_store.start()
    side_x.wait_recv()
    for hop, out in enumerate((own_x, right_x, opp_x, left_x)):
        chip = lax.rem((me - links.core) // 2 + hop, n_dev // 2)
        out[...] = part_x[links.core, chip] + near_x[chip]
    d_g.finish()
    dmid_all[...] = d_all[...]
    x_store.wait()
    links.drain()


def final_kernel(mid_ref, own_x, left_x, opp_x, right_x, dx_ref, dgate_ref, x_out, dx_out, dga_out, dgb_out):
    total = own_x[...] + left_x[...] + opp_x[...] + right_x[...]
    x_out[...] = (mid_ref[...].astype(F32) + total).astype(BF16)
    dx_out[...] = dx_ref[...]
    top_k, tok = dga_out.shape
    dga_out[...] = dgate_ref[:top_k, :tok]
    dgb_out[...] = dgate_ref[top_k:, :tok]


def last_kernel(dims, dg_a, dg_b, dmid_ref, part_in, dx_out, dgate,
                part_a, in_sem, dg_part, near, mine, got, dg_near, dg_mine, dg_got, send_sems, recv_sems):
    part_load = pltpu.make_async_copy(part_in, part_a, in_sem.at[0])
    part_load.start()
    top_k = dims[-1]
    dg_part[:, :top_k, :] = dg_a[...]
    dg_part[:, top_k:, :] = dg_b[...]
    links = Links(dims[0], send_sems, recv_sems)
    links.greet()
    part_load.wait()
    red = Reduce(links, part_a, (near, mine, got))
    dg = Reduce(links, dg_part, (dg_near, dg_mine, dg_got), split=False)
    red.start()
    dg.start()
    red.far()
    red.near_sends()
    dg.far()
    dg.near_sends()
    red.relay()
    dg.relay()
    dx_out[...] = (dmid_ref[...].astype(F32) + red.result()).astype(BF16)
    dgate[...] = dg.result()
    links.drain()


def remote_params(ident):
    return pltpu.CompilerParams(collective_id=ident, has_side_effects=True, vmem_limit_bytes=ALL_VMEM)


def dma_sems(count):
    return [pltpu.SemaphoreType.DMA((count,)), pltpu.SemaphoreType.DMA((count,))]


def solution(mesh):
    n_dev = mesh.shape["ep"]
    tok_spec = P(("dp", "ep"))
    w_spec = P("ep")

    def device_program(x_in, idx_a, idx_b, gate_a, gate_b, dy_out, w1_a, w3_a, w2_a, w1_b, w3_b, w2_b):
        tok, top_k = idx_a.shape
        width = x_in.shape[1]
        local, _, inner = w1_a.shape
        cap = CAP_FACTOR * tok * top_k // (local * n_dev)
        dims = (n_dev, tok, width, local, cap, top_k)
        sds = jax.ShapeDtypeStruct
        rows_all = sds((n_dev, tok, width), BF16)
        part_all = sds((n_dev, tok, width), F32)
        dg_all = sds((n_dev, top_k, LANES), F32)
        map_s = sds((local, n_dev, LANES), F32)
        own = sds((tok, width), BF16)

        weights_v = [pltpu.VMEM((local, width, inner), BF16)] * 2 + [pltpu.VMEM((local, inner, width), BF16)]
        w_sems = pltpu.SemaphoreType.DMA((3, local))
        rows_v = pltpu.VMEM((n_dev, tok, width), BF16)
        expert_v = pltpu.VMEM((n_dev, local, cap, width), BF16)

        count = 4 * Gather.COPIES + Reduce.COPIES
        dy_all, mid_all, mid_own, sa, ga, rela, sb, gb, relb = pl.pallas_call(
            functools.partial(first_kernel, dims),
            out_shape=(rows_all, rows_all, own, map_s, map_s, dg_all, map_s, map_s, dg_all),
            in_specs=[VMEM] * 6 + [HBM] * 3,
            out_specs=[HBM] + [VMEM] * 8,
            scratch_shapes=[rows_v, rows_v, rows_v, pltpu.VMEM((4 * top_k, LANES), F32), pltpu.VMEM((n_dev, 4 * top_k, LANES), F32), expert_v, expert_v,
                            pltpu.VMEM((n_dev, tok, width), F32), *Reduce.scratch(tok, width),
                            pltpu.VMEM((tok, width), BF16), *weights_v, w_sems, pltpu.SemaphoreType.DMA((1,)), *dma_sems(count)],
            compiler_params=remote_params(0), name="first",
        )(x_in, dy_out, idx_a.T, gate_a.T, idx_b.T, gate_b.T, w1_a, w3_a, w2_a)

        part_v = pltpu.VMEM((n_dev, tok, width), F32)

        def backward(x_all, d_all, s, g, rel, w1, w3, w2):
            return pl.pallas_call(
                functools.partial(backward_kernel, dims),
                out_shape=(sds((local, width, inner), F32), sds((local, width, inner), F32),
                           sds((local, inner, width), F32), part_all, dg_all),
                in_specs=[VMEM] * 5 + [HBM] * 3,
                out_specs=[HBM] * 4 + [VMEM],
                scratch_shapes=[expert_v, expert_v, pltpu.VMEM((local, n_dev, LANES), F32), *weights_v,
                                *[pltpu.VMEM((GROUPED, inner, width), BF16)] * 2, pltpu.VMEM((GROUPED, width, inner), BF16),
                                *[pltpu.VMEM((SLOTS, GROUPED, width, inner), F32)] * 2,
                                pltpu.VMEM((SLOTS, GROUPED, inner, width), F32), part_v, w_sems,
                                pltpu.SemaphoreType.DMA((3, SLOTS)), pltpu.SemaphoreType.DMA((n_dev,))],
                compiler_params=pltpu.CompilerParams(vmem_limit_bytes=ALL_VMEM), name="backward",
                cost_estimate=pl.CostEstimate(flops=18 * local * n_dev * cap * width * inner, transcendentals=0,
                                              bytes_accessed=18 * local * width * inner),
            )(x_all, d_all, s, g, rel, w1, w3, w2)

        *grads_b, part_b, dg_b = backward(mid_all, dy_all, sb, gb, relb, w1_b, w3_b, w2_b)

        count = 2 * Gather.COPIES + Reduce.COPIES + 1
        sums = sds((tok, width), F32)
        chip_sums = pltpu.VMEM((n_dev // 2, tok, width), F32)
        x_again, dmid_all, dmid_own, own_x, right_x, opp_x, left_x = pl.pallas_call(
            functools.partial(middle_kernel, dims),
            out_shape=(rows_all, rows_all, own, sums, sums, sums, sums),
            in_specs=[VMEM] * 4 + [HBM] * 5,
            out_specs=[HBM] + [VMEM] * 6,
            scratch_shapes=[part_v, rows_v, pltpu.SemaphoreType.DMA((3,)),
                            pltpu.VMEM((2, n_dev // 2, tok, width), F32), chip_sums, rows_v, rows_v, expert_v,
                            *Reduce.scratch(tok, width), pltpu.VMEM((tok, width), BF16),
                            *weights_v, w_sems, *dma_sems(count)],
            compiler_params=remote_params(1), name="middle",
        )(dy_out, x_in, sb, gb, part_b, mid_all, w1_b, w3_b, w2_b)

        def shift(rows, hop):
            return lax.ppermute(rows, "ep", [(i, (i + 2 * hop) % n_dev) for i in range(n_dev)])

        left_x, opp_x, right_x = shift(right_x, 1), shift(opp_x, 2), shift(left_x, 3)
        *grads_a, part_a, dg_a = backward(x_again, dmid_all, sa, ga, rela, w1_a, w3_a, w2_a)

        dx_in, dgates = pl.pallas_call(
            functools.partial(last_kernel, dims),
            out_shape=(own, sds((2 * top_k, LANES), F32)),
            in_specs=[VMEM] * 3 + [HBM],
            out_specs=[VMEM] * 2,
            scratch_shapes=[part_v, pltpu.SemaphoreType.DMA((1,)), pltpu.VMEM((n_dev, 2 * top_k, LANES), F32),
                            *Reduce.scratch(tok, width), *Reduce.scratch(2 * top_k, LANES), *dma_sems(2 * Reduce.COPIES)],
            compiler_params=remote_params(2), name="last",
        )(dg_a, dg_b, dmid_own, part_a)
        gates = sds((top_k, tok), F32)
        x_out, dx_in, dgate_a, dgate_b = pl.pallas_call(
            final_kernel, out_shape=(own, own, gates, gates), in_specs=[VMEM] * 7, out_specs=[VMEM] * 4, name="final",
            compiler_params=pltpu.CompilerParams(vmem_limit_bytes=60 * MIB),
        )(mid_own, own_x, left_x, opp_x, right_x, dx_in, dgates)
        return (x_out, dx_in, *grads_a, *grads_b, dgate_a.T, dgate_b.T)

    return jax.shard_map(device_program, mesh=mesh, in_specs=(tok_spec,) * 6 + (w_spec,) * 6, out_specs=(tok_spec,) * 10, check_vma=False)
```

```python
import functools

import jax
import jax.numpy as jnp
from jax import lax
from jax.experimental import pallas as pl
from jax.experimental.pallas import tpu as pltpu
from jax.sharding import PartitionSpec as P

BF16 = jnp.bfloat16
F32 = jnp.float32
MESH = pl.DeviceIdType.MESH
LANES = 128
CAP_FACTOR = 4
BF16_MAX = 3.3895313892515355e38
GROUPED = 2
SLOTS = 3
FORWARD_GROUPED = 4
MIB = 1024 * 1024
ALL_VMEM = 64 * MIB - 64 * 1024
VMEM = pl.BlockSpec(memory_space=pltpu.VMEM)
HBM = pl.BlockSpec(memory_space=pltpu.HBM)


def mm(lhs, rhs):
    return jnp.dot(lhs, rhs, preferred_element_type=F32)


def mm_tn(lhs, rhs):
    return lax.dot_general(lhs, rhs, (((0,), (0,)), ((), ())), preferred_element_type=F32)


def iota(shape, dim):
    return lax.broadcasted_iota(jnp.int32, shape, dim)


def routing_maps(me, meta, layer, s_ref, g_ref, rel_ref, top_k, local):
    n_dev = meta.shape[0]
    base = (me * local).astype(F32)
    row = 2 * layer * top_k
    rel_ref[...] = meta[:, row : row + top_k, :] - base
    shape = (local, n_dev, LANES)
    expert = iota(shape, 0).astype(F32)
    hit, gate = jnp.zeros(shape, F32), jnp.zeros(shape, F32)
    for j in range(top_k):
        match = (meta[:, row + j, :] - base)[None] == expert
        hit = jnp.where(match, 1.0, hit)
        gate = jnp.where(match, meta[:, row + top_k + j, :][None], gate)
    hit = hit.reshape(local * n_dev, LANES)
    earlier = (iota((LANES, LANES), 0) < iota((LANES, LANES), 1)).astype(F32).astype(BF16)
    slot = jnp.where(hit > 0.0, mm(hit.astype(BF16), earlier), -1.0)
    s_ref[...] = slot.reshape(shape)
    g_ref[...] = gate


def row_picks(s_map, d, tok, n_dev, cap):
    pairs, lanes = s_map.shape
    n_rows = pairs // n_dev * cap
    spread = iota((n_rows, pairs), 1) == iota((n_rows, pairs), 0) // cap * n_dev + d
    slot = mm(spread.astype(F32).astype(BF16), s_map.astype(BF16))
    return jnp.where(slot == (iota((n_rows, lanes), 0) % cap).astype(F32), 1.0, 0.0).astype(BF16)[:, :tok]


def fill_rows(s_map, d, sources, cap):
    picks = row_picks(s_map, d, sources[0][0].shape[1], sources[0][0].shape[0], cap)
    for rows, out in sources:
        out[d] = mm(picks, rows[d]).astype(BF16).reshape(out.shape[1:])


def limbs(gate):
    hi = jnp.minimum(gate, BF16_MAX).astype(BF16)
    rest = gate - hi.astype(F32)
    mid = rest.astype(BF16)
    return hi, mid, (rest - mid.astype(F32)).astype(BF16)


def scatter_lhs(s_map, g_map, tok):
    stack = [s_map.T[:tok].astype(BF16)]
    if g_map is not None:
        stack += [limb.T[:tok].astype(BF16) for limb in (x.astype(F32) for x in limbs(g_map))]
    return jnp.concatenate(stack, axis=0)


def token_sums(stack, d, out_rows, tok, cap):
    pairs = stack.shape[1]
    n_rows = out_rows.shape[0]
    spread = iota((pairs, n_rows), 0) == iota((pairs, n_rows), 1) // cap * 8 + d
    maps = mm(stack, spread.astype(F32).astype(BF16))
    match = maps[:tok] == (iota((tok, n_rows), 1) % cap).astype(F32)
    if stack.shape[0] == tok:
        return mm(jnp.where(match, 1.0, 0.0).astype(BF16), out_rows)
    terms = (stack.shape[0] - tok) // tok
    lhs = [jnp.where(match, maps[(i + 1) * tok : (i + 2) * tok], 0.0).astype(BF16) for i in range(terms)]
    sums = mm(jnp.concatenate(lhs, axis=0), out_rows)
    total = sums[:tok]
    for i in range(1, terms):
        total = total + sums[i * tok : (i + 1) * tok]
    return total


class Links:
    def __init__(self, n_dev, send_sems, recv_sems):
        me = lax.axis_index("ep")
        self.n = n_dev
        self.me = me
        self.core = lax.rem(me, 2)
        self.partner = me + 1 - 2 * self.core
        self.right = lax.rem(me + 2, n_dev)
        self.left = lax.rem(me + n_dev - 2, n_dev)
        self.opp = lax.rem(me + 4, n_dev)
        side = self.partner - me
        self.right_side, self.left_side = self.right + side, self.left + side
        self.send_sems, self.recv_sems = send_sems, recv_sems
        self.used = 0
        self.started = []

    def greet(self, sides=True):
        barrier = pltpu.get_barrier_semaphore()
        peers = (self.partner, self.left, self.right) + ((self.left_side, self.right_side) if sides else ())
        for peer in peers:
            pl.semaphore_signal(barrier, inc=1, device_id={"ep": peer}, device_id_type=MESH)
        pl.semaphore_wait(barrier, len(peers))

    def copy(self, src, dst, peer):
        slot = self.used
        self.used += 1
        rdma = pltpu.make_async_remote_copy(
            src_ref=src, dst_ref=dst, send_sem=self.send_sems.at[slot], recv_sem=self.recv_sems.at[slot],
            device_id={"ep": peer}, device_id_type=MESH)
        rdma.start()
        self.started.append(rdma)
        return rdma

    def drain(self):
        for rdma in self.started:
            rdma.wait_send()


class Gather:
    COPIES = 9

    def __init__(self, links, own, full, both=False):
        k, self.k, self.full, self.both = links, links, full, both
        self.half = own.shape[0] // 2
        self.to_right = k.copy(own, full.at[k.me], k.right)
        self.to_left = k.copy(own, full.at[k.me], k.left)
        self.to_partner = k.copy(own, full.at[k.me], k.partner)

    def pass_on(self):
        k, half = self.k, self.half
        self.upper, self.lower = pl.ds(0, half), pl.ds(half, half)
        self.to_right.wait_recv()
        self.far_up = [self.forward(k.left, self.upper, k.right)]
        if self.both:
            self.far_up.append(self.forward(k.left, self.upper, k.right_side))
        side_a = self.forward(k.left, pl.ds(0, 2 * half), k.partner)
        self.to_left.wait_recv()
        self.far_low = [self.forward(k.right, self.lower, k.left)]
        if self.both:
            self.far_low.append(self.forward(k.right, self.lower, k.left_side))
        self.sides = [side_a, self.forward(k.right, pl.ds(0, 2 * half), k.partner)]

    def pass_far(self):
        k = self.k
        self.far_up[0].wait_recv()
        self.far_up = [self.forward(k.opp, self.upper, k.partner)]
        self.far_low[0].wait_recv()
        self.far_low = [self.forward(k.opp, self.lower, k.partner)]

    def forward(self, block, at, peer):
        return self.k.copy(self.full.at[block, at], self.full.at[block, at], peer)

    def wait_partner(self):
        self.to_partner.wait_recv()

    def wait_sides(self):
        for copy in self.sides:
            copy.wait_recv()

    def wait_far(self):
        for copy in self.far_up + self.far_low:
            copy.wait_recv()

    def finish(self):
        self.wait_partner()
        self.wait_sides()
        self.wait_far()


class Reduce:
    COPIES = 10

    @staticmethod
    def scratch(rows, width):
        return [pltpu.VMEM((4, rows, width), F32), pltpu.VMEM((4, rows, width), F32), pltpu.VMEM((3, rows, width), F32)]

    def __init__(self, links, part, bufs, split=True):
        self.k, self.part = links, part
        self.near, self.mine, self.got = bufs
        rows = part.shape[1]
        self.rows = rows
        self.half = rows // 2 if split else rows
        self.side = {}

    def block(self, hop, core):
        k = self.k
        return lax.rem(k.me - k.core + 2 * hop, k.n) + core

    def start_side(self, hop):
        k = self.k
        self.side[hop] = k.copy(self.part.at[self.block(hop, 1 - k.core)], self.near.at[hop], k.partner)

    def start(self):
        for hop in (2, 1, 3, 0):
            self.start_side(hop)

    def add(self, hop, lo, hi, extra=None):
        own = self.part[self.block(hop, self.k.core), lo:hi, :]
        total = own + self.near[hop, lo:hi, :]
        if extra is not None:
            total = total + extra
        self.mine[hop, lo:hi, :] = total

    def far(self):
        k, half, rows = self.k, self.half, self.rows
        self.side[2].wait_recv()
        self.add(2, 0, rows)
        a = pl.ds(0, half)
        self.far_a = k.copy(self.mine.at[2, a], self.got.at[2, a], k.right)
        if half < rows:
            b = pl.ds(half, rows - half)
            self.far_b = k.copy(self.mine.at[2, b], self.got.at[2, b], k.left)

    def near_sends(self):
        k, half, rows = self.k, self.half, self.rows
        self.side[1].wait_recv()
        if half < rows:
            b = pl.ds(half, rows - half)
            self.add(1, half, rows)
            self.right_b = k.copy(self.mine.at[1, b], self.got.at[0, b], k.right)
        self.side[3].wait_recv()
        self.add(3, 0, half)
        a = pl.ds(0, half)
        self.left_a = k.copy(self.mine.at[3, a], self.got.at[1, a], k.left)

    def relay(self):
        k, half, rows = self.k, self.half, self.rows
        a = pl.ds(0, half)
        self.far_a.wait_recv()
        self.add(1, 0, half, self.got[2, :half, :])
        self.right_a = k.copy(self.mine.at[1, a], self.got.at[0, a], k.right)
        if half < rows:
            b = pl.ds(half, rows - half)
            self.far_b.wait_recv()
            self.add(3, half, rows, self.got[2, half:, :])
            self.left_b = k.copy(self.mine.at[3, b], self.got.at[1, b], k.left)

    def result(self):
        half, rows = self.half, self.rows
        self.side[0].wait_recv()
        if half < rows:
            self.right_b.wait_recv()
        self.left_a.wait_recv()
        self.right_a.wait_recv()
        if half < rows:
            self.left_b.wait_recv()
        return self.part[self.k.me] + self.near[0] + self.got[0] + self.got[1]


def load_weights(pairs, sems, local):
    def start(e, carry):
        for i, (src, dst) in enumerate(pairs):
            pltpu.make_async_copy(src.at[e], dst.at[e], sems.at[i, e]).start()
        return carry
    lax.fori_loop(0, local, start, 0)


def wait_weights(pairs, sems, e):
    for i, (src, dst) in enumerate(pairs):
        pltpu.make_async_copy(src.at[e], dst.at[e], sems.at[i, e]).wait()


def forward_experts(weights, ready, u_ref, o_ref, cap, first, last):
    n_dev, _, _, width = u_ref.shape
    few = min(FORWARD_GROUPED, last - first)

    def step(g, carry):
        experts = [first + g * few + i for i in range(few)]
        for e in experts:
            ready(e)
        w_gate, w_up, w_down = weights
        rows = [u_ref[:, e].reshape(n_dev * cap, width) for e in experts]
        pre = [(mm(u, w_gate[e]), mm(u, w_up[e])) for u, e in zip(rows, experts)]
        hidden = [(gate * jax.nn.sigmoid(gate) * up).astype(BF16) for gate, up in pre]
        for h, e in zip(hidden, experts):
            o_ref[:, e] = mm(h, w_down[e]).astype(BF16).reshape(n_dev, cap, width)
        return carry
    lax.fori_loop(0, (last - first) // few, step, 0)


def first_kernel(dims, x_ref, dy_ref, idx_a, gate_a, idx_b, gate_b, w1, w3, w2,
                 dy_all, mid_all, mid_own, sa, ga, rela, sb, gb, relb,
                 x_all, y_all, m_all, meta_ref, meta_all, u_ref, o_ref, part, near, mine, got, mid_buf, w1_v, w3_v, w2_v,
                 w_sems, out_sem, send_sems, recv_sems):
    n_dev, tok, width, local, cap, top_k = dims
    pairs = ((w1, w1_v), (w3, w3_v), (w2, w2_v))
    load_weights(pairs, w_sems, local)
    meta_ref[...] = jnp.full(meta_ref.shape, -1.0, F32)
    for i, ref in enumerate((idx_a, gate_a, idx_b, gate_b)):
        meta_ref[i * top_k : (i + 1) * top_k, :tok] = ref[...].astype(F32)
    links = Links(n_dev, send_sems, recv_sems)
    me = links.me
    links.greet()
    meta_g = Gather(links, meta_ref, meta_all)
    x_g = Gather(links, x_ref, x_all)
    meta_all[me] = meta_ref[...]
    x_all[me] = x_ref[...]
    y_all[me] = dy_ref[...]
    meta_g.pass_on()
    x_g.pass_on()
    y_g = Gather(links, dy_ref, y_all)
    meta_g.pass_far()
    meta_g.finish()
    meta = meta_all[...]
    routing_maps(me, meta, 0, sa, ga, rela, top_k, local)
    s_map = sa[...].reshape(local * n_dev, LANES)

    def rows_of(d):
        fill_rows(s_map, d, ((x_all, u_ref),), cap)

    rows_of(me)
    rows_of(links.left)
    rows_of(links.right)
    x_g.wait_partner()
    rows_of(links.partner)
    x_g.pass_far()
    x_g.wait_sides()
    side = 1 - 2 * links.core
    rows_of(links.left + side)
    rows_of(links.right + side)
    rows_of(links.opp)
    y_g.pass_on()
    routing_maps(me, meta, 1, sb, gb, relb, top_k, local)
    x_g.wait_far()
    rows_of(links.opp + side)
    forward_experts((w1_v, w3_v, w2_v), lambda e: wait_weights(pairs, w_sems, e), u_ref, o_ref, cap, 0, local)
    y_g.pass_far()
    stack = scatter_lhs(s_map, ga[...].reshape(local * n_dev, LANES), tok)
    red = Reduce(links, part, (near, mine, got))

    def sums_of(d):
        part[d] = token_sums(stack, d, o_ref[d].reshape(local * cap, width), tok, cap)

    sums_of(red.block(2, 1 - links.core))
    red.start_side(2)
    sums_of(red.block(2, links.core))
    for hop in (1, 3, 0):
        sums_of(red.block(hop, 1 - links.core))
        red.start_side(hop)
    red.far()
    sums_of(red.block(1, links.core))
    sums_of(red.block(3, links.core))
    red.near_sends()
    sums_of(red.block(0, links.core))
    red.relay()
    y_g.finish()
    y_store = pltpu.make_async_copy(y_all, dy_all, out_sem.at[0])
    y_store.start()
    x_mid = (x_ref[...].astype(F32) + red.result()).astype(BF16)
    mid_buf[...] = x_mid
    mid_own[...] = x_mid
    m_all[me] = x_mid
    m_g = Gather(links, mid_buf, m_all, both=True)
    m_g.pass_on()
    m_g.finish()
    mid_all[...] = m_all[...]
    y_store.wait()
    links.drain()


def backward_kernel(dims, x_all, dy_all, s_ref, g_ref, rel_ref, w1, w3, w2,
                    dw1, dw3, dw2, part, dgate,
                    u_ref, y_ref, dg_ref, w1_v, w3_v, w2_v, w1_t, w3_t, w2_t, dw1_v, dw3_v, dw2_v, part_v,
                    w_sems, out_sems, part_sems):
    n_dev, tok, width, local, cap, top_k = dims
    pairs = ((w1, w1_v), (w3, w3_v), (w2, w2_v))
    load_weights(pairs, w_sems, local)
    n_rows = n_dev * cap
    outs = ((dw1_v, dw1), (dw3_v, dw3), (dw2_v, dw2))
    s_map = s_ref[...].reshape(local * n_dev, LANES)

    for d in range(n_dev):
        fill_rows(s_map, d, ((x_all, u_ref), (dy_all, y_ref)), cap)

    def store(g, i, slot):
        src, dst = outs[i]
        return pltpu.make_async_copy(src.at[slot], dst.at[pl.ds(g * GROUPED, GROUPED)], out_sems.at[i, slot])

    def step(g, carry):
        slot = lax.rem(g, SLOTS)
        experts = [g * GROUPED + i for i in range(GROUPED)]
        each = range(GROUPED)
        for e in experts:
            wait_weights(pairs, w_sems, e)

        @pl.when(g >= SLOTS)
        def _():
            for i in range(3):
                store(g - SLOTS, i, slot).wait()
        for i, e in enumerate(experts):
            w2_t[i] = w2_v[e].T
        u = [u_ref[:, e].reshape(n_rows, width) for e in experts]
        dy = [y_ref[:, e].reshape(n_rows, width) for e in experts]
        holds = [s_ref[e][:, None, :] == iota((n_dev, cap, LANES), 1).astype(F32) for e in experts]
        gate_row = [jnp.sum(jnp.where(holds[i], g_ref[e][:, None, :], 0.0), axis=2, keepdims=True).reshape(n_rows, 1)
                    for i, e in enumerate(experts)]
        q = [(gate_row[i] * dy[i].astype(F32)).astype(BF16) for i in each]
        pre = [(mm(u[i], w1_v[e]), mm(u[i], w3_v[e])) for i, e in enumerate(experts)]
        for i, e in enumerate(experts):
            w1_t[i] = w1_v[e].T
            w3_t[i] = w3_v[e].T
        d_hidden = [mm(q[i], w2_t[i]) for i in each]
        sig = [jax.nn.sigmoid(a) for a, _ in pre]
        act = [pre[i][0] * sig[i] for i in each]
        hidden = [(act[i] * pre[i][1]).astype(BF16) for i in each]
        out = [mm(hidden[i], w2_v[e]).astype(BF16) for i, e in enumerate(experts)]
        for i in each:
            dw2_v[slot, i] = mm_tn(hidden[i], q[i])
        d_gate = [(d_hidden[i] * pre[i][1] * sig[i] * (1.0 + pre[i][0] * (1.0 - sig[i]))).astype(BF16) for i in each]
        d_up = [(d_hidden[i] * act[i]).astype(BF16) for i in each]
        for i, e in enumerate(experts):
            dg_row = jnp.sum(dy[i].astype(F32) * out[i].astype(F32), axis=1, keepdims=True).reshape(n_dev, cap, 1)
            dg_ref[e] = jnp.sum(jnp.where(holds[i], dg_row, 0.0), axis=1)
        for i, e in enumerate(experts):
            du = (mm(d_gate[i], w1_t[i]) + mm(d_up[i], w3_t[i])).astype(BF16)
            y_ref[:, e] = du.reshape(n_dev, cap, width)
        for i in each:
            dw1_v[slot, i] = mm_tn(u[i], d_gate[i])
            dw3_v[slot, i] = mm_tn(u[i], d_up[i])
        for i in range(3):
            store(g, i, slot).start()
        return carry
    steps = local // GROUPED
    lax.fori_loop(0, steps, step, 0)

    stack = scatter_lhs(s_map, None, tok)
    for d in range(n_dev):
        part_v[d] = token_sums(stack, d, y_ref[d].reshape(local * cap, width), tok, cap)
        pltpu.make_async_copy(part_v.at[d], part.at[d], part_sems.at[d]).start()
    for d in range(n_dev):
        total = jnp.zeros((top_k, LANES), F32)
        for i in range(local):
            total = jnp.where(rel_ref[d] == float(i), dg_ref[i, d : d + 1, :], total)
        dgate[d] = total
    for g in range(max(steps - SLOTS, 0), steps):
        for i in range(3):
            store(g, i, g % SLOTS).wait()
    for d in range(n_dev):
        pltpu.make_async_copy(part_v.at[d], part.at[d], part_sems.at[d]).wait()


def middle_kernel(dims, dy_ref, x_ref, sb, gb, part_in, mid_in, w1, w3, w2,
                  x_again, dmid_all, dmid_own, own_x, right_x, opp_x, left_x,
                  part_b, mid_all, in_sems, part_x, near_x, d_all, x_all, u_ref, near, mine, got, d_buf, w1_v, w3_v, w2_v,
                  w_sems, send_sems, recv_sems):
    n_dev, tok, width, local, cap, top_k = dims
    pairs = ((w1, w1_v), (w3, w3_v), (w2, w2_v))
    part_load = pltpu.make_async_copy(part_in, part_b, in_sems.at[0])
    mid_load = pltpu.make_async_copy(mid_in, mid_all, in_sems.at[1])
    part_load.start()
    mid_load.start()
    load_weights(pairs, w_sems, local)
    links = Links(n_dev, send_sems, recv_sems)
    me = links.me
    links.greet()
    part_load.wait()
    red = Reduce(links, part_b, (near, mine, got))
    s_map = sb[...].reshape(local * n_dev, LANES)

    def rows_of(d):
        fill_rows(s_map, d, ((mid_all, u_ref),), cap)

    red.start()
    mid_load.wait()
    for d in range(2):
        rows_of(d)
    red.far()
    red.near_sends()
    for d in range(2, n_dev):
        rows_of(d)
    red.relay()
    x_g = Gather(links, x_ref, x_all)
    x_all[me] = x_ref[...]
    half = local // 2 // FORWARD_GROUPED * FORWARD_GROUPED
    forward_experts((w1_v, w3_v, w2_v), lambda e: wait_weights(pairs, w_sems, e), u_ref, u_ref, cap, 0, half)
    dx = (dy_ref[...].astype(F32) + red.result()).astype(BF16)
    d_buf[...] = dx
    dmid_own[...] = dx
    d_all[me] = dx
    d_g = Gather(links, d_buf, d_all, both=True)
    x_g.pass_on()
    forward_experts((w1_v, w3_v, w2_v), lambda e: wait_weights(pairs, w_sems, e), u_ref, u_ref, cap, half, local)
    d_g.pass_on()
    x_g.pass_far()
    stack = scatter_lhs(s_map, gb[...].reshape(local * n_dev, LANES), tok)
    for d in range(n_dev):
        part_x[d % 2, d // 2] = token_sums(stack, d, u_ref[d].reshape(local * cap, width), tok, cap)
    side_x = links.copy(part_x.at[1 - links.core], near_x, links.partner)
    x_g.finish()
    x_store = pltpu.make_async_copy(x_all, x_again, in_sems.at[2])
    x_store.start()
    side_x.wait_recv()
    for hop, out in enumerate((own_x, right_x, opp_x, left_x)):
        chip = lax.rem((me - links.core) // 2 + hop, n_dev // 2)
        out[...] = part_x[links.core, chip] + near_x[chip]
    d_g.finish()
    dmid_all[...] = d_all[...]
    x_store.wait()
    links.drain()


def final_kernel(mid_ref, own_x, left_x, opp_x, right_x, dx_ref, dgate_ref, x_out, dx_out, dga_out, dgb_out):
    total = own_x[...] + left_x[...] + opp_x[...] + right_x[...]
    x_out[...] = (mid_ref[...].astype(F32) + total).astype(BF16)
    dx_out[...] = dx_ref[...]
    top_k, tok = dga_out.shape
    dga_out[...] = dgate_ref[:top_k, :tok]
    dgb_out[...] = dgate_ref[top_k:, :tok]


def last_kernel(dims, dg_a, dg_b, dmid_ref, part_in, dx_out, dgate,
                part_a, in_sem, dg_part, near, mine, got, dg_near, dg_mine, dg_got, send_sems, recv_sems):
    part_load = pltpu.make_async_copy(part_in, part_a, in_sem.at[0])
    part_load.start()
    top_k = dims[-1]
    dg_part[:, :top_k, :] = dg_a[...]
    dg_part[:, top_k:, :] = dg_b[...]
    links = Links(dims[0], send_sems, recv_sems)
    links.greet(sides=False)
    part_load.wait()
    red = Reduce(links, part_a, (near, mine, got))
    dg = Reduce(links, dg_part, (dg_near, dg_mine, dg_got), split=False)
    red.start()
    dg.start()
    red.far()
    red.near_sends()
    dg.far()
    dg.near_sends()
    red.relay()
    dg.relay()
    dx_out[...] = (dmid_ref[...].astype(F32) + red.result()).astype(BF16)
    dgate[...] = dg.result()
    links.drain()


def remote_params(ident):
    return pltpu.CompilerParams(collective_id=ident, has_side_effects=True, vmem_limit_bytes=ALL_VMEM)


def dma_sems(count):
    return [pltpu.SemaphoreType.DMA((count,)), pltpu.SemaphoreType.DMA((count,))]


def solution(mesh):
    n_dev = mesh.shape["ep"]
    tok_spec = P(("dp", "ep"))
    w_spec = P("ep")

    def device_program(x_in, idx_a, idx_b, gate_a, gate_b, dy_out, w1_a, w3_a, w2_a, w1_b, w3_b, w2_b):
        tok, top_k = idx_a.shape
        width = x_in.shape[1]
        local, _, inner = w1_a.shape
        cap = CAP_FACTOR * tok * top_k // (local * n_dev)
        dims = (n_dev, tok, width, local, cap, top_k)
        sds = jax.ShapeDtypeStruct
        rows_all = sds((n_dev, tok, width), BF16)
        part_all = sds((n_dev, tok, width), F32)
        dg_all = sds((n_dev, top_k, LANES), F32)
        map_s = sds((local, n_dev, LANES), F32)
        own = sds((tok, width), BF16)

        weights_v = [pltpu.VMEM((local, width, inner), BF16)] * 2 + [pltpu.VMEM((local, inner, width), BF16)]
        w_sems = pltpu.SemaphoreType.DMA((3, local))
        rows_v = pltpu.VMEM((n_dev, tok, width), BF16)
        expert_v = pltpu.VMEM((n_dev, local, cap, width), BF16)

        count = 4 * Gather.COPIES + Reduce.COPIES
        dy_all, mid_all, mid_own, sa, ga, rela, sb, gb, relb = pl.pallas_call(
            functools.partial(first_kernel, dims),
            out_shape=(rows_all, rows_all, own, map_s, map_s, dg_all, map_s, map_s, dg_all),
            in_specs=[VMEM] * 6 + [HBM] * 3,
            out_specs=[HBM] + [VMEM] * 8,
            scratch_shapes=[rows_v, rows_v, rows_v, pltpu.VMEM((4 * top_k, LANES), F32), pltpu.VMEM((n_dev, 4 * top_k, LANES), F32), expert_v, expert_v,
                            pltpu.VMEM((n_dev, tok, width), F32), *Reduce.scratch(tok, width),
                            pltpu.VMEM((tok, width), BF16), *weights_v, w_sems, pltpu.SemaphoreType.DMA((1,)), *dma_sems(count)],
            compiler_params=remote_params(0), name="first",
        )(x_in, dy_out, idx_a.T, gate_a.T, idx_b.T, gate_b.T, w1_a, w3_a, w2_a)

        part_v = pltpu.VMEM((n_dev, tok, width), F32)

        def backward(x_all, d_all, s, g, rel, w1, w3, w2):
            return pl.pallas_call(
                functools.partial(backward_kernel, dims),
                out_shape=(sds((local, width, inner), F32), sds((local, width, inner), F32),
                           sds((local, inner, width), F32), part_all, dg_all),
                in_specs=[VMEM] * 5 + [HBM] * 3,
                out_specs=[HBM] * 4 + [VMEM],
                scratch_shapes=[expert_v, expert_v, pltpu.VMEM((local, n_dev, LANES), F32), *weights_v,
                                *[pltpu.VMEM((GROUPED, inner, width), BF16)] * 2, pltpu.VMEM((GROUPED, width, inner), BF16),
                                *[pltpu.VMEM((SLOTS, GROUPED, width, inner), F32)] * 2,
                                pltpu.VMEM((SLOTS, GROUPED, inner, width), F32), part_v, w_sems,
                                pltpu.SemaphoreType.DMA((3, SLOTS)), pltpu.SemaphoreType.DMA((n_dev,))],
                compiler_params=pltpu.CompilerParams(vmem_limit_bytes=ALL_VMEM), name="backward",
                cost_estimate=pl.CostEstimate(flops=18 * local * n_dev * cap * width * inner, transcendentals=0,
                                              bytes_accessed=18 * local * width * inner),
            )(x_all, d_all, s, g, rel, w1, w3, w2)

        *grads_b, part_b, dg_b = backward(mid_all, dy_all, sb, gb, relb, w1_b, w3_b, w2_b)

        count = 2 * Gather.COPIES + Reduce.COPIES + 1
        sums = sds((tok, width), F32)
        chip_sums = pltpu.VMEM((n_dev // 2, tok, width), F32)
        x_again, dmid_all, dmid_own, own_x, right_x, opp_x, left_x = pl.pallas_call(
            functools.partial(middle_kernel, dims),
            out_shape=(rows_all, rows_all, own, sums, sums, sums, sums),
            in_specs=[VMEM] * 4 + [HBM] * 5,
            out_specs=[HBM] + [VMEM] * 6,
            scratch_shapes=[part_v, rows_v, pltpu.SemaphoreType.DMA((3,)),
                            pltpu.VMEM((2, n_dev // 2, tok, width), F32), chip_sums, rows_v, rows_v, expert_v,
                            *Reduce.scratch(tok, width), pltpu.VMEM((tok, width), BF16),
                            *weights_v, w_sems, *dma_sems(count)],
            compiler_params=remote_params(1), name="middle",
        )(dy_out, x_in, sb, gb, part_b, mid_all, w1_b, w3_b, w2_b)

        def shift(rows, hop):
            return lax.ppermute(rows, "ep", [(i, (i + 2 * hop) % n_dev) for i in range(n_dev)])

        left_x, opp_x, right_x = shift(right_x, 1), shift(opp_x, 2), shift(left_x, 3)
        *grads_a, part_a, dg_a = backward(x_again, dmid_all, sa, ga, rela, w1_a, w3_a, w2_a)

        dx_in, dgates = pl.pallas_call(
            functools.partial(last_kernel, dims),
            out_shape=(own, sds((2 * top_k, LANES), F32)),
            in_specs=[VMEM] * 3 + [HBM],
            out_specs=[VMEM] * 2,
            scratch_shapes=[part_v, pltpu.SemaphoreType.DMA((1,)), pltpu.VMEM((n_dev, 2 * top_k, LANES), F32),
                            *Reduce.scratch(tok, width), *Reduce.scratch(2 * top_k, LANES), *dma_sems(2 * Reduce.COPIES)],
            compiler_params=remote_params(2), name="last",
        )(dg_a, dg_b, dmid_own, part_a)
        gates = sds((top_k, tok), F32)
        x_out, dx_in, dgate_a, dgate_b = pl.pallas_call(
            final_kernel, out_shape=(own, own, gates, gates), in_specs=[VMEM] * 7, out_specs=[VMEM] * 4, name="final",
            compiler_params=pltpu.CompilerParams(vmem_limit_bytes=60 * MIB),
        )(mid_own, own_x, left_x, opp_x, right_x, dx_in, dgates)
        return (x_out, dx_in, *grads_a, *grads_b, dgate_a.T, dgate_b.T)

    return jax.shard_map(device_program, mesh=mesh, in_specs=(tok_spec,) * 6 + (w_spec,) * 6, out_specs=(tok_spec,) * 10, check_vma=False)
```

```python
import functools

import jax
import jax.numpy as jnp
from jax import lax
from jax.experimental import pallas as pl
from jax.experimental.pallas import tpu as pltpu
from jax.sharding import PartitionSpec as P

BF16 = jnp.bfloat16
F32 = jnp.float32
MESH = pl.DeviceIdType.MESH
LANES = 128
CAP_FACTOR = 4
BF16_MAX = 3.3895313892515355e38
GROUPED = 2
SLOTS = 3
FORWARD_GROUPED = 4
MIB = 1024 * 1024
ALL_VMEM = 64 * MIB - 64 * 1024
VMEM = pl.BlockSpec(memory_space=pltpu.VMEM)
HBM = pl.BlockSpec(memory_space=pltpu.HBM)


def mm(lhs, rhs):
    return jnp.dot(lhs, rhs, preferred_element_type=F32)


def mm_tn(lhs, rhs):
    return lax.dot_general(lhs, rhs, (((0,), (0,)), ((), ())), preferred_element_type=F32)


def iota(shape, dim):
    return lax.broadcasted_iota(jnp.int32, shape, dim)


def routing_maps(me, meta, layer, s_ref, g_ref, rel_ref, top_k, local):
    n_dev = meta.shape[0]
    base = (me * local).astype(F32)
    row = 2 * layer * top_k
    rel_ref[...] = meta[:, row : row + top_k, :] - base
    shape = (local, n_dev, LANES)
    expert = iota(shape, 0).astype(F32)
    hit, gate = jnp.zeros(shape, F32), jnp.zeros(shape, F32)
    for j in range(top_k):
        match = (meta[:, row + j, :] - base)[None] == expert
        hit = jnp.where(match, 1.0, hit)
        gate = jnp.where(match, meta[:, row + top_k + j, :][None], gate)
    hit = hit.reshape(local * n_dev, LANES)
    earlier = (iota((LANES, LANES), 0) < iota((LANES, LANES), 1)).astype(F32).astype(BF16)
    slot = jnp.where(hit > 0.0, mm(hit.astype(BF16), earlier), -1.0)
    s_ref[...] = slot.reshape(shape)
    g_ref[...] = gate


def row_picks(s_map, d, tok, n_dev, cap):
    pairs, lanes = s_map.shape
    n_rows = pairs // n_dev * cap
    spread = iota((n_rows, pairs), 1) == iota((n_rows, pairs), 0) // cap * n_dev + d
    slot = mm(spread.astype(F32).astype(BF16), s_map.astype(BF16))
    return jnp.where(slot == (iota((n_rows, lanes), 0) % cap).astype(F32), 1.0, 0.0).astype(BF16)[:, :tok]


def fill_rows(s_map, d, sources, cap):
    picks = row_picks(s_map, d, sources[0][0].shape[1], sources[0][0].shape[0], cap)
    for rows, out in sources:
        out[d] = mm(picks, rows[d]).astype(BF16).reshape(out.shape[1:])


def limbs(gate):
    hi = jnp.minimum(gate, BF16_MAX).astype(BF16)
    rest = gate - hi.astype(F32)
    mid = rest.astype(BF16)
    return hi, mid, (rest - mid.astype(F32)).astype(BF16)


def scatter_lhs(s_map, g_map, tok):
    stack = [s_map.T[:tok].astype(BF16)]
    if g_map is not None:
        stack += [limb.T[:tok].astype(BF16) for limb in (x.astype(F32) for x in limbs(g_map))]
    return jnp.concatenate(stack, axis=0)


def token_sums(stack, d, out_rows, tok, cap):
    pairs = stack.shape[1]
    n_rows = out_rows.shape[0]
    spread = iota((pairs, n_rows), 0) == iota((pairs, n_rows), 1) // cap * 8 + d
    maps = mm(stack, spread.astype(F32).astype(BF16))
    match = maps[:tok] == (iota((tok, n_rows), 1) % cap).astype(F32)
    if stack.shape[0] == tok:
        return mm(jnp.where(match, 1.0, 0.0).astype(BF16), out_rows)
    terms = (stack.shape[0] - tok) // tok
    lhs = [jnp.where(match, maps[(i + 1) * tok : (i + 2) * tok], 0.0).astype(BF16) for i in range(terms)]
    sums = mm(jnp.concatenate(lhs, axis=0), out_rows)
    total = sums[:tok]
    for i in range(1, terms):
        total = total + sums[i * tok : (i + 1) * tok]
    return total


class Links:
    def __init__(self, n_dev, send_sems, recv_sems):
        me = lax.axis_index("ep")
        self.n = n_dev
        self.me = me
        self.core = lax.rem(me, 2)
        self.partner = me + 1 - 2 * self.core
        self.right = lax.rem(me + 2, n_dev)
        self.left = lax.rem(me + n_dev - 2, n_dev)
        self.opp = lax.rem(me + 4, n_dev)
        side = self.partner - me
        self.right_side, self.left_side = self.right + side, self.left + side
        self.send_sems, self.recv_sems = send_sems, recv_sems
        self.used = 0
        self.started = []

    def greet(self, sides=True):
        barrier = pltpu.get_barrier_semaphore()
        peers = (self.partner, self.left, self.right) + ((self.left_side, self.right_side) if sides else ())
        for peer in peers:
            pl.semaphore_signal(barrier, inc=1, device_id={"ep": peer}, device_id_type=MESH)
        pl.semaphore_wait(barrier, len(peers))

    def copy(self, src, dst, peer):
        slot = self.used
        self.used += 1
        rdma = pltpu.make_async_remote_copy(
            src_ref=src, dst_ref=dst, send_sem=self.send_sems.at[slot], recv_sem=self.recv_sems.at[slot],
            device_id={"ep": peer}, device_id_type=MESH)
        rdma.start()
        self.started.append(rdma)
        return rdma

    def drain(self):
        for rdma in self.started:
            rdma.wait_send()


class Gather:
    COPIES = 9

    def __init__(self, links, own, full, both=False):
        k, self.k, self.full, self.both = links, links, full, both
        self.half = own.shape[0] // 2
        self.to_right = k.copy(own, full.at[k.me], k.right)
        self.to_left = k.copy(own, full.at[k.me], k.left)
        self.to_partner = k.copy(own, full.at[k.me], k.partner)

    def pass_on(self):
        k, half = self.k, self.half
        self.upper, self.lower = pl.ds(0, half), pl.ds(half, half)
        self.to_right.wait_recv()
        self.far_up = [self.forward(k.left, self.upper, k.right)]
        if self.both:
            self.far_up.append(self.forward(k.left, self.upper, k.right_side))
        side_a = self.forward(k.left, pl.ds(0, 2 * half), k.partner)
        self.to_left.wait_recv()
        self.far_low = [self.forward(k.right, self.lower, k.left)]
        if self.both:
            self.far_low.append(self.forward(k.right, self.lower, k.left_side))
        self.sides = [side_a, self.forward(k.right, pl.ds(0, 2 * half), k.partner)]

    def pass_far(self):
        k = self.k
        self.far_up[0].wait_recv()
        self.far_up = [self.forward(k.opp, self.upper, k.partner)]
        self.far_low[0].wait_recv()
        self.far_low = [self.forward(k.opp, self.lower, k.partner)]

    def forward(self, block, at, peer):
        return self.k.copy(self.full.at[block, at], self.full.at[block, at], peer)

    def wait_partner(self):
        self.to_partner.wait_recv()

    def wait_sides(self):
        for copy in self.sides:
            copy.wait_recv()

    def wait_far(self):
        for copy in self.far_up + self.far_low:
            copy.wait_recv()

    def finish(self):
        self.wait_partner()
        self.wait_sides()
        self.wait_far()


class Reduce:
    COPIES = 10

    @staticmethod
    def scratch(rows, width):
        return [pltpu.VMEM((4, rows, width), F32), pltpu.VMEM((4, rows, width), F32), pltpu.VMEM((3, rows, width), F32)]

    def __init__(self, links, part, bufs, split=True):
        self.k, self.part = links, part
        self.near, self.mine, self.got = bufs
        rows = part.shape[1]
        self.rows = rows
        self.half = rows // 2 if split else rows
        self.side = {}

    def block(self, hop, core):
        k = self.k
        return lax.rem(k.me - k.core + 2 * hop, k.n) + core

    def start_side(self, hop):
        k = self.k
        self.side[hop] = k.copy(self.part.at[self.block(hop, 1 - k.core)], self.near.at[hop], k.partner)

    def start(self):
        for hop in (2, 1, 3, 0):
            self.start_side(hop)

    def add(self, hop, lo, hi, extra=None):
        own = self.part[self.block(hop, self.k.core), lo:hi, :]
        total = own + self.near[hop, lo:hi, :]
        if extra is not None:
            total = total + extra
        self.mine[hop, lo:hi, :] = total

    def far(self):
        k, half, rows = self.k, self.half, self.rows
        self.side[2].wait_recv()
        self.add(2, 0, rows)
        a = pl.ds(0, half)
        self.far_a = k.copy(self.mine.at[2, a], self.got.at[2, a], k.right)
        if half < rows:
            b = pl.ds(half, rows - half)
            self.far_b = k.copy(self.mine.at[2, b], self.got.at[2, b], k.left)

    def near_sends(self):
        k, half, rows = self.k, self.half, self.rows
        self.side[1].wait_recv()
        if half < rows:
            b = pl.ds(half, rows - half)
            self.add(1, half, rows)
            self.right_b = k.copy(self.mine.at[1, b], self.got.at[0, b], k.right)
        self.side[3].wait_recv()
        self.add(3, 0, half)
        a = pl.ds(0, half)
        self.left_a = k.copy(self.mine.at[3, a], self.got.at[1, a], k.left)

    def relay(self):
        k, half, rows = self.k, self.half, self.rows
        a = pl.ds(0, half)
        self.far_a.wait_recv()
        self.add(1, 0, half, self.got[2, :half, :])
        self.right_a = k.copy(self.mine.at[1, a], self.got.at[0, a], k.right)
        if half < rows:
            b = pl.ds(half, rows - half)
            self.far_b.wait_recv()
            self.add(3, half, rows, self.got[2, half:, :])
            self.left_b = k.copy(self.mine.at[3, b], self.got.at[1, b], k.left)

    def result(self):
        half, rows = self.half, self.rows
        self.side[0].wait_recv()
        if half < rows:
            self.right_b.wait_recv()
        self.left_a.wait_recv()
        self.right_a.wait_recv()
        if half < rows:
            self.left_b.wait_recv()
        return self.part[self.k.me] + self.near[0] + self.got[0] + self.got[1]


def load_weights(pairs, sems, local):
    def start(e, carry):
        for i, (src, dst) in enumerate(pairs):
            pltpu.make_async_copy(src.at[e], dst.at[e], sems.at[i, e]).start()
        return carry
    lax.fori_loop(0, local, start, 0)


def wait_weights(pairs, sems, e):
    for i, (src, dst) in enumerate(pairs):
        pltpu.make_async_copy(src.at[e], dst.at[e], sems.at[i, e]).wait()


def forward_experts(weights, ready, u_ref, o_ref, cap, first, last):
    n_dev, _, _, width = u_ref.shape
    few = min(FORWARD_GROUPED, last - first)

    def step(g, carry):
        experts = [first + g * few + i for i in range(few)]
        for e in experts:
            ready(e)
        w_gate, w_up, w_down = weights
        rows = [u_ref[:, e].reshape(n_dev * cap, width) for e in experts]
        pre = [(mm(u, w_gate[e]), mm(u, w_up[e])) for u, e in zip(rows, experts)]
        hidden = [(gate * jax.nn.sigmoid(gate) * up).astype(BF16) for gate, up in pre]
        for h, e in zip(hidden, experts):
            o_ref[:, e] = mm(h, w_down[e]).astype(BF16).reshape(n_dev, cap, width)
        return carry
    lax.fori_loop(0, (last - first) // few, step, 0)


def first_kernel(dims, x_ref, dy_ref, idx_a, gate_a, idx_b, gate_b, w1, w3, w2,
                 dy_all, mid_all, mid_own, sa, ga, rela, sb, gb, relb,
                 x_all, y_all, m_all, meta_ref, meta_all, u_ref, o_ref, part, near, mine, got, mid_buf, w1_v, w3_v, w2_v,
                 w_sems, out_sem, send_sems, recv_sems):
    n_dev, tok, width, local, cap, top_k = dims
    pairs = ((w1, w1_v), (w3, w3_v), (w2, w2_v))
    load_weights(pairs, w_sems, local)
    meta_ref[...] = jnp.full(meta_ref.shape, -1.0, F32)
    for i, ref in enumerate((idx_a, gate_a, idx_b, gate_b)):
        meta_ref[i * top_k : (i + 1) * top_k, :tok] = ref[...].astype(F32)
    links = Links(n_dev, send_sems, recv_sems)
    me = links.me
    links.greet()
    meta_g = Gather(links, meta_ref, meta_all)
    x_g = Gather(links, x_ref, x_all)
    meta_all[me] = meta_ref[...]
    x_all[me] = x_ref[...]
    y_all[me] = dy_ref[...]
    meta_g.pass_on()
    x_g.pass_on()
    y_g = Gather(links, dy_ref, y_all)
    meta_g.pass_far()
    meta_g.finish()
    meta = meta_all[...]
    routing_maps(me, meta, 0, sa, ga, rela, top_k, local)
    s_map = sa[...].reshape(local * n_dev, LANES)

    def rows_of(d):
        fill_rows(s_map, d, ((x_all, u_ref),), cap)

    rows_of(me)
    rows_of(links.left)
    rows_of(links.right)
    x_g.wait_partner()
    rows_of(links.partner)
    x_g.pass_far()
    x_g.wait_sides()
    side = 1 - 2 * links.core
    rows_of(links.left + side)
    rows_of(links.right + side)
    rows_of(links.opp)
    y_g.pass_on()
    routing_maps(me, meta, 1, sb, gb, relb, top_k, local)
    x_g.wait_far()
    rows_of(links.opp + side)
    forward_experts((w1_v, w3_v, w2_v), lambda e: wait_weights(pairs, w_sems, e), u_ref, o_ref, cap, 0, local)
    y_g.pass_far()
    stack = scatter_lhs(s_map, ga[...].reshape(local * n_dev, LANES), tok)
    red = Reduce(links, part, (near, mine, got))

    def sums_of(d):
        part[d] = token_sums(stack, d, o_ref[d].reshape(local * cap, width), tok, cap)

    sums_of(red.block(2, 1 - links.core))
    red.start_side(2)
    sums_of(red.block(2, links.core))
    for hop in (1, 3, 0):
        sums_of(red.block(hop, 1 - links.core))
        red.start_side(hop)
    red.far()
    sums_of(red.block(1, links.core))
    sums_of(red.block(3, links.core))
    red.near_sends()
    sums_of(red.block(0, links.core))
    red.relay()
    y_g.finish()
    y_store = pltpu.make_async_copy(y_all, dy_all, out_sem.at[0])
    y_store.start()
    x_mid = (x_ref[...].astype(F32) + red.result()).astype(BF16)
    mid_buf[...] = x_mid
    mid_own[...] = x_mid
    m_all[me] = x_mid
    m_g = Gather(links, mid_buf, m_all, both=True)
    m_g.pass_on()
    m_g.finish()
    mid_all[...] = m_all[...]
    y_store.wait()
    links.drain()


def backward_kernel(dims, x_all, dy_all, s_ref, g_ref, rel_ref, w1, w3, w2,
                    dw1, dw3, dw2, part, dgate,
                    u_ref, y_ref, dg_ref, w1_v, w3_v, w2_v, w1_t, w3_t, w2_t, dw1_v, dw3_v, dw2_v, part_v,
                    w_sems, out_sems, part_sems):
    n_dev, tok, width, local, cap, top_k = dims
    pairs = ((w1, w1_v), (w3, w3_v), (w2, w2_v))
    load_weights(pairs, w_sems, local)
    n_rows = n_dev * cap
    outs = ((dw1_v, dw1), (dw3_v, dw3), (dw2_v, dw2))
    s_map = s_ref[...].reshape(local * n_dev, LANES)

    for d in range(n_dev):
        fill_rows(s_map, d, ((x_all, u_ref), (dy_all, y_ref)), cap)

    def store(g, i, slot):
        src, dst = outs[i]
        return pltpu.make_async_copy(src.at[slot], dst.at[pl.ds(g * GROUPED, GROUPED)], out_sems.at[i, slot])

    def step(g, carry):
        slot = lax.rem(g, SLOTS)
        experts = [g * GROUPED + i for i in range(GROUPED)]
        each = range(GROUPED)
        for e in experts:
            wait_weights(pairs, w_sems, e)

        @pl.when(g >= SLOTS)
        def _():
            for i in range(3):
                store(g - SLOTS, i, slot).wait()
        for i, e in enumerate(experts):
            w2_t[i] = w2_v[e].T
        u = [u_ref[:, e].reshape(n_rows, width) for e in experts]
        dy = [y_ref[:, e].reshape(n_rows, width) for e in experts]
        holds = [s_ref[e][:, None, :] == iota((n_dev, cap, LANES), 1).astype(F32) for e in experts]
        gate_row = [jnp.sum(jnp.where(holds[i], g_ref[e][:, None, :], 0.0), axis=2, keepdims=True).reshape(n_rows, 1)
                    for i, e in enumerate(experts)]
        q = [(gate_row[i] * dy[i].astype(F32)).astype(BF16) for i in each]
        pre = [(mm(u[i], w1_v[e]), mm(u[i], w3_v[e])) for i, e in enumerate(experts)]
        for i, e in enumerate(experts):
            w1_t[i] = w1_v[e].T
            w3_t[i] = w3_v[e].T
        d_hidden = [mm(q[i], w2_t[i]) for i in each]
        sig = [jax.nn.sigmoid(a) for a, _ in pre]
        act = [pre[i][0] * sig[i] for i in each]
        hidden = [(act[i] * pre[i][1]).astype(BF16) for i in each]
        out = [mm(hidden[i], w2_v[e]).astype(BF16) for i, e in enumerate(experts)]
        for i in each:
            dw2_v[slot, i] = mm_tn(hidden[i], q[i])
        d_gate = [(d_hidden[i] * pre[i][1] * sig[i] * (1.0 + pre[i][0] * (1.0 - sig[i]))).astype(BF16) for i in each]
        d_up = [(d_hidden[i] * act[i]).astype(BF16) for i in each]
        for i, e in enumerate(experts):
            dg_row = jnp.sum(dy[i].astype(F32) * out[i].astype(F32), axis=1, keepdims=True).reshape(n_dev, cap, 1)
            dg_ref[e] = jnp.sum(jnp.where(holds[i], dg_row, 0.0), axis=1)
        for i, e in enumerate(experts):
            du = (mm(d_gate[i], w1_t[i]) + mm(d_up[i], w3_t[i])).astype(BF16)
            y_ref[:, e] = du.reshape(n_dev, cap, width)
        for i in each:
            dw1_v[slot, i] = mm_tn(u[i], d_gate[i])
            dw3_v[slot, i] = mm_tn(u[i], d_up[i])
        for i in range(3):
            store(g, i, slot).start()
        return carry
    steps = local // GROUPED
    lax.fori_loop(0, steps, step, 0)

    stack = scatter_lhs(s_map, None, tok)
    for d in range(n_dev):
        part_v[d] = token_sums(stack, d, y_ref[d].reshape(local * cap, width), tok, cap)
        pltpu.make_async_copy(part_v.at[d], part.at[d], part_sems.at[d]).start()
    for d in range(n_dev):
        total = jnp.zeros((top_k, LANES), F32)
        for i in range(local):
            total = jnp.where(rel_ref[d] == float(i), dg_ref[i, d : d + 1, :], total)
        dgate[d] = total
    for g in range(max(steps - SLOTS, 0), steps):
        for i in range(3):
            store(g, i, g % SLOTS).wait()
    for d in range(n_dev):
        pltpu.make_async_copy(part_v.at[d], part.at[d], part_sems.at[d]).wait()


def middle_kernel(dims, dy_ref, x_ref, sb, gb, part_in, mid_in, w1, w3, w2,
                  x_again, dmid_all, dmid_own, own_x, right_x, opp_x, left_x,
                  part_b, mid_all, in_sems, part_x, near_x, d_all, x_all, u_ref, near, mine, got, d_buf, w1_v, w3_v, w2_v,
                  w_sems, send_sems, recv_sems):
    n_dev, tok, width, local, cap, top_k = dims
    pairs = ((w1, w1_v), (w3, w3_v), (w2, w2_v))
    part_load = pltpu.make_async_copy(part_in, part_b, in_sems.at[0])
    mid_load = pltpu.make_async_copy(mid_in, mid_all, in_sems.at[1])
    part_load.start()
    mid_load.start()
    load_weights(pairs, w_sems, local)
    links = Links(n_dev, send_sems, recv_sems)
    me = links.me
    links.greet()
    part_load.wait()
    red = Reduce(links, part_b, (near, mine, got))
    s_map = sb[...].reshape(local * n_dev, LANES)

    def rows_of(d):
        fill_rows(s_map, d, ((mid_all, u_ref),), cap)

    red.start()
    mid_load.wait()
    for d in range(2):
        rows_of(d)
    red.far()
    red.near_sends()
    for d in range(2, n_dev):
        rows_of(d)
    red.relay()
    x_g = Gather(links, x_ref, x_all, both=True)
    x_all[me] = x_ref[...]
    half = local // 2 // FORWARD_GROUPED * FORWARD_GROUPED
    forward_experts((w1_v, w3_v, w2_v), lambda e: wait_weights(pairs, w_sems, e), u_ref, u_ref, cap, 0, half)
    dx = (dy_ref[...].astype(F32) + red.result()).astype(BF16)
    d_buf[...] = dx
    dmid_own[...] = dx
    d_all[me] = dx
    d_g = Gather(links, d_buf, d_all, both=True)
    x_g.pass_on()
    forward_experts((w1_v, w3_v, w2_v), lambda e: wait_weights(pairs, w_sems, e), u_ref, u_ref, cap, half, local)
    d_g.pass_on()
    stack = scatter_lhs(s_map, gb[...].reshape(local * n_dev, LANES), tok)
    for d in range(n_dev):
        part_x[d % 2, d // 2] = token_sums(stack, d, u_ref[d].reshape(local * cap, width), tok, cap)
    side_x = links.copy(part_x.at[1 - links.core], near_x, links.partner)
    x_g.finish()
    x_store = pltpu.make_async_copy(x_all, x_again, in_sems.at[2])
    x_store.start()
    side_x.wait_recv()
    for hop, out in enumerate((own_x, right_x, opp_x, left_x)):
        chip = lax.rem((me - links.core) // 2 + hop, n_dev // 2)
        out[...] = part_x[links.core, chip] + near_x[chip]
    d_g.finish()
    dmid_all[...] = d_all[...]
    x_store.wait()
    links.drain()


def final_kernel(mid_ref, own_x, left_x, opp_x, right_x, dx_ref, dgate_ref, x_out, dx_out, dga_out, dgb_out):
    total = own_x[...] + left_x[...] + opp_x[...] + right_x[...]
    x_out[...] = (mid_ref[...].astype(F32) + total).astype(BF16)
    dx_out[...] = dx_ref[...]
    top_k, tok = dga_out.shape
    dga_out[...] = dgate_ref[:top_k, :tok]
    dgb_out[...] = dgate_ref[top_k:, :tok]


def last_kernel(dims, dg_a, dg_b, dmid_ref, part_in, dx_out, dgate,
                part_a, in_sem, dg_part, near, mine, got, dg_near, dg_mine, dg_got, send_sems, recv_sems):
    part_load = pltpu.make_async_copy(part_in, part_a, in_sem.at[0])
    part_load.start()
    top_k = dims[-1]
    dg_part[:, :top_k, :] = dg_a[...]
    dg_part[:, top_k:, :] = dg_b[...]
    links = Links(dims[0], send_sems, recv_sems)
    links.greet(sides=False)
    part_load.wait()
    red = Reduce(links, part_a, (near, mine, got))
    dg = Reduce(links, dg_part, (dg_near, dg_mine, dg_got), split=False)
    red.start()
    dg.start()
    red.far()
    red.near_sends()
    dg.far()
    dg.near_sends()
    red.relay()
    dg.relay()
    dx_out[...] = (dmid_ref[...].astype(F32) + red.result()).astype(BF16)
    dgate[...] = dg.result()
    links.drain()


def remote_params(ident):
    return pltpu.CompilerParams(collective_id=ident, has_side_effects=True, vmem_limit_bytes=ALL_VMEM)


def dma_sems(count):
    return [pltpu.SemaphoreType.DMA((count,)), pltpu.SemaphoreType.DMA((count,))]


def solution(mesh):
    n_dev = mesh.shape["ep"]
    tok_spec = P(("dp", "ep"))
    w_spec = P("ep")

    def device_program(x_in, idx_a, idx_b, gate_a, gate_b, dy_out, w1_a, w3_a, w2_a, w1_b, w3_b, w2_b):
        tok, top_k = idx_a.shape
        width = x_in.shape[1]
        local, _, inner = w1_a.shape
        cap = CAP_FACTOR * tok * top_k // (local * n_dev)
        dims = (n_dev, tok, width, local, cap, top_k)
        sds = jax.ShapeDtypeStruct
        rows_all = sds((n_dev, tok, width), BF16)
        part_all = sds((n_dev, tok, width), F32)
        dg_all = sds((n_dev, top_k, LANES), F32)
        map_s = sds((local, n_dev, LANES), F32)
        own = sds((tok, width), BF16)

        weights_v = [pltpu.VMEM((local, width, inner), BF16)] * 2 + [pltpu.VMEM((local, inner, width), BF16)]
        w_sems = pltpu.SemaphoreType.DMA((3, local))
        rows_v = pltpu.VMEM((n_dev, tok, width), BF16)
        expert_v = pltpu.VMEM((n_dev, local, cap, width), BF16)

        count = 4 * Gather.COPIES + Reduce.COPIES
        dy_all, mid_all, mid_own, sa, ga, rela, sb, gb, relb = pl.pallas_call(
            functools.partial(first_kernel, dims),
            out_shape=(rows_all, rows_all, own, map_s, map_s, dg_all, map_s, map_s, dg_all),
            in_specs=[VMEM] * 6 + [HBM] * 3,
            out_specs=[HBM] + [VMEM] * 8,
            scratch_shapes=[rows_v, rows_v, rows_v, pltpu.VMEM((4 * top_k, LANES), F32), pltpu.VMEM((n_dev, 4 * top_k, LANES), F32), expert_v, expert_v,
                            pltpu.VMEM((n_dev, tok, width), F32), *Reduce.scratch(tok, width),
                            pltpu.VMEM((tok, width), BF16), *weights_v, w_sems, pltpu.SemaphoreType.DMA((1,)), *dma_sems(count)],
            compiler_params=remote_params(0), name="first",
        )(x_in, dy_out, idx_a.T, gate_a.T, idx_b.T, gate_b.T, w1_a, w3_a, w2_a)

        part_v = pltpu.VMEM((n_dev, tok, width), F32)

        def backward(x_all, d_all, s, g, rel, w1, w3, w2):
            return pl.pallas_call(
                functools.partial(backward_kernel, dims),
                out_shape=(sds((local, width, inner), F32), sds((local, width, inner), F32),
                           sds((local, inner, width), F32), part_all, dg_all),
                in_specs=[VMEM] * 5 + [HBM] * 3,
                out_specs=[HBM] * 4 + [VMEM],
                scratch_shapes=[expert_v, expert_v, pltpu.VMEM((local, n_dev, LANES), F32), *weights_v,
                                *[pltpu.VMEM((GROUPED, inner, width), BF16)] * 2, pltpu.VMEM((GROUPED, width, inner), BF16),
                                *[pltpu.VMEM((SLOTS, GROUPED, width, inner), F32)] * 2,
                                pltpu.VMEM((SLOTS, GROUPED, inner, width), F32), part_v, w_sems,
                                pltpu.SemaphoreType.DMA((3, SLOTS)), pltpu.SemaphoreType.DMA((n_dev,))],
                compiler_params=pltpu.CompilerParams(vmem_limit_bytes=ALL_VMEM), name="backward",
                cost_estimate=pl.CostEstimate(flops=18 * local * n_dev * cap * width * inner, transcendentals=0,
                                              bytes_accessed=18 * local * width * inner),
            )(x_all, d_all, s, g, rel, w1, w3, w2)

        *grads_b, part_b, dg_b = backward(mid_all, dy_all, sb, gb, relb, w1_b, w3_b, w2_b)

        count = 2 * Gather.COPIES + Reduce.COPIES + 1
        sums = sds((tok, width), F32)
        chip_sums = pltpu.VMEM((n_dev // 2, tok, width), F32)
        x_again, dmid_all, dmid_own, own_x, right_x, opp_x, left_x = pl.pallas_call(
            functools.partial(middle_kernel, dims),
            out_shape=(rows_all, rows_all, own, sums, sums, sums, sums),
            in_specs=[VMEM] * 4 + [HBM] * 5,
            out_specs=[HBM] + [VMEM] * 6,
            scratch_shapes=[part_v, rows_v, pltpu.SemaphoreType.DMA((3,)),
                            pltpu.VMEM((2, n_dev // 2, tok, width), F32), chip_sums, rows_v, rows_v, expert_v,
                            *Reduce.scratch(tok, width), pltpu.VMEM((tok, width), BF16),
                            *weights_v, w_sems, *dma_sems(count)],
            compiler_params=remote_params(1), name="middle",
        )(dy_out, x_in, sb, gb, part_b, mid_all, w1_b, w3_b, w2_b)

        def shift(rows, hop):
            return lax.ppermute(rows, "ep", [(i, (i + 2 * hop) % n_dev) for i in range(n_dev)])

        left_x, opp_x, right_x = shift(right_x, 1), shift(opp_x, 2), shift(left_x, 3)
        *grads_a, part_a, dg_a = backward(x_again, dmid_all, sa, ga, rela, w1_a, w3_a, w2_a)

        dx_in, dgates = pl.pallas_call(
            functools.partial(last_kernel, dims),
            out_shape=(own, sds((2 * top_k, LANES), F32)),
            in_specs=[VMEM] * 3 + [HBM],
            out_specs=[VMEM] * 2,
            scratch_shapes=[part_v, pltpu.SemaphoreType.DMA((1,)), pltpu.VMEM((n_dev, 2 * top_k, LANES), F32),
                            *Reduce.scratch(tok, width), *Reduce.scratch(2 * top_k, LANES), *dma_sems(2 * Reduce.COPIES)],
            compiler_params=remote_params(2), name="last",
        )(dg_a, dg_b, dmid_own, part_a)
        gates = sds((top_k, tok), F32)
        x_out, dx_in, dgate_a, dgate_b = pl.pallas_call(
            final_kernel, out_shape=(own, own, gates, gates), in_specs=[VMEM] * 7, out_specs=[VMEM] * 4, name="final",
            compiler_params=pltpu.CompilerParams(vmem_limit_bytes=60 * MIB),
        )(mid_own, own_x, left_x, opp_x, right_x, dx_in, dgates)
        return (x_out, dx_in, *grads_a, *grads_b, dgate_a.T, dgate_b.T)

    return jax.shard_map(device_program, mesh=mesh, in_specs=(tok_spec,) * 6 + (w_spec,) * 6, out_specs=(tok_spec,) * 10, check_vma=False)
```
